32 devices in a mesh: seq: 8 (over z, x), head: 4 (over y, core).
Axes of the slice: x: 2, y: 2, z: 4, core: 2. Of those that a mesh axis runs over, the one named last changes fastest.
Arguments:
- inputs: bfloat16 [24, 1024, 512], P('seq', 'head'), may hold values from -6 to 6
- cotangent: bfloat16 [24, 1024, 512], P('seq', 'head'), may hold values from -6 to 6
- span_offset: int32 [24, 64], P('seq', 'head'), may hold values from 0 to 8
- span_len: int32 [24, 64], P('seq', 'head'), may hold values from 1 to 8
- owner_slot: int32 [256], replicated, may hold values from 0 to 255, as said below
- master: float32 [256, 128, 128], P(('seq', 'head')), as said below
- moment_one: float32 [256, 128, 128], P(('seq', 'head')), as said below
- moment_two: float32 [256, 128, 128], P(('seq', 'head')), may hold values from 294.912 to 29491.2, as said below
- basis_left: float32 [256, 128, 128], P(('seq', 'head')), may hold values from -1 to 1, as said below
- basis_right: float32 [256, 128, 128], P(('seq', 'head')), may hold values from -1 to 1, as said below
- average: float32 [256, 128, 128], P(('seq', 'head')), may hold values from -0.25 to 0.25
- vec_master: float32 [6144], P(('seq', 'head')), as said below
- vec_moment_one: float32 [6144], P(('seq', 'head')), may hold values from -343.46005 to 343.46005
- vec_moment_two: float32 [6144], P(('seq', 'head')), may hold values from 7372.8 to 29491.2
Outputs:
- layer_out: bfloat16 [24, 1024, 512], P('seq', 'head')
- input_grad: float32 [24, 1024, 512], P('seq', 'head')
- slot_grad: float32 [256, 128, 128], P(('seq', 'head'))
- vec_grad: float32 [6144], P(('seq', 'head'))
- new_moment_one: float32 [256, 128, 128], P(('seq', 'head'))
- new_moment_two: float32 [256, 128, 128], P(('seq', 'head'))
- new_master: float32 [256, 128, 128], P(('seq', 'head'))
- new_master_bf16: bfloat16 [256, 128, 128], P(('seq', 'head'))
- new_average: float32 [256, 128, 128], P(('seq', 'head'))
- new_vec_moment_one: float32 [6144], P(('seq', 'head'))
- new_vec_moment_two: float32 [6144], P(('seq', 'head'))
- new_vec: float32 [6144], P(('seq', 'head'))
The draws below stay inside these ranges and needn't reach their ends.
Inputs may be any that keep to these rules, and one draw needn't show every extreme that they name: `owner_slot`: A permutation of the slots; values of 192 or more mark empty slots. `master`: Real-valued blocks. `moment_one`: Real-valued, of both signs. `moment_two`: Positive. `basis_left`: each block is orthogonal. `basis_right`: each block is orthogonal. `vec_master`: the gains g_1 and g_2 are positive.
All inputs are finite; a program needn't handle non-finite values.
Results may differ from the reference program's by a relative error of at most 0.013.
The reference program's roundings to bfloat16 on the way count: a program that leaves them out, or rounds other values in their place, can miss the bound.
Values may be sent and summed in bfloat16 or wider, within the bound.
A program may use at most 128 MiB of HBM per device.

```python
import math
import jax
import jax.numpy as jnp
from jax import lax

D = 512
HEADS = 8
FF = 2048
LEN = 1024
WIN = 16
MAXW = 8
BLK = 128
SLOTS = 256
STEP = 5
SEQS = 24
TOKENS = 24576
NSPAN = 64
NBLK = 192
VEC = 6144


def slot_owner(base_key):
    return jax.random.permutation(jax.random.fold_in(base_key, 11), SLOTS).astype(jnp.int32)


def slot_kind(base_key):
    block = slot_owner(base_key)
    square = D // BLK * (D // BLK)
    oblong = D // BLK * (FF // BLK)
    return jnp.where(block < 4 * square, block // square, jnp.where(block < 4 * square + oblong, 4, jnp.where(block < NBLK, 5, 6)))


def lookup(kinds, table):
    return jnp.asarray(table, jnp.float32)[kinds]


def unit_noise(base_key, shape):
    return jax.random.normal(base_key, shape, jnp.float32)


def grad_size(base_key):
    return lookup(slot_kind(base_key), [0.7, 0.7, 1.0, 0.2, 0.3, 0.5, 0.5]) * math.sqrt(0.3 * TOKENS)


def draw_owner_slot(key, part):
    return slot_owner(key)


def draw_master(key, part):
    scale = lookup(slot_kind(key), [1.4, 1.4, 1.0, 3.0, 1.0, 1.0, 1.0]) / math.sqrt(D)
    return unit_noise(jax.random.fold_in(key, 21), (SLOTS, BLK, BLK)) * scale[:, None, None]


def draw_moment_one(key, part):
    return unit_noise(jax.random.fold_in(key, 22), (SLOTS, BLK, BLK)) * grad_size(key)[:, None, None]


def draw_moment_two(key, part):
    base_key = jax.random.fold_in(key, 23)
    factor = jnp.exp(jax.random.uniform(base_key, (SLOTS, BLK, BLK), jnp.float32, 0.0, math.log(4.0)))
    size = grad_size(key)
    return factor * (size * size)[:, None, None]


def orthogonal(base_key):
    row_index = jnp.arange(BLK, dtype=jnp.int32).astype(jnp.float32)
    col_index = jnp.arange(BLK, dtype=jnp.int32).astype(jnp.float32)
    angle = math.pi * (2.0 * row_index[:, None] + 1.0) * col_index[None, :] / (2.0 * BLK)
    weights = jnp.where(col_index == 0.0, math.sqrt(1.0 / BLK), math.sqrt(2.0 / BLK))
    table = jnp.cos(angle) * weights[None, :]
    left_signs = (2 * jax.random.randint(jax.random.fold_in(base_key, 1), (SLOTS, BLK), 0, 2) - 1).astype(jnp.float32)
    right_signs = (2 * jax.random.randint(jax.random.fold_in(base_key, 2), (SLOTS, BLK), 0, 2) - 1).astype(jnp.float32)
    return left_signs[:, :, None] * table[None, :, :] * right_signs[:, None, :]


def draw_basis_left(key, part):
    return orthogonal(jax.random.fold_in(key, 24))


def draw_basis_right(key, part):
    return orthogonal(jax.random.fold_in(key, 25))


def draw_vec_master(key, part):
    position = jnp.arange(8 * D + FF, dtype=jnp.int32)
    gain_one = (position >= 3 * D) & (position < 4 * D)
    gain_two = (position >= 6 * D + FF) & (position < 7 * D + FF)
    gains = jnp.exp(jax.random.uniform(jax.random.fold_in(key, 26), (8 * D + FF,), jnp.float32, math.log(0.5), math.log(2.0)))
    shifts = 0.5 * unit_noise(jax.random.fold_in(key, 27), (8 * D + FF,))
    return jnp.where(gain_one | gain_two, gains, shifts)


def with_ends(drawn, own_key, low, top_value):
    place = [jax.random.randint(jax.random.fold_in(own_key, axis), (), 0, length) for axis, length in enumerate(drawn.shape)]
    widest = drawn.shape.index(max(drawn.shape))
    neighbour = place[:widest] + [(place[widest] + 1) % drawn.shape[widest]] + place[widest + 1:]
    return drawn.at[tuple(place)].set(low).at[tuple(neighbour)].set(top_value)


def block_scale(rng, dims, split, smallest, largest):
    def one(dim, shards_of):
        heights = jax.random.uniform(jax.random.fold_in(jax.random.fold_in(rng, 6), dim), (shards_of,), jnp.float32, smallest / len(split), largest / len(split))
        return jnp.repeat(jnp.exp(heights), dims[dim] // shards_of).reshape((-1,) + (1,) * (len(dims) - dim - 1))

    loudness = one(*split[0])
    for cut in split[1:]:
        loudness = loudness * one(*cut)
    return loudness


def gaussian(own_key, dims, deviation, bound, cuts=(), kind=jnp.bfloat16):
    level = block_scale(own_key, dims, cuts, -0.22, 0.18) if cuts else 1.0
    entries = jax.random.normal(own_key, dims, jnp.float32) * deviation * level
    return jnp.minimum(jnp.maximum(entries, -bound), bound).astype(kind)


def setup_inputs(seed: int = 0) -> dict:
    arg_keys = jax.random.split(jax.random.key(seed), 15)
    inputs = gaussian(arg_keys[0], (SEQS, LEN, D), 1.0, 6.0, ((0, 8), (1, 4)))
    cotangent = gaussian(arg_keys[1], (SEQS, LEN, D), 1.0, 6.0, ((0, 8), (1, 4)))
    span_offset = with_ends(jax.random.randint(arg_keys[2], (SEQS, NSPAN), 0, WIN - MAXW + 1), jax.random.fold_in(arg_keys[2], 1), 0, WIN - MAXW).astype(jnp.int32)
    span_len = with_ends(jax.random.randint(arg_keys[3], (SEQS, NSPAN), 1, MAXW + 1), jax.random.fold_in(arg_keys[3], 1), 1, MAXW).astype(jnp.int32)
    owner_slot = draw_owner_slot(jax.random.fold_in(arg_keys[14], 71), 0)
    master = draw_master(jax.random.fold_in(arg_keys[14], 71), 0)
    moment_one = draw_moment_one(jax.random.fold_in(arg_keys[14], 71), 0)
    moment_two = draw_moment_two(jax.random.fold_in(arg_keys[14], 71), 0)
    basis_left = draw_basis_left(jax.random.fold_in(arg_keys[14], 71), 0)
    basis_right = draw_basis_right(jax.random.fold_in(arg_keys[14], 71), 0)
    average = gaussian(arg_keys[10], (SLOTS, BLK, BLK), D ** -0.5, 0.25, ((0, 32),), jnp.float32)
    vec_master = draw_vec_master(jax.random.fold_in(arg_keys[14], 71), 0)
    vec_moment_one = gaussian(arg_keys[12], (VEC,), ((TOKENS * 0.3) ** 0.5), 343.46005, ((0, 32),), jnp.float32)
    vec_moment_two = jnp.clip(jnp.exp(math.log(29491.2) - 1.3862944 * jax.random.uniform(arg_keys[13], (VEC,), jnp.float32) ** block_scale(arg_keys[13], (VEC,), ((0, 32),), -0.2, 0.2)), 7372.8, 29491.2)
    return {"inputs": inputs, "cotangent": cotangent, "span_offset": span_offset, "span_len": span_len, "owner_slot": owner_slot, "master": master, "moment_one": moment_one, "moment_two": moment_two, "basis_left": basis_left, "basis_right": basis_right, "average": average, "vec_master": vec_master, "vec_moment_one": vec_moment_one, "vec_moment_two": vec_moment_two}


@jax.custom_vjp
def low(v):
    return lax.optimization_barrier(v.astype(jnp.bfloat16)).astype(jnp.float32)

@jax.custom_vjp
def low_back(v):
    return v

def low_keep(v):
    return (low(v), None)

def low_pass(kept, grad):
    return (grad,)

def back_keep(v):
    return (v, None)

def back_low(kept, grad):
    return (low(grad),)
low.defvjp(low_keep, low_pass)
low_back.defvjp(back_keep, back_low)
HIGH = lax.Precision.HIGHEST
NORM_EPS = 1e-06
ADAM_EPS = 1e-08
RATE = 0.05
VEC_RATE = 0.2
DECAY = 0.01
KEEP = 0.9

def split_matrices(blocks):
    rows_d = D // BLK
    cols_f = FF // BLK
    square = rows_d * rows_d

    def build(pieces, row_count, col_count):
        return pieces.reshape(row_count, col_count, BLK, BLK).transpose(0, 2, 1, 3).reshape(row_count * BLK, col_count * BLK)
    matrices = [build(blocks[number * square:(number + 1) * square], rows_d, rows_d) for number in range(4)]
    offset = 4 * square
    matrices.append(build(blocks[offset:offset + rows_d * cols_f], rows_d, cols_f))
    matrices.append(build(blocks[offset + rows_d * cols_f:offset + 2 * rows_d * cols_f], cols_f, rows_d))
    return matrices

def join_matrices(matrices):
    pieces = []
    for matrix in matrices:
        row_count = matrix.shape[0] // BLK
        col_count = matrix.shape[1] // BLK
        pieces.append(matrix.reshape(row_count, BLK, col_count, BLK).transpose(0, 2, 1, 3).reshape(row_count * col_count, BLK, BLK))
    return jnp.concatenate(pieces, 0)

def split_vector(vector):
    widths = [D, D, D, D, D, FF, D, D, D]
    pieces = []
    offset = 0
    for extent in widths:
        pieces.append(vector[offset:offset + extent])
        offset = offset + extent
    return pieces

def layer_norm(values, gain, shift):
    center = values - lax.optimization_barrier(jnp.mean(values, axis=-1, keepdims=True))
    spread = lax.optimization_barrier(jnp.mean(center * center, axis=-1, keepdims=True))
    return center * lax.rsqrt(spread + NORM_EPS) * gain + shift

def gelu_value(values):
    return 0.5 * values * (1.0 + lax.erf(values * 0.7071067811865476))

def span_mask(span_offset, span_len):
    offsets = jnp.repeat(span_offset, WIN, axis=1)
    extents = jnp.repeat(span_len, WIN, axis=1)
    within = (jnp.arange(offsets.shape[1], dtype=jnp.int32) % WIN)[None, :]
    return ((within >= offsets) & (within < offsets + extents)).astype(jnp.float32)

def attend(query, keys_in, values_in):
    count, length_full, heads, size = query.shape
    block = min(512, length_full)
    scale = 1.0 / math.sqrt(size)

    def one_item(items):
        q_item, k_item, v_item = items
        outputs = []
        for begin_row in range(0, length_full, block):
            scores = jnp.einsum('qd,kd->qk', q_item[begin_row:begin_row + block], k_item, precision=HIGH) * scale
            scores = low_back(scores)
            highest = lax.optimization_barrier(jnp.max(scores, axis=-1, keepdims=True))
            weights_exp = jnp.exp(scores - highest)
            probs = weights_exp / lax.optimization_barrier(jnp.sum(weights_exp, axis=-1, keepdims=True))
            outputs.append(jnp.einsum('qk,kd->qd', low(probs), v_item, precision=HIGH))
        return jnp.concatenate(outputs, 0)
    items = tuple((tensor.transpose(0, 2, 1, 3).reshape(count * heads, length_full, size) for tensor in (query, keys_in, values_in)))
    context = lax.map(jax.checkpoint(one_item), items)
    return context.reshape(count, heads, length_full, size).transpose(0, 2, 1, 3)

def forward(matrices, vector, block_inputs):
    w_query, w_key, w_value, w_out, w_up, w_down = [low(matrix) for matrix in matrices]
    b_query, b_value, b_out, gain_one, shift_one, b_up, b_down, gain_two, shift_two = split_vector(vector)
    count, length_full, width = block_inputs.shape
    token_rows = block_inputs.reshape(count * length_full, width)
    query = low(low_back(jnp.dot(token_rows, w_query, precision=HIGH) + b_query))
    keys_all = low(low_back(jnp.dot(token_rows, w_key, precision=HIGH)))
    values_all = low(low_back(jnp.dot(token_rows, w_value, precision=HIGH) + b_value))
    shape_four = (count, length_full, HEADS, width // HEADS)
    context = attend(query.reshape(shape_four), keys_all.reshape(shape_four), values_all.reshape(shape_four))
    context = low(low_back(context.reshape(count * length_full, width)))
    branch = low_back(jnp.dot(context, w_out, precision=HIGH) + b_out)
    first = layer_norm(token_rows + branch, gain_one, shift_one)
    hidden_in = low_back(jnp.dot(low(first), w_up, precision=HIGH) + b_up)
    hidden_act = low(gelu_value(hidden_in))
    ffn_out = low_back(jnp.dot(hidden_act, w_down, precision=HIGH) + b_down)
    result = layer_norm(first + ffn_out, gain_two, shift_two)
    return result.reshape(count, length_full, width)

def rotate_adam(grads, master, moment_one, moment_two, basis_left, basis_right):
    rotated = jnp.einsum('sji,sjk->sik', basis_left, grads, precision=HIGH)
    rotated = jnp.einsum('sik,skl->sil', rotated, basis_right, precision=HIGH)
    first = 0.5 * moment_one + 0.5 * rotated
    second = 0.5 * moment_two + 0.5 * rotated * rotated
    correct = 1.0 - 0.5 ** STEP
    normed = first / correct / (jnp.sqrt(second / correct) + ADAM_EPS)
    turned = jnp.einsum('sij,sjk->sik', basis_left, normed, precision=HIGH)
    turned = jnp.einsum('sik,slk->sil', turned, basis_right, precision=HIGH)
    updated = master - RATE * (turned + DECAY * master)
    return (first, second, updated)

def reference(inputs, cotangent, span_offset, span_len, owner_slot, master, moment_one, moment_two, basis_left, basis_right, average, vec_master, vec_moment_one, vec_moment_two):
    inverse = jnp.zeros((SLOTS,), jnp.int32).at[owner_slot].set(jnp.arange(SLOTS, dtype=jnp.int32))
    matrices = tuple(split_matrices(master[inverse[:NBLK]]))
    mask = span_mask(span_offset, span_len)
    group = math.gcd(SEQS, max(1, 4096 // LEN))
    steps_count = SEQS // group
    grouped_inputs = inputs.astype(jnp.float32).reshape(steps_count, group, LEN, D)
    grouped_cots = (cotangent.astype(jnp.float32) * mask[:, :, None]).reshape(steps_count, group, LEN, D)

    def one_group(carry, item):
        block_inputs, block_cots = item
        result, pull = jax.vjp(forward, matrices, vec_master, block_inputs)
        grad_mats, grad_vec, grad_inputs = pull(block_cots)
        summed = tuple((total + term for total, term in zip(carry[0], grad_mats)))
        return ((summed, carry[1] + grad_vec), (result.astype(jnp.bfloat16), grad_inputs))
    start_carry = (tuple((jnp.zeros_like(matrix) for matrix in matrices)), jnp.zeros_like(vec_master))
    (grad_mats, vec_grad), (outputs, grad_inputs) = lax.scan(one_group, start_carry, (grouped_inputs, grouped_cots))
    layer_out = outputs.reshape(SEQS, LEN, D)
    input_grad = grad_inputs.reshape(SEQS, LEN, D)
    grad_blocks = join_matrices(list(grad_mats))
    padded = jnp.concatenate([grad_blocks, jnp.zeros((SLOTS - NBLK, BLK, BLK), jnp.float32)], 0)
    slot_grad = padded[owner_slot]
    first, second, updated = rotate_adam(slot_grad, master, moment_one, moment_two, basis_left, basis_right)
    correct = 1.0 - 0.5 ** STEP
    vec_first = 0.5 * vec_moment_one + 0.5 * vec_grad
    vec_second = 0.5 * vec_moment_two + 0.5 * vec_grad * vec_grad
    vec_new = vec_master - VEC_RATE * (vec_first / correct) / (jnp.sqrt(vec_second / correct) + ADAM_EPS)
    return (layer_out, input_grad, slot_grad, vec_grad, first, second, updated, updated.astype(jnp.bfloat16), KEEP * average + (1.0 - KEEP) * updated, vec_first, vec_second, vec_new)
```

```python
import functools
import math

import jax
import jax.numpy as jnp
from jax import lax
from jax.experimental import pallas as pl
from jax.experimental.pallas import tpu as pltpu
from jax.sharding import PartitionSpec as P

D = 512
FF = 2048
WIN = 16
BLK = 128
STEP = 5
HD = 64
NBLK = 192


NORM_EPS = 1e-06
ADAM_EPS = 1e-08
RATE = 0.05
VEC_RATE = 0.2
DECAY = 0.01
KEEP = 0.9
HIGH = lax.Precision.HIGHEST


def as_sent(array):

    def short(part):
        return part.astype(jnp.bfloat16) if part.dtype == jnp.float32 else part

    return jax.tree.map(short, array)


def split_matrices(blocks):
    rows_d = D // BLK
    cols_f = FF // BLK
    square = rows_d * rows_d

    def build(pieces, row_count, col_count):
        return (
            pieces.reshape(row_count, col_count, BLK, BLK)
            .transpose(0, 2, 1, 3)
            .reshape(row_count * BLK, col_count * BLK)
        )

    matrices = [
        build(blocks[number * square : (number + 1) * square], rows_d, rows_d)
        for number in range(4)
    ]
    offset = 4 * square
    matrices.append(build(blocks[offset : offset + rows_d * cols_f], rows_d, cols_f))
    matrices.append(
        build(blocks[offset + rows_d * cols_f : offset + 2 * rows_d * cols_f], cols_f, rows_d)
    )
    return matrices


def join_matrices(matrices):
    pieces = []
    for matrix in matrices:
        row_count = matrix.shape[0] // BLK
        col_count = matrix.shape[1] // BLK
        pieces.append(
            matrix.reshape(row_count, BLK, col_count, BLK)
            .transpose(0, 2, 1, 3)
            .reshape(row_count * col_count, BLK, BLK)
        )
    return jnp.concatenate(pieces, 0)


def split_vector(vector):
    widths = [D, D, D, D, D, FF, D, D, D]
    pieces = []
    offset = 0
    for extent in widths:
        pieces.append(vector[offset : offset + extent])
        offset = offset + extent
    return pieces


def layer_norm(values, gain, shift):
    center = values - jnp.mean(values, axis=-1, keepdims=True)
    spread = jnp.mean(center * center, axis=-1, keepdims=True)
    return center * lax.rsqrt(spread + NORM_EPS) * gain + shift


def gelu_value(values):
    return 0.5 * values * (1.0 + lax.erf(values * 0.7071067811865476))


def gelu_slope(values):
    return (
        0.5 * (1.0 + lax.erf(values * 0.7071067811865476))
        + values * jnp.exp(-0.5 * values * values) * 0.3989422804014327
    )


def span_mask(span_offset, span_len):
    offsets = jnp.repeat(span_offset, WIN, axis=1)
    extents = jnp.repeat(span_len, WIN, axis=1)
    within = (jnp.arange(offsets.shape[1], dtype=jnp.int32) % WIN)[None, :]
    return ((within >= offsets) & (within < offsets + extents)).astype(jnp.float32)


def attend_forward(query, keys_in, values_in, scale):
    length_full = query.shape[0]
    block = min(512, length_full)
    outputs = []
    totals = []
    for begin_row in range(0, length_full, block):
        scores = (
            jnp.einsum(
                "qhd,khd->hqk",
                query[begin_row : begin_row + block],
                keys_in,
                preferred_element_type=jnp.float32,
            )
            * scale
        )
        highest = jnp.max(scores, axis=-1, keepdims=True)
        weights_exp = jnp.exp(scores - highest)
        summed = jnp.sum(weights_exp, axis=-1, keepdims=True)
        probs = (weights_exp / summed).astype(jnp.bfloat16)
        outputs.append(
            jnp.einsum("hqk,khd->qhd", probs, values_in, preferred_element_type=jnp.float32)
        )
        totals.append(highest + jnp.log(summed))
    return (jnp.concatenate(outputs, 0).astype(jnp.bfloat16), jnp.concatenate(totals, 1))


def attend_backward(query, keys_in, values_in, grad_ctx, log_total, scale):
    length_full = query.shape[0]
    block = min(512, length_full)
    grad_keys = jnp.zeros(keys_in.shape, jnp.float32)
    grad_values = jnp.zeros(values_in.shape, jnp.float32)
    grad_queries = []
    for begin_row in range(0, length_full, block):
        rows_query = query[begin_row : begin_row + block]
        rows_grad = grad_ctx[begin_row : begin_row + block]
        scores = (
            jnp.einsum("qhd,khd->hqk", rows_query, keys_in, preferred_element_type=jnp.float32)
            * scale
        )
        probs = jnp.exp(scores - log_total[:, begin_row : begin_row + block])
        grad_probs = jnp.einsum(
            "qhd,khd->hqk", rows_grad, values_in, preferred_element_type=jnp.float32
        )
        inner = jnp.sum(probs * grad_probs, axis=-1, keepdims=True)
        grad_scores = (probs * (grad_probs - inner)).astype(jnp.bfloat16)
        grad_queries.append(
            jnp.einsum("hqk,khd->qhd", grad_scores, keys_in, preferred_element_type=jnp.float32)
            * scale
        )
        grad_keys = (
            grad_keys
            + jnp.einsum(
                "hqk,qhd->khd", grad_scores, rows_query, preferred_element_type=jnp.float32
            )
            * scale
        )
        grad_values = grad_values + jnp.einsum(
            "hqk,qhd->khd",
            probs.astype(jnp.bfloat16),
            rows_grad,
            preferred_element_type=jnp.float32,
        )
    return (
        jnp.concatenate(grad_queries, 0).astype(jnp.bfloat16),
        grad_keys.astype(jnp.bfloat16),
        grad_values.astype(jnp.bfloat16),
    )


def rotate_adam(grads, master, moment_one, moment_two, basis_left, basis_right):
    rotated = jnp.einsum("sji,sjk->sik", basis_left, grads, precision=HIGH)
    rotated = jnp.einsum("sik,skl->sil", rotated, basis_right, precision=HIGH)
    first = 0.5 * moment_one + 0.5 * rotated
    second = 0.5 * moment_two + 0.5 * rotated * rotated
    correct = 1.0 - 0.5**STEP
    normed = first / correct / (jnp.sqrt(second / correct) + ADAM_EPS)
    turned = jnp.einsum("sij,sjk->sik", basis_left, normed, precision=HIGH)
    turned = jnp.einsum("sik,slk->sil", turned, basis_right, precision=HIGH)
    updated = master - RATE * (turned + DECAY * master)
    return (first, second, updated)


def weight_grad(left, right):
    return jnp.einsum("ti,to->io", left, right, preferred_element_type=jnp.float32)


def back_product(grads, weight):
    return jnp.einsum("to,io->ti", grads, weight, preferred_element_type=jnp.float32)


MESH = pl.DeviceIdType.MESH
VEC_ROWS = 16


def cut(seq_size, head_size):
    cores = 2 if head_size % 2 == 0 else 1
    rows = 1
    while 2 * (rows * 2) ** 2 <= seq_size and seq_size % (rows * 2) == 0:
        rows = rows * 2
    return (seq_size // rows, rows, head_size // cores, cores)


def place(dims):
    size_z, size_x, size_y, size_c = dims
    seq = lax.axis_index("seq")
    head = lax.axis_index("head")
    return (
        lax.div(seq, size_x),
        lax.rem(seq, size_x),
        lax.div(head, size_c),
        lax.rem(head, size_c),
    )


def device(dims, coords):
    return (coords[0] * dims[1] + coords[1], coords[2] * dims[3] + coords[3])


def flat(dims, coords):
    return ((coords[0] * dims[1] + coords[1]) * dims[2] + coords[2]) * dims[3] + coords[3]


def moved(dims, coords, axis, step):
    new = list(coords)
    new[axis] = lax.rem(coords[axis] + step, dims[axis])
    return tuple(new)


def greet(dims, coords):
    barrier = pltpu.get_barrier_semaphore()
    count = 0
    for axis in range(4):
        for step in range(1, dims[axis]):
            pl.semaphore_signal(
                barrier,
                inc=1,
                device_id=device(dims, moved(dims, coords, axis, step)),
                device_id_type=MESH,
            )
            count = count + 1
    pl.semaphore_wait(barrier, count)


def greet_head(head_size):
    barrier = pltpu.get_barrier_semaphore()
    seq = lax.axis_index("seq")
    head = lax.axis_index("head")
    for step in range(1, head_size):
        pl.semaphore_signal(
            barrier, inc=1, device_id=(seq, lax.rem(head + step, head_size)), device_id_type=MESH
        )
    pl.semaphore_wait(barrier, head_size - 1)


def gather_kernel(
    dims, x_ref, w_ref, xf_ref, wf_ref, own_sem, x_send, x_recv, w_send, w_recv
):
    me = place(dims)
    size_z, size_x, size_y, size_c = dims
    head_me = me[2] * size_c + me[3]
    own_x = pltpu.make_async_copy(x_ref, xf_ref.at[:, head_me], own_sem.at[0])
    own_w = pltpu.make_async_copy(w_ref, wf_ref.at[flat(dims, me)], own_sem.at[1])
    own_x.start()
    own_w.start()
    greet(dims, me)
    started = []

    def send_x(source, head, target, number):
        copy = pltpu.make_async_remote_copy(
            src_ref=source,
            dst_ref=xf_ref.at[:, head],
            send_sem=x_send.at[number],
            recv_sem=x_recv.at[head],
            device_id=device(dims, target),
            device_id_type=MESH,
        )
        copy.start()
        started.append(copy)

    def arrived_x(head):
        pltpu.make_async_remote_copy(
            src_ref=x_ref,
            dst_ref=xf_ref.at[:, head],
            send_sem=x_send.at[0],
            recv_sem=x_recv.at[head],
            device_id=device(dims, me),
            device_id_type=MESH,
        ).wait_recv()

    count = [0]

    def send_w(source, index, target):
        number = count[0]
        count[0] = number + 1
        copy = pltpu.make_async_remote_copy(
            src_ref=source,
            dst_ref=wf_ref.at[index],
            send_sem=w_send.at[number],
            recv_sem=w_recv.at[index],
            device_id=device(dims, target),
            device_id_type=MESH,
        )
        copy.start()
        started.append(copy)

    def arrived_w(index):
        pltpu.make_async_remote_copy(
            src_ref=w_ref,
            dst_ref=wf_ref.at[index],
            send_sem=w_send.at[0],
            recv_sem=w_recv.at[index],
            device_id=device(dims, me),
            device_id_type=MESH,
        ).wait_recv()

    order = [0, 2, 1, 3]

    def forward(source, coords, after):
        for axis in order[after:]:
            for step in range(1, dims[axis]):
                send_w(source, flat(dims, coords), moved(dims, me, axis, step))

    number = 0
    for step in range(1, size_y):
        send_x(x_ref, head_me, moved(dims, me, 2, step), number)
        number = number + 1
    for step in range(1, size_c):
        send_x(x_ref, head_me, moved(dims, me, 3, step), number)
        number = number + 1
    forward(w_ref, me, 0)
    held = [me]
    for level in range(3):
        axis = order[level]
        fresh = []
        for step in range(1, dims[axis]):
            for coords in held:
                source = moved(dims, coords, axis, step)
                arrived_w(flat(dims, source))
                forward(wf_ref.at[flat(dims, source)], source, level + 1)
                fresh.append(source)
        held = held + fresh
        if level == 1:
            for step in range(1, size_y):
                other = moved(dims, me, 2, step)
                head = other[2] * size_c + other[3]
                arrived_x(head)
                for hop in range(1, size_c):
                    send_x(xf_ref.at[:, head], head, moved(dims, me, 3, hop), number)
                    number = number + 1
    for step in range(1, size_c):
        for coords in held:
            arrived_w(flat(dims, moved(dims, coords, 3, step)))
        for across in range(size_y):
            other = moved(dims, moved(dims, me, 3, step), 2, across)
            arrived_x(other[2] * size_c + other[3])
    for copy in started:
        copy.wait_send()
    own_x.wait()
    own_w.wait()


def gather_all(dims, inputs, packed):
    size_z, size_x, size_y, size_c = dims
    total = size_z * size_x * size_y * size_c
    head_size = size_y * size_c
    seq_local, tok_local, width = inputs.shape
    any_space = pl.BlockSpec(memory_space=pl.ANY)
    whole = pl.BlockSpec(memory_space=pltpu.VMEM)
    sends_x = (size_y - 1) * size_c + size_c - 1
    sends_w = (
        (size_z - 1)
        + size_z * (size_y - 1)
        + size_z * size_y * (size_x - 1)
        + size_z * size_y * size_x * (size_c - 1)
    )
    return pl.pallas_call(
        functools.partial(gather_kernel, dims),
        out_shape=(
            jax.ShapeDtypeStruct((seq_local, head_size, tok_local, width), inputs.dtype),
            jax.ShapeDtypeStruct((total,) + packed.shape, packed.dtype),
        ),
        in_specs=[whole, whole],
        out_specs=(any_space, any_space),
        scratch_shapes=[
            pltpu.SemaphoreType.DMA((2,)),
            pltpu.SemaphoreType.DMA((max(sends_x, 1),)),
            pltpu.SemaphoreType.DMA((head_size,)),
            pltpu.SemaphoreType.DMA((max(sends_w, 1),)),
            pltpu.SemaphoreType.DMA((total,)),
        ],
        compiler_params=pltpu.CompilerParams(collective_id=0, has_side_effects=True),
        name="gather_all",
    )(inputs, packed)


def exchange_kernel(head_size, src_ref, dst_ref, own_sem, send_sem, recv_sem):
    seq = lax.axis_index("seq")
    head = lax.axis_index("head")
    own = pltpu.make_async_copy(src_ref.at[head], dst_ref.at[head], own_sem)
    own.start()
    greet_head(head_size)
    copies = []
    for step in [2, 1, 3] if head_size == 4 else range(1, head_size):
        peer = lax.rem(head + step, head_size)
        copy = pltpu.make_async_remote_copy(
            src_ref=src_ref.at[peer],
            dst_ref=dst_ref.at[head],
            send_sem=send_sem.at[step],
            recv_sem=recv_sem.at[step],
            device_id=(seq, peer),
            device_id_type=MESH,
        )
        copy.start()
        copies.append(copy)
    for copy in copies:
        copy.wait()
    own.wait()


def exchange(array, number):
    head_size = array.shape[0]
    if head_size == 1:
        return array
    whole = pl.BlockSpec(memory_space=pltpu.VMEM)
    return pl.pallas_call(
        functools.partial(exchange_kernel, head_size),
        out_shape=jax.ShapeDtypeStruct(array.shape, array.dtype),
        in_specs=[whole],
        out_specs=whole,
        scratch_shapes=[
            pltpu.SemaphoreType.DMA,
            pltpu.SemaphoreType.DMA((head_size,)),
            pltpu.SemaphoreType.DMA((head_size,)),
        ],
        compiler_params=pltpu.CompilerParams(collective_id=number, has_side_effects=True),
        name="exchange",
    )(array)


def scatter_kernel(
    dims,
    slots,
    owner_ref,
    blocks_ref,
    vec_ref,
    grad_ref,
    vec_out_ref,
    term,
    got_c,
    got_x,
    got_y,
    got_z,
    send_c,
    send_x,
    send_y,
    send_z,
    recv_c,
    recv_x,
    recv_y,
    recv_z,
):
    me = place(dims)
    size_z, size_x, size_y, size_c = dims
    rows = slots * BLK
    greet(dims, me)

    def block_of(dest, slot):
        owner = owner_ref[dest * slots + slot]
        block = blocks_ref[jnp.minimum(owner, NBLK - 1)]
        return jnp.where(owner < NBLK, block, jnp.zeros_like(block))

    def total_of(dest, extras, keep_block, keep_vec):
        def one(slot, carry):
            value = block_of(dest, slot).astype(jnp.float32)
            span = pl.ds(pl.multiple_of(slot * BLK, BLK), BLK)
            for ref, lead in extras:
                value = value + ref[lead + (span,)].astype(jnp.float32)
            keep_block(slot, span, value)
            return carry

        lax.fori_loop(0, slots, one, 0)
        value = vec_ref[dest].astype(jnp.float32)
        for ref, lead in extras:
            value = value + ref[lead + (pl.ds(rows, VEC_ROWS),)].astype(jnp.float32)
        keep_vec(value)

    def into_term(dest, extras):
        def keep_block(slot, span, value):
            term[dest, span] = value.astype(jnp.bfloat16)

        def keep_vec(value):
            term[dest, pl.ds(rows, VEC_ROWS)] = value.astype(jnp.bfloat16)

        total_of(dest, extras, keep_block, keep_vec)

    def remote(dest, got, send, recv, hop, index, target):
        return pltpu.make_async_remote_copy(
            src_ref=term.at[dest],
            dst_ref=got.at[hop, index],
            send_sem=send.at[hop, index],
            recv_sem=recv.at[hop, index],
            device_id=device(dims, target),
            device_id_type=MESH,
        )

    def each(axis, count, coords_of, extras_of, got, send, recv):
        for step in range(1, dims[axis]):
            target = moved(dims, me, axis, step)

            def one(index, carry, step=step, target=target):
                coords = list(coords_of(index))
                coords[axis] = target[axis]
                dest = flat(dims, coords)
                into_term(dest, extras_of(coords))
                remote(dest, got, send, recv, step - 1, index, target).start()
                return carry

            lax.fori_loop(0, count, one, 0)

    def wait_for(axis, got, send, recv, index):
        found = []
        for step in range(1, dims[axis]):
            remote(0, got, send, recv, step - 1, index, moved(dims, me, axis, step)).wait_recv()
            found.append((got, (step - 1, index)))
        return found

    def index_c(coords):
        away = lax.rem(coords[1] - me[1] + size_x, size_x)
        order = lax.rem(away + size_x - 1, size_x)
        return (order * size_z + coords[0]) * size_y + coords[2]

    def coords_c(index):
        order = lax.div(index, size_z * size_y)
        rest = lax.rem(index, size_z * size_y)
        x = lax.rem(me[1] + 1 + order, size_x)
        return (lax.div(rest, size_y), x, lax.rem(rest, size_y), me[3])

    def coords_x(index):
        return (lax.div(index, size_y), me[1], lax.rem(index, size_y), me[3])

    def coords_y(index):
        return (index, me[1], me[2], me[3])

    def coords_z(index):
        return me

    def extras_c(coords):
        return []

    def extras_x(coords):
        return wait_for(3, got_c, send_c, recv_c, index_c(coords))

    def extras_y(coords):
        return extras_x(coords) + wait_for(
            1, got_x, send_x, recv_x, coords[0] * size_y + coords[2]
        )

    def extras_z(coords):
        return extras_y(coords) + wait_for(2, got_y, send_y, recv_y, coords[0])

    each(3, size_z * size_x * size_y, coords_c, extras_c, got_c, send_c, recv_c)
    each(1, size_z * size_y, coords_x, extras_x, got_x, send_x, recv_x)
    each(2, size_z, coords_y, extras_y, got_y, send_y, recv_y)
    each(0, 1, coords_z, extras_z, got_z, send_z, recv_z)
    extras = extras_z(me) + wait_for(0, got_z, send_z, recv_z, 0)

    def keep_block(slot, span, value):
        grad_ref[slot] = value

    def keep_vec(value):
        vec_out_ref[...] = value

    total_of(flat(dims, me), extras, keep_block, keep_vec)

    def drain(axis, count, got, send, recv):
        for step in range(1, dims[axis]):

            def one(index, carry, step=step):
                remote(
                    0, got, send, recv, step - 1, index, moved(dims, me, axis, step)
                ).wait_send()
                return carry

            lax.fori_loop(0, count, one, 0)

    drain(3, size_z * size_x * size_y, got_c, send_c, recv_c)
    drain(1, size_z * size_y, got_x, send_x, recv_x)
    drain(2, size_z, got_y, send_y, recv_y)
    drain(0, 1, got_z, send_z, recv_z)


def scatter_sums(dims, owner_slot, blocks, vec_terms):
    size_z, size_x, size_y, size_c = dims
    total = size_z * size_x * size_y * size_c
    slots = owner_slot.shape[0] // total
    chunk = (slots * BLK + VEC_ROWS, BLK)
    shapes = [
        (max(size_c - 1, 1), size_z * size_x * size_y),
        (max(size_x - 1, 1), size_z * size_y),
        (max(size_y - 1, 1), size_z),
        (max(size_z - 1, 1), 1),
    ]
    whole = pl.BlockSpec(memory_space=pltpu.VMEM)
    return pl.pallas_call(
        functools.partial(scatter_kernel, dims, slots),
        out_shape=(
            jax.ShapeDtypeStruct((slots, BLK, BLK), jnp.float32),
            jax.ShapeDtypeStruct((VEC_ROWS, BLK), jnp.float32),
        ),
        in_specs=[pl.BlockSpec(memory_space=pltpu.SMEM), whole, whole],
        out_specs=(whole, whole),
        scratch_shapes=[pltpu.VMEM((total,) + chunk, jnp.bfloat16)]
        + [pltpu.VMEM(shape + chunk, jnp.bfloat16) for shape in shapes]
        + [pltpu.SemaphoreType.DMA(shape) for shape in shapes]
        + [pltpu.SemaphoreType.DMA(shape) for shape in shapes],
        compiler_params=pltpu.CompilerParams(
            collective_id=1, has_side_effects=True, vmem_limit_bytes=60 * 1024 * 1024
        ),
        name="scatter_sums",
    )(owner_slot, blocks, vec_terms)


def three_parts(values):
    high = lax.reduce_precision(values, 8, 7)
    rest = values - high
    middle = lax.reduce_precision(rest, 8, 7)
    low = lax.reduce_precision(rest - middle, 8, 7)
    return [part.astype(jnp.bfloat16) for part in (high, middle, low)]


def as_rows(vector, rows):
    return jnp.pad(vector, (0, rows * BLK - vector.shape[0])).reshape(rows, BLK)


def ceil_to(value, unit):
    return -(-value // unit) * unit


def to_tokens(array, head_size, number, parts=1):
    seq_local, length, columns = array.shape
    tokens = length // head_size
    array = array.reshape(seq_local, head_size, tokens, columns).transpose(1, 0, 2, 3)
    got = exchange(array, number).reshape(head_size, seq_local * tokens, parts, columns // parts)
    return got.transpose(1, 2, 0, 3).reshape(seq_local * tokens, head_size * columns)


def to_heads(rows, seq_local, head_size, number):
    columns = rows.shape[1] // head_size
    array = rows.reshape(seq_local, rows.shape[0] // seq_local, head_size, columns)
    got = exchange(array.transpose(2, 0, 1, 3), number)
    return got.transpose(1, 0, 2, 3).reshape(seq_local, -1, columns)


def body(
    inputs,
    cotangent,
    span_offset,
    span_len,
    owner_slot,
    master,
    moment_one,
    moment_two,
    basis_left,
    basis_right,
    average,
    vec_master,
    vec_moment_one,
    vec_moment_two,
):
    both = ("seq", "head")
    seq_size = lax.axis_size("seq")
    head_size = lax.axis_size("head")
    total = seq_size * head_size
    head_index = lax.axis_index("head")
    seq_local, tok_local, width = inputs.shape
    slots_local = master.shape[0]
    slot_total = slots_local * total
    vec_local = vec_master.shape[0]

    dims = cut(seq_size, head_size)

    packed = jnp.concatenate(
        [
            master.astype(jnp.bfloat16).reshape(slots_local * BLK, BLK),
            as_rows(jnp.concatenate(three_parts(vec_master)), VEC_ROWS),
        ],
        0,
    )
    inputs_full, gathered = gather_all(dims, inputs, packed)
    all_slots = gathered[:, : slots_local * BLK].reshape(slot_total, BLK, BLK)
    parts = (
        gathered[:, slots_local * BLK :]
        .reshape(total, VEC_ROWS * BLK)[:, : 3 * vec_local]
        .reshape(total, 3, vec_local)
        .astype(jnp.float32)
    )
    all_vector = ((parts[:, 2] + parts[:, 1]) + parts[:, 0]).reshape(-1)

    inverse = (
        jnp.zeros((slot_total,), jnp.int32)
        .at[owner_slot]
        .set(jnp.arange(slot_total, dtype=jnp.int32))
    )
    w_query, w_key, w_value, w_out, w_up, w_down = split_matrices(all_slots[inverse[:NBLK]])
    b_query, b_value, b_out, gain_one, shift_one, b_up, b_down, gain_two, shift_two = split_vector(
        all_vector
    )
    token_rows = inputs.reshape(seq_local * tok_local, width)
    local_shape = (seq_local, tok_local, width)
    length_full = head_size * tok_local
    full_rows = inputs_full.reshape(seq_local * length_full, width)
    cols = width // head_size
    begin = head_index * cols

    def own(array):
        return lax.dynamic_slice_in_dim(array, begin, cols, array.ndim - 1)

    w_own = jnp.concatenate([own(w_query), own(w_key), own(w_value)], 1)
    b_own = jnp.concatenate([own(b_query), jnp.zeros((cols,), jnp.float32), own(b_value)], 0)
    qkv = (jnp.dot(full_rows, w_own, preferred_element_type=jnp.float32) + b_own).astype(
        jnp.bfloat16
    )
    head_local = cols // HD
    scale = 1.0 / math.sqrt(HD)
    split_shape = (seq_local, length_full, head_local, HD)
    q_split = qkv[:, :cols].reshape(split_shape)
    k_split = qkv[:, cols : 2 * cols].reshape(split_shape)
    v_split = qkv[:, 2 * cols :].reshape(split_shape)

    def forward_item(items):
        return attend_forward(items[0], items[1], items[2], scale)

    context, log_total = lax.map(forward_item, (q_split, k_split, v_split))
    context_rows = to_tokens(context.reshape(seq_local, length_full, cols), head_size, 2)
    branch = jnp.dot(context_rows, w_out, preferred_element_type=jnp.float32) + b_out
    z_one = token_rows.astype(jnp.float32) + branch
    first = layer_norm(z_one, gain_one, shift_one)
    first_low = first.astype(jnp.bfloat16)
    hidden_in = jnp.dot(first_low, w_up, preferred_element_type=jnp.float32) + b_up
    hidden_act = gelu_value(hidden_in).astype(jnp.bfloat16)
    ffn_out = jnp.dot(hidden_act, w_down, preferred_element_type=jnp.float32) + b_down
    z_two = first + ffn_out
    result, pull_two = jax.vjp(layer_norm, z_two, gain_two, shift_two)
    layer_out = result.astype(jnp.bfloat16).reshape(local_shape)
    mask = span_mask(span_offset, span_len)
    grad_out = (cotangent.astype(jnp.float32) * mask[:, :, None]).reshape(
        seq_local * tok_local, width
    )
    d_ztwo, d_gain_two, d_shift_two = pull_two(grad_out)
    d_ffn = d_ztwo.astype(jnp.bfloat16)
    grad_down = weight_grad(hidden_act, d_ffn)
    grad_bdown = jnp.sum(d_ffn.astype(jnp.float32), axis=0)
    d_hidden = back_product(d_ffn, w_down)
    d_hidden_in = (d_hidden * gelu_slope(hidden_in)).astype(jnp.bfloat16)
    grad_up = weight_grad(first_low, d_hidden_in)
    grad_bup = jnp.sum(d_hidden_in.astype(jnp.float32), axis=0)
    d_first = d_ztwo + back_product(d_hidden_in, w_up)
    sink, pull_one = jax.vjp(layer_norm, z_one, gain_one, shift_one)
    d_zone, d_gain_one, d_shift_one = pull_one(d_first)
    d_branch = d_zone.astype(jnp.bfloat16)
    grad_out_w = weight_grad(context_rows, d_branch)
    grad_bout = jnp.sum(d_branch.astype(jnp.float32), axis=0)

    d_context = back_product(d_branch, w_out).astype(jnp.bfloat16)
    d_context_split = to_heads(d_context, seq_local, head_size, 3).reshape(split_shape)

    def backward_item(items):
        return attend_backward(items[0], items[1], items[2], items[3], items[4], scale)

    d_query, d_keys, d_values = lax.map(
        backward_item, (q_split, k_split, v_split, d_context_split, log_total)
    )
    joined = (seq_local, length_full, cols)
    d_all = jnp.concatenate(
        [d_query.reshape(joined), d_keys.reshape(joined), d_values.reshape(joined)], 2
    )
    d_all_rows = d_all.reshape(seq_local * length_full, 3 * cols)
    grad_own = weight_grad(full_rows, d_all_rows)
    grad_b_own = jnp.sum(d_all_rows.astype(jnp.float32), axis=0)
    d_local = to_tokens(d_all, head_size, 4, 3)
    w_all = jnp.concatenate([w_query, w_key, w_value], 1)
    input_grad = (d_zone + back_product(d_local, w_all)).reshape(local_shape)

    def put(array):
        empty = jnp.zeros(array.shape[:-1] + (width,), array.dtype)
        return lax.dynamic_update_slice_in_dim(empty, array, begin, array.ndim - 1)

    matrices = [put(grad_own[:, n * cols : (n + 1) * cols]) for n in range(3)]
    blocks = join_matrices(
        [matrix.astype(jnp.bfloat16) for matrix in matrices + [grad_out_w, grad_up, grad_down]]
    )
    vector_terms = jnp.concatenate(
        [
            put(grad_b_own[:cols]),
            put(grad_b_own[2 * cols :]),
            grad_bout,
            d_gain_one,
            d_shift_one,
            grad_bup,
            grad_bdown,
            d_gain_two,
            d_shift_two,
        ],
        0,
    ).reshape(total, vec_local)
    vec_terms = jnp.pad(vector_terms, ((0, 0), (0, VEC_ROWS * BLK - vec_local)))
    vec_terms = vec_terms.astype(jnp.bfloat16).reshape(total, VEC_ROWS, BLK)
    slot_grad, vec_sums = scatter_sums(dims, owner_slot, blocks, vec_terms)
    vec_grad = vec_sums.reshape(-1)[:vec_local]
    first_moment, second_moment, updated = rotate_adam(
        slot_grad, master, moment_one, moment_two, basis_left, basis_right
    )
    correct = 1.0 - 0.5**STEP
    vec_first = 0.5 * vec_moment_one + 0.5 * vec_grad
    vec_second = 0.5 * vec_moment_two + 0.5 * vec_grad * vec_grad
    vec_new = vec_master - VEC_RATE * (vec_first / correct) / (
        jnp.sqrt(vec_second / correct) + ADAM_EPS
    )
    new_average = KEEP * average + (1.0 - KEEP) * updated
    return (
        layer_out,
        input_grad,
        slot_grad,
        vec_grad,
        first_moment,
        second_moment,
        updated,
        updated.astype(jnp.bfloat16),
        new_average,
        vec_first,
        vec_second,
        vec_new,
    )


def solution(mesh):
    placed = (
        P("seq", "head", None),
        P("seq", "head", None),
        P("seq", "head"),
        P("seq", "head"),
        P(),
        P(("seq", "head"), None, None),
        P(("seq", "head"), None, None),
        P(("seq", "head"), None, None),
        P(("seq", "head"), None, None),
        P(("seq", "head"), None, None),
        P(("seq", "head"), None, None),
        P(("seq", "head")),
        P(("seq", "head")),
        P(("seq", "head")),
    )
    return jax.shard_map(
        body,
        mesh=mesh,
        in_specs=placed,
        out_specs=(
            P("seq", "head", None),
            P("seq", "head", None),
            P(("seq", "head"), None, None),
            P(("seq", "head")),
            P(("seq", "head"), None, None),
            P(("seq", "head"), None, None),
            P(("seq", "head"), None, None),
            P(("seq", "head"), None, None),
            P(("seq", "head"), None, None),
            P(("seq", "head")),
            P(("seq", "head")),
            P(("seq", "head")),
        ),
        check_vma=False,
    )
```

```python
import functools
import math

import jax
import jax.numpy as jnp
from jax import lax
from jax.experimental import pallas as pl
from jax.experimental.pallas import tpu as pltpu
from jax.sharding import PartitionSpec as P

D = 512
FF = 2048
WIN = 16
BLK = 128
STEP = 5
HD = 64
NBLK = 192
QUERIES = 256
SCALE = 1.0 / math.sqrt(HD)


NORM_EPS = 1e-06
ADAM_EPS = 1e-08
RATE = 0.05
VEC_RATE = 0.2
DECAY = 0.01
KEEP = 0.9
HIGH = lax.Precision.HIGHEST


def join_matrices(matrices):
    pieces = []
    for matrix in matrices:
        row_count = matrix.shape[0] // BLK
        col_count = matrix.shape[1] // BLK
        pieces.append(
            matrix.reshape(row_count, BLK, col_count, BLK)
            .transpose(0, 2, 1, 3)
            .reshape(row_count * col_count, BLK, BLK)
        )
    return jnp.concatenate(pieces, 0)


def split_vector(vector):
    widths = [D, D, D, D, D, FF, D, D, D]
    pieces = []
    offset = 0
    for extent in widths:
        pieces.append(vector[offset : offset + extent])
        offset = offset + extent
    return pieces


def layer_norm(values, gain, shift):
    center = values - jnp.mean(values, axis=-1, keepdims=True)
    spread = jnp.mean(center * center, axis=-1, keepdims=True)
    return center * lax.rsqrt(spread + NORM_EPS) * gain + shift


def gelu_value(values):
    return 0.5 * values * (1.0 + lax.erf(values * 0.7071067811865476))


def gelu_slope(values):
    return (
        0.5 * (1.0 + lax.erf(values * 0.7071067811865476))
        + values * jnp.exp(-0.5 * values * values) * 0.3989422804014327
    )


def span_mask(span_offset, span_len):
    offsets = jnp.repeat(span_offset, WIN, axis=1)
    extents = jnp.repeat(span_len, WIN, axis=1)
    within = (jnp.arange(offsets.shape[1], dtype=jnp.int32) % WIN)[None, :]
    return ((within >= offsets) & (within < offsets + extents)).astype(jnp.float32)


def contract(left, right, left_axis, right_axis):
    return lax.dot_general(
        left, right, (((left_axis,), (right_axis,)), ((), ())), preferred_element_type=jnp.float32
    )


def forward_kernel(x_ref, w_ref, b_ref, qkv_ref, ctx_ref, lse_ref):
    head_size, tokens, width = x_ref.shape[0], x_ref.shape[1], x_ref.shape[2]
    length = head_size * tokens
    cols = w_ref.shape[1] // 3
    rows = x_ref[...].reshape(length, width)
    qkv_ref[...] = (contract(rows, w_ref[...], 1, 0) + b_ref[...]).astype(jnp.bfloat16)
    step = min(QUERIES, tokens)
    for number in range(cols // HD):
        low = number * HD
        keys = qkv_ref[:, cols + low : cols + low + HD]
        values = qkv_ref[:, 2 * cols + low : 2 * cols + low + HD]
        for begin in range(0, length, step):
            query = qkv_ref[begin : begin + step, low : low + HD] * jnp.bfloat16(SCALE)
            scores = contract(keys, query, 1, 1)
            highest = jnp.max(scores, axis=0, keepdims=True)
            weights = jnp.exp(scores - highest)
            summed = jnp.sum(weights, axis=0, keepdims=True)
            probs = (weights * (1.0 / summed)).astype(jnp.bfloat16)
            context = contract(values, probs, 0, 0).T.astype(jnp.bfloat16)
            ctx_ref[begin // tokens, pl.ds(begin % tokens, step), low : low + HD] = context
            lse_ref[number : number + 1, begin : begin + step] = highest + jnp.log(summed)


def attend(inputs_full, weights, bias):
    seq_local, head_size, tokens, width = inputs_full.shape
    length = head_size * tokens
    cols = weights.shape[1] // 3
    return pl.pallas_call(
        forward_kernel,
        grid=(seq_local,),
        out_shape=(
            jax.ShapeDtypeStruct((seq_local, length, 3 * cols), jnp.bfloat16),
            jax.ShapeDtypeStruct((head_size, seq_local, tokens, cols), jnp.bfloat16),
            jax.ShapeDtypeStruct((seq_local, 8, length), jnp.float32),
        ),
        in_specs=[
            pl.BlockSpec((None, head_size, tokens, width), lambda s: (s, 0, 0, 0)),
            pl.BlockSpec((width, 3 * cols), lambda s: (0, 0)),
            pl.BlockSpec((1, 3 * cols), lambda s: (0, 0)),
        ],
        out_specs=(
            pl.BlockSpec((None, length, 3 * cols), lambda s: (s, 0, 0)),
            pl.BlockSpec((head_size, None, tokens, cols), lambda s: (0, s, 0, 0)),
            pl.BlockSpec((None, 8, length), lambda s: (s, 0, 0)),
        ),
        compiler_params=pltpu.CompilerParams(vmem_limit_bytes=48 * 1024 * 1024),
        name="attend",
    )(inputs_full, weights, bias)


def backward_kernel(x_ref, qkv_ref, lse_ref, dctx_ref, grad_ref, dw_ref, db_ref, dall, acc):
    head_size, tokens, width = x_ref.shape[0], x_ref.shape[1], x_ref.shape[2]
    length = head_size * tokens
    cols = qkv_ref.shape[1] // 3
    step = min(QUERIES, tokens)
    scale = jnp.bfloat16(SCALE)
    for number in range(cols // HD):
        low = number * HD
        keys = qkv_ref[:, cols + low : cols + low + HD]
        values = qkv_ref[:, 2 * cols + low : 2 * cols + low + HD]
        for begin in range(0, length, step):
            query = qkv_ref[begin : begin + step, low : low + HD] * scale
            dctx = dctx_ref[begin // tokens, pl.ds(begin % tokens, step), low : low + HD]
            scores = contract(keys, query, 1, 1)
            probs = jnp.exp(scores - lse_ref[number : number + 1, begin : begin + step])
            dprobs = contract(values, dctx, 1, 1)
            inner = jnp.sum(probs * dprobs, axis=0, keepdims=True)
            dscores = (probs * (dprobs - inner)).astype(jnp.bfloat16)
            dkey = contract(dscores, query, 1, 0)
            dvalue = contract(probs.astype(jnp.bfloat16), dctx, 1, 0)
            if begin == 0:
                acc[0] = dkey
                acc[1] = dvalue
            else:
                acc[0] += dkey
                acc[1] += dvalue
            dquery = contract(keys, dscores, 0, 0).T * SCALE
            dall[begin : begin + step, low : low + HD] = dquery.astype(jnp.bfloat16)
        dall[:, cols + low : cols + low + HD] = acc[0].astype(jnp.bfloat16)
        dall[:, 2 * cols + low : 2 * cols + low + HD] = acc[1].astype(jnp.bfloat16)
    rows = x_ref[...].reshape(length, width)
    delta = dall[...]
    grad_ref[...] = delta.reshape(head_size, tokens, 3 * cols)
    dw = contract(rows, delta, 0, 0)
    db = jnp.sum(delta.astype(jnp.float32), axis=0, keepdims=True)

    @pl.when(pl.program_id(0) == 0)
    def _():
        dw_ref[...] = dw
        db_ref[...] = db

    @pl.when(pl.program_id(0) > 0)
    def _():
        dw_ref[...] += dw
        db_ref[...] += db


def attend_back(inputs_full, qkv, lse, dctx):
    seq_local, head_size, tokens, width = inputs_full.shape
    length = head_size * tokens
    cols = qkv.shape[2] // 3
    return pl.pallas_call(
        backward_kernel,
        grid=(seq_local,),
        out_shape=(
            jax.ShapeDtypeStruct((head_size, seq_local, tokens, 3 * cols), jnp.bfloat16),
            jax.ShapeDtypeStruct((width, 3 * cols), jnp.float32),
            jax.ShapeDtypeStruct((1, 3 * cols), jnp.float32),
        ),
        in_specs=[
            pl.BlockSpec((None, head_size, tokens, width), lambda s: (s, 0, 0, 0)),
            pl.BlockSpec((None, length, 3 * cols), lambda s: (s, 0, 0)),
            pl.BlockSpec((None, 8, length), lambda s: (s, 0, 0)),
            pl.BlockSpec((head_size, None, tokens, cols), lambda s: (0, s, 0, 0)),
        ],
        out_specs=(
            pl.BlockSpec((head_size, None, tokens, 3 * cols), lambda s: (0, s, 0, 0)),
            pl.BlockSpec((width, 3 * cols), lambda s: (0, 0)),
            pl.BlockSpec((1, 3 * cols), lambda s: (0, 0)),
        ),
        scratch_shapes=[
            pltpu.VMEM((length, 3 * cols), jnp.bfloat16),
            pltpu.VMEM((2, length, HD), jnp.float32),
        ],
        compiler_params=pltpu.CompilerParams(vmem_limit_bytes=48 * 1024 * 1024),
        name="attend_back",
    )(inputs_full, qkv, lse, dctx)


def input_grad_kernel(dz_ref, d_ref, w_ref, out_ref):
    total = dz_ref[...]
    for number in range(d_ref.shape[0]):
        total = total + contract(d_ref[number], w_ref[number], 1, 1)
    out_ref[...] = total


def input_grads(d_zone, deltas, weights):
    head_size, seq_local, tokens, columns = deltas.shape
    width = d_zone.shape[1]
    return pl.pallas_call(
        input_grad_kernel,
        grid=(seq_local,),
        out_shape=jax.ShapeDtypeStruct((seq_local, tokens, width), jnp.float32),
        in_specs=[
            pl.BlockSpec((tokens, width), lambda s: (s, 0)),
            pl.BlockSpec((head_size, None, tokens, columns), lambda s: (0, s, 0, 0)),
            pl.BlockSpec((head_size, width, columns), lambda s: (0, 0, 0)),
        ],
        out_specs=pl.BlockSpec((None, tokens, width), lambda s: (s, 0, 0)),
        name="input_grads",
    )(d_zone, deltas, weights)


def rotate_adam(grads, master, moment_one, moment_two, basis_left, basis_right):
    rotated = jnp.einsum("sji,sjk->sik", basis_left, grads, precision=HIGH)
    rotated = jnp.einsum("sik,skl->sil", rotated, basis_right, precision=HIGH)
    first = 0.5 * moment_one + 0.5 * rotated
    second = 0.5 * moment_two + 0.5 * rotated * rotated
    correct = 1.0 - 0.5**STEP
    normed = first / correct / (jnp.sqrt(second / correct) + ADAM_EPS)
    turned = jnp.einsum("sij,sjk->sik", basis_left, normed, precision=HIGH)
    turned = jnp.einsum("sik,slk->sil", turned, basis_right, precision=HIGH)
    updated = master - RATE * (turned + DECAY * master)
    return (first, second, updated)


def weight_grad(left, right):
    return jnp.einsum("ti,to->io", left, right, preferred_element_type=jnp.float32)


def back_product(grads, weight):
    return jnp.einsum("to,io->ti", grads, weight, preferred_element_type=jnp.float32)


MESH = pl.DeviceIdType.MESH
VEC_ROWS = 16
PIECE = 16


def cut(seq_size, head_size):
    cores = 2 if head_size % 2 == 0 else 1
    rows = 1
    while 2 * (rows * 2) ** 2 <= seq_size and seq_size % (rows * 2) == 0:
        rows = rows * 2
    return (seq_size // rows, rows, head_size // cores, cores)


def place(dims):
    size_z, size_x, size_y, size_c = dims
    seq = lax.axis_index("seq")
    head = lax.axis_index("head")
    return (
        lax.div(seq, size_x),
        lax.rem(seq, size_x),
        lax.div(head, size_c),
        lax.rem(head, size_c),
    )


def device(dims, coords):
    return (coords[0] * dims[1] + coords[1], coords[2] * dims[3] + coords[3])


def flat(dims, coords):
    return ((coords[0] * dims[1] + coords[1]) * dims[2] + coords[2]) * dims[3] + coords[3]


def moved(dims, coords, axis, step):
    new = list(coords)
    new[axis] = lax.rem(coords[axis] + step, dims[axis])
    return tuple(new)


def greet(dims, coords):
    barrier = pltpu.get_barrier_semaphore()
    count = 0
    for axis in range(4):
        for step in range(1, dims[axis]):
            pl.semaphore_signal(
                barrier,
                inc=1,
                device_id=device(dims, moved(dims, coords, axis, step)),
                device_id_type=MESH,
            )
            count = count + 1
    pl.semaphore_wait(barrier, count)


def greet_head(head_size):
    barrier = pltpu.get_barrier_semaphore()
    seq = lax.axis_index("seq")
    head = lax.axis_index("head")
    for step in range(1, head_size):
        pl.semaphore_signal(
            barrier, inc=1, device_id=(seq, lax.rem(head + step, head_size)), device_id_type=MESH
        )
    pl.semaphore_wait(barrier, head_size - 1)


def gather_kernel(
    dims,
    inv_ref,
    x_ref,
    w_ref,
    xf_ref,
    qkv_ref,
    out_ref,
    up_ref,
    down_ref,
    vec_ref,
    wf_ref,
    own_sem,
    x_send,
    x_recv,
    w_send,
    w_recv,
):
    me = place(dims)
    size_z, size_x, size_y, size_c = dims
    head_me = me[2] * size_c + me[3]
    chunk = w_ref.shape[0]

    def spot(index):
        return wf_ref.at[pl.ds(index * chunk, chunk)]

    own_x = pltpu.make_async_copy(x_ref, xf_ref.at[:, head_me], own_sem.at[0])
    own_w = pltpu.make_async_copy(w_ref, spot(flat(dims, me)), own_sem.at[1])
    own_x.start()
    own_w.start()
    greet(dims, me)
    started = []

    def send_x(source, head, target, number):
        copy = pltpu.make_async_remote_copy(
            src_ref=source,
            dst_ref=xf_ref.at[:, head],
            send_sem=x_send.at[number],
            recv_sem=x_recv.at[head],
            device_id=device(dims, target),
            device_id_type=MESH,
        )
        copy.start()
        started.append(copy)

    def arrived_x(head):
        pltpu.make_async_remote_copy(
            src_ref=x_ref,
            dst_ref=xf_ref.at[:, head],
            send_sem=x_send.at[0],
            recv_sem=x_recv.at[head],
            device_id=device(dims, me),
            device_id_type=MESH,
        ).wait_recv()

    count = [0]

    def send_w(source, index, target):
        number = count[0]
        count[0] = number + 1
        copy = pltpu.make_async_remote_copy(
            src_ref=source,
            dst_ref=spot(index),
            send_sem=w_send.at[number],
            recv_sem=w_recv.at[index],
            device_id=device(dims, target),
            device_id_type=MESH,
        )
        copy.start()
        started.append(copy)

    def arrived_w(index):
        pltpu.make_async_remote_copy(
            src_ref=w_ref,
            dst_ref=spot(index),
            send_sem=w_send.at[0],
            recv_sem=w_recv.at[index],
            device_id=device(dims, me),
            device_id_type=MESH,
        ).wait_recv()

    order = [0, 2, 1, 3]

    def forward(source, coords, after):
        for axis in order[after:]:
            for step in range(1, dims[axis]):
                send_w(source, flat(dims, coords), moved(dims, me, axis, step))

    number = 0
    for step in range(1, size_y):
        send_x(x_ref, head_me, moved(dims, me, 2, step), number)
        number = number + 1
    for step in range(1, size_c):
        send_x(x_ref, head_me, moved(dims, me, 3, step), number)
        number = number + 1
    forward(w_ref, me, 0)
    held = [me]
    for level in range(3):
        axis = order[level]
        fresh = []
        for step in range(1, dims[axis]):
            for coords in held:
                source = moved(dims, coords, axis, step)
                arrived_w(flat(dims, source))
                forward(spot(flat(dims, source)), source, level + 1)
                fresh.append(source)
        held = held + fresh
        if level == 1:
            for step in range(1, size_y):
                other = moved(dims, me, 2, step)
                head = other[2] * size_c + other[3]
                arrived_x(head)
                for hop in range(1, size_c):
                    send_x(xf_ref.at[:, head], head, moved(dims, me, 3, hop), number)
                    number = number + 1
    for step in range(1, size_c):
        for coords in held:
            arrived_w(flat(dims, moved(dims, coords, 3, step)))
        for across in range(size_y):
            other = moved(dims, moved(dims, me, 3, step), 2, across)
            arrived_x(other[2] * size_c + other[3])
    for copy in started:
        copy.wait_send()
    own_x.wait()
    own_w.wait()
    unpack(dims, inv_ref, wf_ref, qkv_ref, out_ref, up_ref, down_ref)
    chunk = w_ref.shape[0]
    for number in range(vec_ref.shape[0]):
        vec_ref[number] = wf_ref[(number + 1) * chunk - 1]


def unpack(dims, inv_ref, wf_ref, qkv_ref, out_ref, up_ref, down_ref):
    head_size = dims[2] * dims[3]
    width = out_ref.shape[0]
    hidden = up_ref.shape[1]
    cols = width // head_size
    across = width // BLK

    def block(number):
        piece = inv_ref[number]
        return jnp.concatenate([wf_ref[piece + part] for part in range(BLK // PIECE)], 0)

    def rows_of(row_count, first, col_count, store):
        def one(row, carry):
            span = pl.ds(pl.multiple_of(row * BLK, BLK), BLK)
            for col in range(col_count):
                store(span, col, block(first + row * col_count + col))
            return carry

        lax.fori_loop(0, row_count, one, 0)

    for number in range(3):

        def store_qkv(span, col, value, number=number):
            for begin in range(0, BLK, min(cols, BLK)):
                head = (col * BLK + begin) // cols
                lane = (col * BLK + begin) % cols
                part = min(cols, BLK)
                qkv_ref[head, span, number * cols + lane : number * cols + lane + part] = value[
                    :, begin : begin + part
                ]

        rows_of(across, number * across * across, across, store_qkv)

    def store_in(ref):
        def store(span, col, value):
            ref[span, col * BLK : (col + 1) * BLK] = value

        return store

    rows_of(across, 3 * across * across, across, store_in(out_ref))
    first = 4 * across * across
    rows_of(across, first, hidden // BLK, store_in(up_ref))
    first = first + across * (hidden // BLK)
    rows_of(hidden // BLK, first, across, store_in(down_ref))


def gather_all(dims, inverse, inputs, packed):
    size_z, size_x, size_y, size_c = dims
    total = size_z * size_x * size_y * size_c
    head_size = size_y * size_c
    seq_local, tok_local, width = inputs.shape
    any_space = pl.BlockSpec(memory_space=pl.ANY)
    whole = pl.BlockSpec(memory_space=pltpu.VMEM)
    sends_x = (size_y - 1) * size_c + size_c - 1
    sends_w = (
        (size_z - 1)
        + size_z * (size_y - 1)
        + size_z * size_y * (size_x - 1)
        + size_z * size_y * size_x * (size_c - 1)
    )
    return pl.pallas_call(
        functools.partial(gather_kernel, dims),
        out_shape=(
            jax.ShapeDtypeStruct((seq_local, head_size, tok_local, width), inputs.dtype),
            jax.ShapeDtypeStruct((head_size, width, 3 * width // head_size), packed.dtype),
            jax.ShapeDtypeStruct((width, width), packed.dtype),
            jax.ShapeDtypeStruct((width, FF), packed.dtype),
            jax.ShapeDtypeStruct((FF, width), packed.dtype),
            jax.ShapeDtypeStruct((total, VEC_ROWS, BLK), packed.dtype),
        ),
        in_specs=[pl.BlockSpec(memory_space=pltpu.SMEM), whole, whole],
        out_specs=(any_space, whole, whole, whole, whole, whole),
        scratch_shapes=[
            pltpu.VMEM((total * packed.shape[0],) + packed.shape[1:], packed.dtype),
            pltpu.SemaphoreType.DMA((2,)),
            pltpu.SemaphoreType.DMA((max(sends_x, 1),)),
            pltpu.SemaphoreType.DMA((head_size,)),
            pltpu.SemaphoreType.DMA((max(sends_w, 1),)),
            pltpu.SemaphoreType.DMA((total,)),
        ],
        compiler_params=pltpu.CompilerParams(
            collective_id=0, has_side_effects=True, vmem_limit_bytes=40 * 1024 * 1024
        ),
        name="gather_all",
    )(inverse, inputs, packed)


def exchange_kernel(head_size, src_ref, dst_ref, own_sem, send_sem, recv_sem):
    seq = lax.axis_index("seq")
    head = lax.axis_index("head")
    own = pltpu.make_async_copy(src_ref.at[head], dst_ref.at[head], own_sem)
    own.start()
    greet_head(head_size)
    copies = []
    for step in [2, 1, 3] if head_size == 4 else range(1, head_size):
        peer = lax.rem(head + step, head_size)
        copy = pltpu.make_async_remote_copy(
            src_ref=src_ref.at[peer],
            dst_ref=dst_ref.at[head],
            send_sem=send_sem.at[step],
            recv_sem=recv_sem.at[step],
            device_id=(seq, peer),
            device_id_type=MESH,
        )
        copy.start()
        copies.append(copy)
    for copy in copies:
        copy.wait()
    own.wait()


def exchange(array, number):
    head_size = array.shape[0]
    if head_size == 1:
        return array
    whole = pl.BlockSpec(memory_space=pltpu.VMEM)
    return pl.pallas_call(
        functools.partial(exchange_kernel, head_size),
        out_shape=jax.ShapeDtypeStruct(array.shape, array.dtype),
        in_specs=[whole],
        out_specs=whole,
        scratch_shapes=[
            pltpu.SemaphoreType.DMA,
            pltpu.SemaphoreType.DMA((head_size,)),
            pltpu.SemaphoreType.DMA((head_size,)),
        ],
        compiler_params=pltpu.CompilerParams(collective_id=number, has_side_effects=True),
        name="exchange",
    )(array)


def scatter_kernel(
    dims,
    slots,
    owner_ref,
    blocks_ref,
    vec_ref,
    grad_ref,
    vec_out_ref,
    term,
    got_c,
    got_x,
    got_y,
    got_z,
    send_c,
    send_x,
    send_y,
    send_z,
    recv_c,
    recv_x,
    recv_y,
    recv_z,
):
    me = place(dims)
    size_z, size_x, size_y, size_c = dims
    rows = slots * BLK
    greet(dims, me)

    def block_of(dest, slot):
        owner = owner_ref[dest * slots + slot]
        block = blocks_ref[jnp.minimum(owner, NBLK - 1)]
        return jnp.where(owner < NBLK, block, jnp.zeros_like(block))

    def total_of(dest, extras, keep_block, keep_vec):
        def one(slot, carry):
            value = block_of(dest, slot).astype(jnp.float32)
            span = pl.ds(pl.multiple_of(slot * BLK, BLK), BLK)
            for ref, lead in extras:
                value = value + ref[lead + (span,)].astype(jnp.float32)
            keep_block(slot, span, value)
            return carry

        lax.fori_loop(0, slots, one, 0)
        value = vec_ref[dest].astype(jnp.float32)
        for ref, lead in extras:
            value = value + ref[lead + (pl.ds(rows, VEC_ROWS),)].astype(jnp.float32)
        keep_vec(value)

    def into_term(dest, extras):
        def keep_block(slot, span, value):
            term[dest, span] = value.astype(jnp.bfloat16)

        def keep_vec(value):
            term[dest, pl.ds(rows, VEC_ROWS)] = value.astype(jnp.bfloat16)

        total_of(dest, extras, keep_block, keep_vec)

    def remote(dest, got, send, recv, hop, index, target):
        return pltpu.make_async_remote_copy(
            src_ref=term.at[dest],
            dst_ref=got.at[hop, index],
            send_sem=send.at[hop, index],
            recv_sem=recv.at[hop, index],
            device_id=device(dims, target),
            device_id_type=MESH,
        )

    def each(axis, count, coords_of, extras_of, got, send, recv):
        for step in range(1, dims[axis]):
            target = moved(dims, me, axis, step)

            def one(index, carry, step=step, target=target):
                coords = list(coords_of(index))
                coords[axis] = target[axis]
                dest = flat(dims, coords)
                into_term(dest, extras_of(coords))
                remote(dest, got, send, recv, step - 1, index, target).start()
                return carry

            lax.fori_loop(0, count, one, 0)

    def wait_for(axis, got, send, recv, index):
        found = []
        for step in range(1, dims[axis]):
            remote(0, got, send, recv, step - 1, index, moved(dims, me, axis, step)).wait_recv()
            found.append((got, (step - 1, index)))
        return found

    def index_c(coords):
        away = lax.rem(coords[1] - me[1] + size_x, size_x)
        order = lax.rem(away + size_x - 1, size_x)
        return (order * size_z + coords[0]) * size_y + coords[2]

    def coords_c(index):
        order = lax.div(index, size_z * size_y)
        rest = lax.rem(index, size_z * size_y)
        x = lax.rem(me[1] + 1 + order, size_x)
        return (lax.div(rest, size_y), x, lax.rem(rest, size_y), me[3])

    def coords_x(index):
        return (lax.div(index, size_y), me[1], lax.rem(index, size_y), me[3])

    def coords_y(index):
        return (index, me[1], me[2], me[3])

    def coords_z(index):
        return me

    def extras_c(coords):
        return []

    def extras_x(coords):
        return wait_for(3, got_c, send_c, recv_c, index_c(coords))

    def extras_y(coords):
        return extras_x(coords) + wait_for(
            1, got_x, send_x, recv_x, coords[0] * size_y + coords[2]
        )

    def extras_z(coords):
        return extras_y(coords) + wait_for(2, got_y, send_y, recv_y, coords[0])

    each(3, size_z * size_x * size_y, coords_c, extras_c, got_c, send_c, recv_c)
    each(1, size_z * size_y, coords_x, extras_x, got_x, send_x, recv_x)
    each(2, size_z, coords_y, extras_y, got_y, send_y, recv_y)
    each(0, 1, coords_z, extras_z, got_z, send_z, recv_z)
    extras = extras_z(me) + wait_for(0, got_z, send_z, recv_z, 0)

    def keep_block(slot, span, value):
        grad_ref[slot] = value

    def keep_vec(value):
        vec_out_ref[...] = value

    total_of(flat(dims, me), extras, keep_block, keep_vec)

    def drain(axis, count, got, send, recv):
        for step in range(1, dims[axis]):

            def one(index, carry, step=step):
                remote(
                    0, got, send, recv, step - 1, index, moved(dims, me, axis, step)
                ).wait_send()
                return carry

            lax.fori_loop(0, count, one, 0)

    drain(3, size_z * size_x * size_y, got_c, send_c, recv_c)
    drain(1, size_z * size_y, got_x, send_x, recv_x)
    drain(2, size_z, got_y, send_y, recv_y)
    drain(0, 1, got_z, send_z, recv_z)


def scatter_sums(dims, owner_slot, blocks, vec_terms):
    size_z, size_x, size_y, size_c = dims
    total = size_z * size_x * size_y * size_c
    slots = owner_slot.shape[0] // total
    chunk = (slots * BLK + VEC_ROWS, BLK)
    shapes = [
        (max(size_c - 1, 1), size_z * size_x * size_y),
        (max(size_x - 1, 1), size_z * size_y),
        (max(size_y - 1, 1), size_z),
        (max(size_z - 1, 1), 1),
    ]
    whole = pl.BlockSpec(memory_space=pltpu.VMEM)
    return pl.pallas_call(
        functools.partial(scatter_kernel, dims, slots),
        out_shape=(
            jax.ShapeDtypeStruct((slots, BLK, BLK), jnp.float32),
            jax.ShapeDtypeStruct((VEC_ROWS, BLK), jnp.float32),
        ),
        in_specs=[pl.BlockSpec(memory_space=pltpu.SMEM), whole, whole],
        out_specs=(whole, whole),
        scratch_shapes=[pltpu.VMEM((total,) + chunk, jnp.bfloat16)]
        + [pltpu.VMEM(shape + chunk, jnp.bfloat16) for shape in shapes]
        + [pltpu.SemaphoreType.DMA(shape) for shape in shapes]
        + [pltpu.SemaphoreType.DMA(shape) for shape in shapes],
        compiler_params=pltpu.CompilerParams(
            collective_id=1, has_side_effects=True, vmem_limit_bytes=60 * 1024 * 1024
        ),
        name="scatter_sums",
    )(owner_slot, blocks, vec_terms)


def three_parts(values):
    high = lax.reduce_precision(values, 8, 7)
    rest = values - high
    middle = lax.reduce_precision(rest, 8, 7)
    low = lax.reduce_precision(rest - middle, 8, 7)
    return [part.astype(jnp.bfloat16) for part in (high, middle, low)]


def as_rows(vector, rows):
    return jnp.pad(vector, (0, rows * BLK - vector.shape[0])).reshape(rows, BLK)


def ceil_to(value, unit):
    return -(-value // unit) * unit


def body(
    inputs,
    cotangent,
    span_offset,
    span_len,
    owner_slot,
    master,
    moment_one,
    moment_two,
    basis_left,
    basis_right,
    average,
    vec_master,
    vec_moment_one,
    vec_moment_two,
):
    both = ("seq", "head")
    seq_size = lax.axis_size("seq")
    head_size = lax.axis_size("head")
    total = seq_size * head_size
    head_index = lax.axis_index("head")
    seq_local, tok_local, width = inputs.shape
    slots_local = master.shape[0]
    slot_total = slots_local * total
    vec_local = vec_master.shape[0]

    dims = cut(seq_size, head_size)

    packed = jnp.concatenate(
        [
            master.astype(jnp.bfloat16).reshape(slots_local * BLK, BLK),
            as_rows(jnp.concatenate(three_parts(vec_master)), VEC_ROWS),
        ],
        0,
    ).reshape(-1, PIECE, BLK)
    numbers = jnp.arange(slot_total, dtype=jnp.int32)
    inverse = jnp.sum(
        jnp.where(owner_slot[:, None] == numbers[None, :], numbers[:, None], 0), axis=0
    )
    pieces = (inverse // slots_local) * packed.shape[0]
    pieces = pieces + (inverse % slots_local) * (BLK // PIECE)
    inputs_full, w_qkv, w_out, w_up, w_down, vec_parts = gather_all(
        dims, pieces, inputs, packed
    )
    parts = (
        vec_parts
        .reshape(total, VEC_ROWS * BLK)[:, : 3 * vec_local]
        .reshape(total, 3, vec_local)
        .astype(jnp.float32)
    )
    all_vector = ((parts[:, 2] + parts[:, 1]) + parts[:, 0]).reshape(-1)

    b_query, b_value, b_out, gain_one, shift_one, b_up, b_down, gain_two, shift_two = split_vector(
        all_vector
    )
    token_rows = inputs.reshape(seq_local * tok_local, width)
    local_shape = (seq_local, tok_local, width)
    cols = width // head_size
    begin = head_index * cols

    def own(array):
        return lax.dynamic_slice_in_dim(array, begin, cols, array.ndim - 1)

    w_own = lax.dynamic_index_in_dim(w_qkv, head_index, 0, keepdims=False)
    b_own = jnp.concatenate([own(b_query), jnp.zeros((cols,), jnp.float32), own(b_value)], 0)
    qkv, context, log_total = attend(inputs_full, w_own, b_own[None, :])
    context_rows = exchange(context, 2).transpose(1, 2, 0, 3).reshape(seq_local * tok_local, width)
    branch = jnp.dot(context_rows, w_out, preferred_element_type=jnp.float32) + b_out
    z_one = token_rows.astype(jnp.float32) + branch
    first = layer_norm(z_one, gain_one, shift_one)
    first_low = first.astype(jnp.bfloat16)
    hidden_in = jnp.dot(first_low, w_up, preferred_element_type=jnp.float32) + b_up
    hidden_act = gelu_value(hidden_in).astype(jnp.bfloat16)
    ffn_out = jnp.dot(hidden_act, w_down, preferred_element_type=jnp.float32) + b_down
    z_two = first + ffn_out
    result, pull_two = jax.vjp(layer_norm, z_two, gain_two, shift_two)
    layer_out = result.astype(jnp.bfloat16).reshape(local_shape)
    mask = span_mask(span_offset, span_len)
    grad_out = (cotangent.astype(jnp.float32) * mask[:, :, None]).reshape(
        seq_local * tok_local, width
    )
    d_ztwo, d_gain_two, d_shift_two = pull_two(grad_out)
    d_ffn = d_ztwo.astype(jnp.bfloat16)
    grad_down = weight_grad(hidden_act, d_ffn)
    grad_bdown = jnp.sum(d_ffn.astype(jnp.float32), axis=0)
    d_hidden = back_product(d_ffn, w_down)
    d_hidden_in = (d_hidden * gelu_slope(hidden_in)).astype(jnp.bfloat16)
    grad_up = weight_grad(first_low, d_hidden_in)
    grad_bup = jnp.sum(d_hidden_in.astype(jnp.float32), axis=0)
    d_first = d_ztwo + back_product(d_hidden_in, w_up)
    sink, pull_one = jax.vjp(layer_norm, z_one, gain_one, shift_one)
    d_zone, d_gain_one, d_shift_one = pull_one(d_first)
    d_branch = d_zone.astype(jnp.bfloat16)
    grad_out_w = weight_grad(context_rows, d_branch)
    grad_bout = jnp.sum(d_branch.astype(jnp.float32), axis=0)

    d_context = back_product(d_branch, w_out).astype(jnp.bfloat16)
    d_context = d_context.reshape(seq_local, tok_local, head_size, cols).transpose(2, 0, 1, 3)
    d_all, grad_own, grad_b_own = attend_back(
        inputs_full, qkv, log_total, exchange(d_context, 3)
    )
    grad_b_own = grad_b_own.reshape(-1)
    input_grad = input_grads(d_zone, exchange(d_all, 4), w_qkv)

    def put(array):
        empty = jnp.zeros(array.shape[:-1] + (width,), array.dtype)
        return lax.dynamic_update_slice_in_dim(empty, array, begin, array.ndim - 1)

    matrices = [put(grad_own[:, n * cols : (n + 1) * cols]) for n in range(3)]
    blocks = join_matrices(
        [matrix.astype(jnp.bfloat16) for matrix in matrices + [grad_out_w, grad_up, grad_down]]
    )
    vector_terms = jnp.concatenate(
        [
            put(grad_b_own[:cols]),
            put(grad_b_own[2 * cols :]),
            grad_bout,
            d_gain_one,
            d_shift_one,
            grad_bup,
            grad_bdown,
            d_gain_two,
            d_shift_two,
        ],
        0,
    ).reshape(total, vec_local)
    vec_terms = jnp.pad(vector_terms, ((0, 0), (0, VEC_ROWS * BLK - vec_local)))
    vec_terms = vec_terms.astype(jnp.bfloat16).reshape(total, VEC_ROWS, BLK)
    slot_grad, vec_sums = scatter_sums(dims, owner_slot, blocks, vec_terms)
    vec_grad = vec_sums.reshape(-1)[:vec_local]
    first_moment, second_moment, updated = rotate_adam(
        slot_grad, master, moment_one, moment_two, basis_left, basis_right
    )
    correct = 1.0 - 0.5**STEP
    vec_first = 0.5 * vec_moment_one + 0.5 * vec_grad
    vec_second = 0.5 * vec_moment_two + 0.5 * vec_grad * vec_grad
    vec_new = vec_master - VEC_RATE * (vec_first / correct) / (
        jnp.sqrt(vec_second / correct) + ADAM_EPS
    )
    new_average = KEEP * average + (1.0 - KEEP) * updated
    return (
        layer_out,
        input_grad,
        slot_grad,
        vec_grad,
        first_moment,
        second_moment,
        updated,
        updated.astype(jnp.bfloat16),
        new_average,
        vec_first,
        vec_second,
        vec_new,
    )


def solution(mesh):
    placed = (
        P("seq", "head", None),
        P("seq", "head", None),
        P("seq", "head"),
        P("seq", "head"),
        P(),
        P(("seq", "head"), None, None),
        P(("seq", "head"), None, None),
        P(("seq", "head"), None, None),
        P(("seq", "head"), None, None),
        P(("seq", "head"), None, None),
        P(("seq", "head"), None, None),
        P(("seq", "head")),
        P(("seq", "head")),
        P(("seq", "head")),
    )
    return jax.shard_map(
        body,
        mesh=mesh,
        in_specs=placed,
        out_specs=(
            P("seq", "head", None),
            P("seq", "head", None),
            P(("seq", "head"), None, None),
            P(("seq", "head")),
            P(("seq", "head"), None, None),
            P(("seq", "head"), None, None),
            P(("seq", "head"), None, None),
            P(("seq", "head"), None, None),
            P(("seq", "head"), None, None),
            P(("seq", "head")),
            P(("seq", "head")),
            P(("seq", "head")),
        ),
        check_vma=False,
    )
```

```python
import functools
import math

import jax
import jax.numpy as jnp
from jax import lax
from jax.experimental import pallas as pl
from jax.experimental.pallas import tpu as pltpu
from jax.sharding import PartitionSpec as P

D = 512
FF = 2048
WIN = 16
BLK = 128
STEP = 5
HD = 64
NBLK = 192
QUERIES = 256
SCALE = 1.0 / math.sqrt(HD)


NORM_EPS = 1e-06
ADAM_EPS = 1e-08
RATE = 0.05
VEC_RATE = 0.2
DECAY = 0.01
KEEP = 0.9
HIGH = lax.Precision.HIGHEST


def join_matrices(matrices):
    pieces = []
    for matrix in matrices:
        row_count = matrix.shape[0] // BLK
        col_count = matrix.shape[1] // BLK
        pieces.append(
            matrix.reshape(row_count, BLK, col_count, BLK)
            .transpose(0, 2, 1, 3)
            .reshape(row_count * col_count, BLK, BLK)
        )
    return jnp.concatenate(pieces, 0)


def split_vector(vector):
    widths = [D, D, D, D, D, FF, D, D, D]
    pieces = []
    offset = 0
    for extent in widths:
        pieces.append(vector[offset : offset + extent])
        offset = offset + extent
    return pieces


def layer_norm(values, gain, shift):
    center = values - jnp.mean(values, axis=-1, keepdims=True)
    spread = jnp.mean(center * center, axis=-1, keepdims=True)
    return center * lax.rsqrt(spread + NORM_EPS) * gain + shift


def gelu_value(values):
    return 0.5 * values * (1.0 + lax.erf(values * 0.7071067811865476))


def gelu_slope(values):
    return (
        0.5 * (1.0 + lax.erf(values * 0.7071067811865476))
        + values * jnp.exp(-0.5 * values * values) * 0.3989422804014327
    )


def span_mask(span_offset, span_len):
    offsets = jnp.repeat(span_offset, WIN, axis=1)
    extents = jnp.repeat(span_len, WIN, axis=1)
    within = (jnp.arange(offsets.shape[1], dtype=jnp.int32) % WIN)[None, :]
    return ((within >= offsets) & (within < offsets + extents)).astype(jnp.float32)


def contract(left, right, left_axis, right_axis):
    return lax.dot_general(
        left, right, (((left_axis,), (right_axis,)), ((), ())), preferred_element_type=jnp.float32
    )


def swap(source, target, send_sem, recv_sem, own_sem, item):
    head_size = source.shape[1]
    seq = lax.axis_index("seq")
    head = lax.axis_index("head")
    copies = []
    for step in [2, 1, 3] if head_size == 4 else range(1, head_size):
        peer = lax.rem(head + step, head_size)
        copies.append(
            pltpu.make_async_remote_copy(
                src_ref=source.at[item, peer],
                dst_ref=target.at[head, item],
                send_sem=send_sem.at[item, step],
                recv_sem=recv_sem.at[item, step],
                device_id=(seq, peer),
                device_id_type=MESH,
            )
        )
    copies.append(
        pltpu.make_async_copy(source.at[item, head], target.at[head, item], own_sem.at[item])
    )
    return copies


def swap_step(source, target, send_sem, recv_sem, own_sem):
    item = pl.program_id(0)
    for copy in swap(source, target, send_sem, recv_sem, own_sem, item):
        copy.start()

    @pl.when(item == pl.num_programs(0) - 1)
    def _():
        for number in range(source.shape[0]):
            for copy in swap(source, target, send_sem, recv_sem, own_sem, number):
                copy.wait()


def swap_scratch(items, head_size, tokens, columns):
    return [
        pltpu.VMEM((items, head_size, tokens, columns), jnp.bfloat16),
        pltpu.SemaphoreType.DMA((items, head_size)),
        pltpu.SemaphoreType.DMA((items, head_size)),
        pltpu.SemaphoreType.DMA((items,)),
    ]


def forward_kernel(
    x_ref, w_ref, b_ref, qkv_ref, ctx_out, lse_ref, ctx_ref, send_sem, recv_sem, own_sem
):
    item = pl.program_id(0)

    @pl.when(item == 0)
    def _():
        greet_head(ctx_ref.shape[1])

    head_size, tokens, width = x_ref.shape[0], x_ref.shape[1], x_ref.shape[2]
    length = head_size * tokens
    cols = w_ref.shape[1] // 3
    rows = x_ref[...].reshape(length, width)
    qkv_ref[...] = (contract(rows, w_ref[...], 1, 0) + b_ref[...]).astype(jnp.bfloat16)
    step = min(QUERIES, tokens)
    for number in range(cols // HD):
        low = number * HD
        keys = qkv_ref[:, cols + low : cols + low + HD]
        values = qkv_ref[:, 2 * cols + low : 2 * cols + low + HD]
        for begin in range(0, length, step):
            query = qkv_ref[begin : begin + step, low : low + HD] * jnp.bfloat16(SCALE)
            scores = contract(keys, query, 1, 1)
            highest = jnp.max(scores, axis=0, keepdims=True)
            weights = jnp.exp(scores - highest)
            summed = jnp.sum(weights, axis=0, keepdims=True)
            probs = (weights * (1.0 / summed)).astype(jnp.bfloat16)
            context = contract(values, probs, 0, 0).T.astype(jnp.bfloat16)
            ctx_ref[item, begin // tokens, pl.ds(begin % tokens, step), low : low + HD] = context
            lse_ref[number : number + 1, begin : begin + step] = highest + jnp.log(summed)
    swap_step(ctx_ref, ctx_out, send_sem, recv_sem, own_sem)


def attend(inputs_full, weights, bias):
    seq_local, head_size, tokens, width = inputs_full.shape
    length = head_size * tokens
    cols = weights.shape[1] // 3
    return pl.pallas_call(
        forward_kernel,
        grid=(seq_local,),
        out_shape=(
            jax.ShapeDtypeStruct((seq_local, length, 3 * cols), jnp.bfloat16),
            jax.ShapeDtypeStruct((head_size, seq_local, tokens, cols), jnp.bfloat16),
            jax.ShapeDtypeStruct((seq_local, 8, length), jnp.float32),
        ),
        in_specs=[
            pl.BlockSpec((None, head_size, tokens, width), lambda s: (s, 0, 0, 0)),
            pl.BlockSpec((width, 3 * cols), lambda s: (0, 0)),
            pl.BlockSpec((1, 3 * cols), lambda s: (0, 0)),
        ],
        out_specs=(
            pl.BlockSpec((None, length, 3 * cols), lambda s: (s, 0, 0)),
            pl.BlockSpec(memory_space=pl.ANY),
            pl.BlockSpec((None, 8, length), lambda s: (s, 0, 0)),
        ),
        scratch_shapes=swap_scratch(seq_local, head_size, tokens, cols),
        compiler_params=pltpu.CompilerParams(
            collective_id=2, has_side_effects=True, vmem_limit_bytes=48 * 1024 * 1024
        ),
        name="attend",
    )(inputs_full, weights, bias)


def backward_kernel(
    x_ref,
    qkv_ref,
    lse_ref,
    dctx_ref,
    grad_out,
    dw_ref,
    db_ref,
    dall,
    acc,
    grad_ref,
    send_sem,
    recv_sem,
    own_sem,
):
    item = pl.program_id(0)

    @pl.when(item == 0)
    def _():
        greet_head(grad_ref.shape[1])

    head_size, tokens, width = x_ref.shape[0], x_ref.shape[1], x_ref.shape[2]
    length = head_size * tokens
    cols = qkv_ref.shape[1] // 3
    step = min(QUERIES, tokens)
    scale = jnp.bfloat16(SCALE)
    for number in range(cols // HD):
        low = number * HD
        keys = qkv_ref[:, cols + low : cols + low + HD]
        values = qkv_ref[:, 2 * cols + low : 2 * cols + low + HD]
        for begin in range(0, length, step):
            query = qkv_ref[begin : begin + step, low : low + HD] * scale
            dctx = dctx_ref[begin // tokens, pl.ds(begin % tokens, step), low : low + HD]
            scores = contract(keys, query, 1, 1)
            probs = jnp.exp(scores - lse_ref[number : number + 1, begin : begin + step])
            dprobs = contract(values, dctx, 1, 1)
            inner = jnp.sum(probs * dprobs, axis=0, keepdims=True)
            dscores = (probs * (dprobs - inner)).astype(jnp.bfloat16)
            dkey = contract(dscores, query, 1, 0)
            dvalue = contract(probs.astype(jnp.bfloat16), dctx, 1, 0)
            if begin == 0:
                acc[0] = dkey
                acc[1] = dvalue
            else:
                acc[0] += dkey
                acc[1] += dvalue
            dquery = contract(keys, dscores, 0, 0).T * SCALE
            dall[begin : begin + step, low : low + HD] = dquery.astype(jnp.bfloat16)
        dall[:, cols + low : cols + low + HD] = acc[0].astype(jnp.bfloat16)
        dall[:, 2 * cols + low : 2 * cols + low + HD] = acc[1].astype(jnp.bfloat16)
    rows = x_ref[...].reshape(length, width)
    delta = dall[...]
    grad_ref[item] = delta.reshape(head_size, tokens, 3 * cols)
    swap_step(grad_ref, grad_out, send_sem, recv_sem, own_sem)
    dw = contract(rows, delta, 0, 0)
    db = jnp.sum(delta.astype(jnp.float32), axis=0, keepdims=True)

    @pl.when(pl.program_id(0) == 0)
    def _():
        dw_ref[...] = dw
        db_ref[...] = db

    @pl.when(pl.program_id(0) > 0)
    def _():
        dw_ref[...] += dw
        db_ref[...] += db


def attend_back(inputs_full, qkv, lse, dctx):
    seq_local, head_size, tokens, width = inputs_full.shape
    length = head_size * tokens
    cols = qkv.shape[2] // 3
    return pl.pallas_call(
        backward_kernel,
        grid=(seq_local,),
        out_shape=(
            jax.ShapeDtypeStruct((head_size, seq_local, tokens, 3 * cols), jnp.bfloat16),
            jax.ShapeDtypeStruct((width, 3 * cols), jnp.float32),
            jax.ShapeDtypeStruct((1, 3 * cols), jnp.float32),
        ),
        in_specs=[
            pl.BlockSpec((None, head_size, tokens, width), lambda s: (s, 0, 0, 0)),
            pl.BlockSpec((None, length, 3 * cols), lambda s: (s, 0, 0)),
            pl.BlockSpec((None, 8, length), lambda s: (s, 0, 0)),
            pl.BlockSpec((head_size, None, tokens, cols), lambda s: (0, s, 0, 0)),
        ],
        out_specs=(
            pl.BlockSpec(memory_space=pl.ANY),
            pl.BlockSpec((width, 3 * cols), lambda s: (0, 0)),
            pl.BlockSpec((1, 3 * cols), lambda s: (0, 0)),
        ),
        scratch_shapes=[
            pltpu.VMEM((length, 3 * cols), jnp.bfloat16),
            pltpu.VMEM((2, length, HD), jnp.float32),
        ]
        + swap_scratch(seq_local, head_size, tokens, 3 * cols),
        compiler_params=pltpu.CompilerParams(
            collective_id=4, has_side_effects=True, vmem_limit_bytes=48 * 1024 * 1024
        ),
        name="attend_back",
    )(inputs_full, qkv, lse, dctx)


def input_grad_kernel(dz_ref, d_ref, w_ref, out_ref):
    total = dz_ref[...]
    for number in range(d_ref.shape[0]):
        total = total + contract(d_ref[number], w_ref[number], 1, 1)
    out_ref[...] = total


def input_grads(d_zone, deltas, weights):
    head_size, seq_local, tokens, columns = deltas.shape
    width = d_zone.shape[1]
    return pl.pallas_call(
        input_grad_kernel,
        grid=(seq_local,),
        out_shape=jax.ShapeDtypeStruct((seq_local, tokens, width), jnp.float32),
        in_specs=[
            pl.BlockSpec((tokens, width), lambda s: (s, 0)),
            pl.BlockSpec((head_size, None, tokens, columns), lambda s: (0, s, 0, 0)),
            pl.BlockSpec((head_size, width, columns), lambda s: (0, 0, 0)),
        ],
        out_specs=pl.BlockSpec((None, tokens, width), lambda s: (s, 0, 0)),
        name="input_grads",
    )(d_zone, deltas, weights)


def rotate_adam(grads, master, moment_one, moment_two, basis_left, basis_right):
    rotated = jnp.einsum("sji,sjk->sik", basis_left, grads, precision=HIGH)
    rotated = jnp.einsum("sik,skl->sil", rotated, basis_right, precision=HIGH)
    first = 0.5 * moment_one + 0.5 * rotated
    second = 0.5 * moment_two + 0.5 * rotated * rotated
    correct = 1.0 - 0.5**STEP
    normed = first / correct / (jnp.sqrt(second / correct) + ADAM_EPS)
    turned = jnp.einsum("sij,sjk->sik", basis_left, normed, precision=HIGH)
    turned = jnp.einsum("sik,slk->sil", turned, basis_right, precision=HIGH)
    updated = master - RATE * (turned + DECAY * master)
    return (first, second, updated)


def weight_grad(left, right):
    return jnp.einsum("ti,to->io", left, right, preferred_element_type=jnp.float32)


def back_product(grads, weight):
    return jnp.einsum("to,io->ti", grads, weight, preferred_element_type=jnp.float32)


MESH = pl.DeviceIdType.MESH
VEC_ROWS = 16
PIECE = 16


def cut(seq_size, head_size):
    cores = 2 if head_size % 2 == 0 else 1
    rows = 1
    while 2 * (rows * 2) ** 2 <= seq_size and seq_size % (rows * 2) == 0:
        rows = rows * 2
    return (seq_size // rows, rows, head_size // cores, cores)


def place(dims):
    size_z, size_x, size_y, size_c = dims
    seq = lax.axis_index("seq")
    head = lax.axis_index("head")
    return (
        lax.div(seq, size_x),
        lax.rem(seq, size_x),
        lax.div(head, size_c),
        lax.rem(head, size_c),
    )


def device(dims, coords):
    return (coords[0] * dims[1] + coords[1], coords[2] * dims[3] + coords[3])


def flat(dims, coords):
    return ((coords[0] * dims[1] + coords[1]) * dims[2] + coords[2]) * dims[3] + coords[3]


def moved(dims, coords, axis, step):
    new = list(coords)
    new[axis] = lax.rem(coords[axis] + step, dims[axis])
    return tuple(new)


def greet(dims, coords):
    barrier = pltpu.get_barrier_semaphore()
    count = 0
    for axis in range(4):
        for step in range(1, dims[axis]):
            pl.semaphore_signal(
                barrier,
                inc=1,
                device_id=device(dims, moved(dims, coords, axis, step)),
                device_id_type=MESH,
            )
            count = count + 1
    pl.semaphore_wait(barrier, count)


def greet_head(head_size):
    barrier = pltpu.get_barrier_semaphore()
    seq = lax.axis_index("seq")
    head = lax.axis_index("head")
    for step in range(1, head_size):
        pl.semaphore_signal(
            barrier, inc=1, device_id=(seq, lax.rem(head + step, head_size)), device_id_type=MESH
        )
    pl.semaphore_wait(barrier, head_size - 1)


def gather_kernel(
    dims,
    inv_ref,
    x_ref,
    w_ref,
    xf_ref,
    qkv_ref,
    out_ref,
    up_ref,
    down_ref,
    vec_ref,
    wf_ref,
    own_sem,
    x_send,
    x_recv,
    w_send,
    w_recv,
):
    me = place(dims)
    size_z, size_x, size_y, size_c = dims
    head_me = me[2] * size_c + me[3]
    chunk = w_ref.shape[0]

    def spot(index):
        return wf_ref.at[pl.ds(index * chunk, chunk)]

    own_x = pltpu.make_async_copy(x_ref, xf_ref.at[:, head_me], own_sem.at[0])
    own_w = pltpu.make_async_copy(w_ref, spot(flat(dims, me)), own_sem.at[1])
    own_x.start()
    own_w.start()
    greet(dims, me)
    started = []

    def send_x(source, head, target, number):
        copy = pltpu.make_async_remote_copy(
            src_ref=source,
            dst_ref=xf_ref.at[:, head],
            send_sem=x_send.at[number],
            recv_sem=x_recv.at[head],
            device_id=device(dims, target),
            device_id_type=MESH,
        )
        copy.start()
        started.append(copy)

    def arrived_x(head):
        pltpu.make_async_remote_copy(
            src_ref=x_ref,
            dst_ref=xf_ref.at[:, head],
            send_sem=x_send.at[0],
            recv_sem=x_recv.at[head],
            device_id=device(dims, me),
            device_id_type=MESH,
        ).wait_recv()

    count = [0]

    def send_w(source, index, target):
        number = count[0]
        count[0] = number + 1
        copy = pltpu.make_async_remote_copy(
            src_ref=source,
            dst_ref=spot(index),
            send_sem=w_send.at[number],
            recv_sem=w_recv.at[index],
            device_id=device(dims, target),
            device_id_type=MESH,
        )
        copy.start()
        started.append(copy)

    def arrived_w(index):
        pltpu.make_async_remote_copy(
            src_ref=w_ref,
            dst_ref=spot(index),
            send_sem=w_send.at[0],
            recv_sem=w_recv.at[index],
            device_id=device(dims, me),
            device_id_type=MESH,
        ).wait_recv()

    order = [0, 2, 1, 3]

    def forward(source, coords, after):
        for axis in order[after:]:
            for step in range(1, dims[axis]):
                send_w(source, flat(dims, coords), moved(dims, me, axis, step))

    number = 0
    for step in range(1, size_y):
        send_x(x_ref, head_me, moved(dims, me, 2, step), number)
        number = number + 1
    for step in range(1, size_c):
        send_x(x_ref, head_me, moved(dims, me, 3, step), number)
        number = number + 1
    forward(w_ref, me, 0)
    held = [me]
    for level in range(3):
        axis = order[level]
        fresh = []
        for step in range(1, dims[axis]):
            for coords in held:
                source = moved(dims, coords, axis, step)
                arrived_w(flat(dims, source))
                forward(spot(flat(dims, source)), source, level + 1)
                fresh.append(source)
        held = held + fresh
        if level == 1:
            for step in range(1, size_y):
                other = moved(dims, me, 2, step)
                head = other[2] * size_c + other[3]
                arrived_x(head)
                for hop in range(1, size_c):
                    send_x(xf_ref.at[:, head], head, moved(dims, me, 3, hop), number)
                    number = number + 1
    for step in range(1, size_c):
        for coords in held:
            arrived_w(flat(dims, moved(dims, coords, 3, step)))
        for across in range(size_y):
            other = moved(dims, moved(dims, me, 3, step), 2, across)
            arrived_x(other[2] * size_c + other[3])
    for copy in started:
        copy.wait_send()
    own_x.wait()
    own_w.wait()
    unpack(dims, inv_ref, wf_ref, qkv_ref, out_ref, up_ref, down_ref)
    chunk = w_ref.shape[0]
    for number in range(vec_ref.shape[0]):
        vec_ref[number] = wf_ref[(number + 1) * chunk - 1]


def unpack(dims, inv_ref, wf_ref, qkv_ref, out_ref, up_ref, down_ref):
    head_size = dims[2] * dims[3]
    width = out_ref.shape[0]
    hidden = up_ref.shape[1]
    cols = width // head_size
    across = width // BLK

    def block(number):
        piece = inv_ref[number]
        return jnp.concatenate([wf_ref[piece + part] for part in range(BLK // PIECE)], 0)

    def rows_of(row_count, first, col_count, store):
        def one(row, carry):
            span = pl.ds(pl.multiple_of(row * BLK, BLK), BLK)
            for col in range(col_count):
                store(span, col, block(first + row * col_count + col))
            return carry

        lax.fori_loop(0, row_count, one, 0)

    for number in range(3):

        def store_qkv(span, col, value, number=number):
            for begin in range(0, BLK, min(cols, BLK)):
                head = (col * BLK + begin) // cols
                lane = (col * BLK + begin) % cols
                part = min(cols, BLK)
                qkv_ref[head, span, number * cols + lane : number * cols + lane + part] = value[
                    :, begin : begin + part
                ]

        rows_of(across, number * across * across, across, store_qkv)

    def store_in(ref):
        def store(span, col, value):
            ref[span, col * BLK : (col + 1) * BLK] = value

        return store

    rows_of(across, 3 * across * across, across, store_in(out_ref))
    first = 4 * across * across
    rows_of(across, first, hidden // BLK, store_in(up_ref))
    first = first + across * (hidden // BLK)
    rows_of(hidden // BLK, first, across, store_in(down_ref))


def gather_all(dims, inverse, inputs, packed):
    size_z, size_x, size_y, size_c = dims
    total = size_z * size_x * size_y * size_c
    head_size = size_y * size_c
    seq_local, tok_local, width = inputs.shape
    any_space = pl.BlockSpec(memory_space=pl.ANY)
    whole = pl.BlockSpec(memory_space=pltpu.VMEM)
    sends_x = (size_y - 1) * size_c + size_c - 1
    sends_w = (
        (size_z - 1)
        + size_z * (size_y - 1)
        + size_z * size_y * (size_x - 1)
        + size_z * size_y * size_x * (size_c - 1)
    )
    return pl.pallas_call(
        functools.partial(gather_kernel, dims),
        out_shape=(
            jax.ShapeDtypeStruct((seq_local, head_size, tok_local, width), inputs.dtype),
            jax.ShapeDtypeStruct((head_size, width, 3 * width // head_size), packed.dtype),
            jax.ShapeDtypeStruct((width, width), packed.dtype),
            jax.ShapeDtypeStruct((width, FF), packed.dtype),
            jax.ShapeDtypeStruct((FF, width), packed.dtype),
            jax.ShapeDtypeStruct((total, VEC_ROWS, BLK), packed.dtype),
        ),
        in_specs=[pl.BlockSpec(memory_space=pltpu.SMEM), whole, whole],
        out_specs=(any_space, whole, whole, whole, whole, whole),
        scratch_shapes=[
            pltpu.VMEM((total * packed.shape[0],) + packed.shape[1:], packed.dtype),
            pltpu.SemaphoreType.DMA((2,)),
            pltpu.SemaphoreType.DMA((max(sends_x, 1),)),
            pltpu.SemaphoreType.DMA((head_size,)),
            pltpu.SemaphoreType.DMA((max(sends_w, 1),)),
            pltpu.SemaphoreType.DMA((total,)),
        ],
        compiler_params=pltpu.CompilerParams(
            collective_id=0, has_side_effects=True, vmem_limit_bytes=40 * 1024 * 1024
        ),
        name="gather_all",
    )(inverse, inputs, packed)


def exchange_kernel(head_size, src_ref, dst_ref, own_sem, send_sem, recv_sem):
    seq = lax.axis_index("seq")
    head = lax.axis_index("head")
    own = pltpu.make_async_copy(src_ref.at[head], dst_ref.at[head], own_sem)
    own.start()
    greet_head(head_size)
    copies = []
    for step in [2, 1, 3] if head_size == 4 else range(1, head_size):
        peer = lax.rem(head + step, head_size)
        copy = pltpu.make_async_remote_copy(
            src_ref=src_ref.at[peer],
            dst_ref=dst_ref.at[head],
            send_sem=send_sem.at[step],
            recv_sem=recv_sem.at[step],
            device_id=(seq, peer),
            device_id_type=MESH,
        )
        copy.start()
        copies.append(copy)
    for copy in copies:
        copy.wait()
    own.wait()


def exchange(array, number):
    head_size = array.shape[0]
    if head_size == 1:
        return array
    whole = pl.BlockSpec(memory_space=pltpu.VMEM)
    return pl.pallas_call(
        functools.partial(exchange_kernel, head_size),
        out_shape=jax.ShapeDtypeStruct(array.shape, array.dtype),
        in_specs=[whole],
        out_specs=whole,
        scratch_shapes=[
            pltpu.SemaphoreType.DMA,
            pltpu.SemaphoreType.DMA((head_size,)),
            pltpu.SemaphoreType.DMA((head_size,)),
        ],
        compiler_params=pltpu.CompilerParams(collective_id=number, has_side_effects=True),
        name="exchange",
    )(array)


def scatter_kernel(
    dims,
    slots,
    owner_ref,
    blocks_ref,
    vec_ref,
    grad_ref,
    vec_out_ref,
    term,
    got_c,
    got_x,
    got_y,
    got_z,
    send_c,
    send_x,
    send_y,
    send_z,
    recv_c,
    recv_x,
    recv_y,
    recv_z,
):
    me = place(dims)
    size_z, size_x, size_y, size_c = dims
    rows = slots * BLK
    greet(dims, me)

    def block_of(dest, slot):
        owner = owner_ref[dest * slots + slot]
        block = blocks_ref[jnp.minimum(owner, NBLK - 1)]
        return jnp.where(owner < NBLK, block, jnp.zeros_like(block))

    def total_of(dest, extras, keep_block, keep_vec):
        def one(slot, carry):
            value = block_of(dest, slot).astype(jnp.float32)
            span = pl.ds(pl.multiple_of(slot * BLK, BLK), BLK)
            for ref, lead in extras:
                value = value + ref[lead + (span,)].astype(jnp.float32)
            keep_block(slot, span, value)
            return carry

        lax.fori_loop(0, slots, one, 0)
        value = vec_ref[dest].astype(jnp.float32)
        for ref, lead in extras:
            value = value + ref[lead + (pl.ds(rows, VEC_ROWS),)].astype(jnp.float32)
        keep_vec(value)

    def into_term(dest, extras):
        def keep_block(slot, span, value):
            term[dest, span] = value.astype(jnp.bfloat16)

        def keep_vec(value):
            term[dest, pl.ds(rows, VEC_ROWS)] = value.astype(jnp.bfloat16)

        total_of(dest, extras, keep_block, keep_vec)

    def remote(dest, got, send, recv, hop, index, target):
        return pltpu.make_async_remote_copy(
            src_ref=term.at[dest],
            dst_ref=got.at[hop, index],
            send_sem=send.at[hop, index],
            recv_sem=recv.at[hop, index],
            device_id=device(dims, target),
            device_id_type=MESH,
        )

    def each(axis, begin, end, coords_of, extras_of, got, send, recv, only=None):
        for step in range(1, dims[axis]) if only is None else [only]:
            target = moved(dims, me, axis, step)

            def one(index, carry, step=step, target=target):
                coords = list(coords_of(index))
                coords[axis] = target[axis]
                dest = flat(dims, coords)
                into_term(dest, extras_of(coords))
                remote(dest, got, send, recv, step - 1, index, target).start()
                return carry

            if end == begin + 1:
                one(begin, 0)
            else:
                lax.fori_loop(begin, end, one, 0)

    def wait_for(axis, got, send, recv, index):
        found = []
        for step in range(1, dims[axis]):
            remote(0, got, send, recv, step - 1, index, moved(dims, me, axis, step)).wait_recv()
            found.append((got, (step - 1, index)))
        return found

    def turn_z(order):
        return lax.rem(me[0] + 1 + order, size_z)

    def order_z(coords):
        return lax.rem(coords[0] - me[0] + 2 * size_z - 1, size_z)

    def index_c(coords):
        order_x = lax.rem(coords[1] - me[1] + size_x - 1 + size_x, size_x)
        return (order_z(coords) * size_x + order_x) * size_y + coords[2]

    def coords_c(index):
        order_x = lax.rem(lax.div(index, size_y), size_x)
        return (
            turn_z(lax.div(index, size_x * size_y)),
            lax.rem(me[1] + 1 + order_x, size_x),
            lax.rem(index, size_y),
            me[3],
        )

    def coords_x(index):
        return (turn_z(lax.div(index, size_y)), me[1], lax.rem(index, size_y), me[3])

    def coords_y(index):
        return (turn_z(index), me[1], me[2], me[3])

    def coords_z(index):
        return me

    def extras_c(coords):
        return []

    def extras_x(coords):
        return wait_for(3, got_c, send_c, recv_c, index_c(coords))

    def extras_y(coords):
        return extras_x(coords) + wait_for(
            1, got_x, send_x, recv_x, order_z(coords) * size_y + coords[2]
        )

    def extras_z(coords):
        return extras_y(coords) + wait_for(2, got_y, send_y, recv_y, order_z(coords))

    def stage_c(order):
        group = size_x * size_y
        each(3, order * group, (order + 1) * group, coords_c, extras_c, got_c, send_c, recv_c)

    def stage_x(order):
        group = size_y
        each(1, order * group, (order + 1) * group, coords_x, extras_x, got_x, send_x, recv_x)

    stage_c(0)
    for order in range(1, size_z):
        stage_c(order)
        stage_x(order - 1)
    stage_x(size_z - 1)
    for order in range(size_z):
        each(2, order, order + 1, coords_y, extras_y, got_y, send_y, recv_y)
        if order + 1 < size_z:
            each(0, 0, 1, coords_z, extras_z, got_z, send_z, recv_z, only=order + 1)
    extras = extras_z(me) + wait_for(0, got_z, send_z, recv_z, 0)

    def keep_block(slot, span, value):
        grad_ref[slot] = value

    def keep_vec(value):
        vec_out_ref[...] = value

    total_of(flat(dims, me), extras, keep_block, keep_vec)

    def drain(axis, count, got, send, recv):
        for step in range(1, dims[axis]):

            def one(index, carry, step=step):
                remote(
                    0, got, send, recv, step - 1, index, moved(dims, me, axis, step)
                ).wait_send()
                return carry

            lax.fori_loop(0, count, one, 0)

    drain(3, size_z * size_x * size_y, got_c, send_c, recv_c)
    drain(1, size_z * size_y, got_x, send_x, recv_x)
    drain(2, size_z, got_y, send_y, recv_y)
    drain(0, 1, got_z, send_z, recv_z)


def scatter_sums(dims, owner_slot, blocks, vec_terms):
    size_z, size_x, size_y, size_c = dims
    total = size_z * size_x * size_y * size_c
    slots = owner_slot.shape[0] // total
    chunk = (slots * BLK + VEC_ROWS, BLK)
    shapes = [
        (max(size_c - 1, 1), size_z * size_x * size_y),
        (max(size_x - 1, 1), size_z * size_y),
        (max(size_y - 1, 1), size_z),
        (max(size_z - 1, 1), 1),
    ]
    whole = pl.BlockSpec(memory_space=pltpu.VMEM)
    return pl.pallas_call(
        functools.partial(scatter_kernel, dims, slots),
        out_shape=(
            jax.ShapeDtypeStruct((slots, BLK, BLK), jnp.float32),
            jax.ShapeDtypeStruct((VEC_ROWS, BLK), jnp.float32),
        ),
        in_specs=[pl.BlockSpec(memory_space=pltpu.SMEM), whole, whole],
        out_specs=(whole, whole),
        scratch_shapes=[pltpu.VMEM((total,) + chunk, jnp.bfloat16)]
        + [pltpu.VMEM(shape + chunk, jnp.bfloat16) for shape in shapes]
        + [pltpu.SemaphoreType.DMA(shape) for shape in shapes]
        + [pltpu.SemaphoreType.DMA(shape) for shape in shapes],
        compiler_params=pltpu.CompilerParams(
            collective_id=1, has_side_effects=True, vmem_limit_bytes=60 * 1024 * 1024
        ),
        name="scatter_sums",
    )(owner_slot, blocks, vec_terms)


def three_parts(values):
    high = lax.reduce_precision(values, 8, 7)
    rest = values - high
    middle = lax.reduce_precision(rest, 8, 7)
    low = lax.reduce_precision(rest - middle, 8, 7)
    return [part.astype(jnp.bfloat16) for part in (high, middle, low)]


def as_rows(vector, rows):
    return jnp.pad(vector, (0, rows * BLK - vector.shape[0])).reshape(rows, BLK)


def ceil_to(value, unit):
    return -(-value // unit) * unit


def body(
    inputs,
    cotangent,
    span_offset,
    span_len,
    owner_slot,
    master,
    moment_one,
    moment_two,
    basis_left,
    basis_right,
    average,
    vec_master,
    vec_moment_one,
    vec_moment_two,
):
    both = ("seq", "head")
    seq_size = lax.axis_size("seq")
    head_size = lax.axis_size("head")
    total = seq_size * head_size
    head_index = lax.axis_index("head")
    seq_local, tok_local, width = inputs.shape
    slots_local = master.shape[0]
    slot_total = slots_local * total
    vec_local = vec_master.shape[0]

    dims = cut(seq_size, head_size)

    packed = jnp.concatenate(
        [
            master.astype(jnp.bfloat16).reshape(slots_local * BLK, BLK),
            as_rows(jnp.concatenate(three_parts(vec_master)), VEC_ROWS),
        ],
        0,
    ).reshape(-1, PIECE, BLK)
    numbers = jnp.arange(slot_total, dtype=jnp.int32)
    inverse = jnp.sum(
        jnp.where(owner_slot[:, None] == numbers[None, :], numbers[:, None], 0), axis=0
    )
    pieces = (inverse // slots_local) * packed.shape[0]
    pieces = pieces + (inverse % slots_local) * (BLK // PIECE)
    inputs_full, w_qkv, w_out, w_up, w_down, vec_parts = gather_all(
        dims, pieces, inputs, packed
    )
    parts = (
        vec_parts
        .reshape(total, VEC_ROWS * BLK)[:, : 3 * vec_local]
        .reshape(total, 3, vec_local)
        .astype(jnp.float32)
    )
    all_vector = ((parts[:, 2] + parts[:, 1]) + parts[:, 0]).reshape(-1)

    b_query, b_value, b_out, gain_one, shift_one, b_up, b_down, gain_two, shift_two = split_vector(
        all_vector
    )
    token_rows = inputs.reshape(seq_local * tok_local, width)
    local_shape = (seq_local, tok_local, width)
    cols = width // head_size
    begin = head_index * cols

    def own(array):
        return lax.dynamic_slice_in_dim(array, begin, cols, array.ndim - 1)

    w_own = lax.dynamic_index_in_dim(w_qkv, head_index, 0, keepdims=False)
    b_own = jnp.concatenate([own(b_query), jnp.zeros((cols,), jnp.float32), own(b_value)], 0)
    qkv, context, log_total = attend(inputs_full, w_own, b_own[None, :])
    context_rows = context.transpose(1, 2, 0, 3).reshape(seq_local * tok_local, width)
    branch = jnp.dot(context_rows, w_out, preferred_element_type=jnp.float32) + b_out
    z_one = token_rows.astype(jnp.float32) + branch
    first = layer_norm(z_one, gain_one, shift_one)
    first_low = first.astype(jnp.bfloat16)
    hidden_in = jnp.dot(first_low, w_up, preferred_element_type=jnp.float32) + b_up
    hidden_act = gelu_value(hidden_in).astype(jnp.bfloat16)
    ffn_out = jnp.dot(hidden_act, w_down, preferred_element_type=jnp.float32) + b_down
    z_two = first + ffn_out
    result, pull_two = jax.vjp(layer_norm, z_two, gain_two, shift_two)
    layer_out = result.astype(jnp.bfloat16).reshape(local_shape)
    mask = span_mask(span_offset, span_len)
    grad_out = (cotangent.astype(jnp.float32) * mask[:, :, None]).reshape(
        seq_local * tok_local, width
    )
    d_ztwo, d_gain_two, d_shift_two = pull_two(grad_out)
    d_ffn = d_ztwo.astype(jnp.bfloat16)
    grad_down = weight_grad(hidden_act, d_ffn)
    grad_bdown = jnp.sum(d_ffn.astype(jnp.float32), axis=0)
    d_hidden = back_product(d_ffn, w_down)
    d_hidden_in = (d_hidden * gelu_slope(hidden_in)).astype(jnp.bfloat16)
    grad_up = weight_grad(first_low, d_hidden_in)
    grad_bup = jnp.sum(d_hidden_in.astype(jnp.float32), axis=0)
    d_first = d_ztwo + back_product(d_hidden_in, w_up)
    sink, pull_one = jax.vjp(layer_norm, z_one, gain_one, shift_one)
    d_zone, d_gain_one, d_shift_one = pull_one(d_first)
    d_branch = d_zone.astype(jnp.bfloat16)
    grad_out_w = weight_grad(context_rows, d_branch)
    grad_bout = jnp.sum(d_branch.astype(jnp.float32), axis=0)

    d_context = back_product(d_branch, w_out).astype(jnp.bfloat16)
    d_context = d_context.reshape(seq_local, tok_local, head_size, cols).transpose(2, 0, 1, 3)
    d_all, grad_own, grad_b_own = attend_back(
        inputs_full, qkv, log_total, exchange(d_context, 3)
    )
    grad_b_own = grad_b_own.reshape(-1)
    input_grad = input_grads(d_zone, d_all, w_qkv)

    def put(array):
        empty = jnp.zeros(array.shape[:-1] + (width,), array.dtype)
        return lax.dynamic_update_slice_in_dim(empty, array, begin, array.ndim - 1)

    matrices = [put(grad_own[:, n * cols : (n + 1) * cols]) for n in range(3)]
    blocks = join_matrices(
        [matrix.astype(jnp.bfloat16) for matrix in matrices + [grad_out_w, grad_up, grad_down]]
    )
    vector_terms = jnp.concatenate(
        [
            put(grad_b_own[:cols]),
            put(grad_b_own[2 * cols :]),
            grad_bout,
            d_gain_one,
            d_shift_one,
            grad_bup,
            grad_bdown,
            d_gain_two,
            d_shift_two,
        ],
        0,
    ).reshape(total, vec_local)
    vec_terms = jnp.pad(vector_terms, ((0, 0), (0, VEC_ROWS * BLK - vec_local)))
    vec_terms = vec_terms.astype(jnp.bfloat16).reshape(total, VEC_ROWS, BLK)
    slot_grad, vec_sums = scatter_sums(dims, owner_slot, blocks, vec_terms)
    vec_grad = vec_sums.reshape(-1)[:vec_local]
    first_moment, second_moment, updated = rotate_adam(
        slot_grad, master, moment_one, moment_two, basis_left, basis_right
    )
    correct = 1.0 - 0.5**STEP
    vec_first = 0.5 * vec_moment_one + 0.5 * vec_grad
    vec_second = 0.5 * vec_moment_two + 0.5 * vec_grad * vec_grad
    vec_new = vec_master - VEC_RATE * (vec_first / correct) / (
        jnp.sqrt(vec_second / correct) + ADAM_EPS
    )
    new_average = KEEP * average + (1.0 - KEEP) * updated
    return (
        layer_out,
        input_grad,
        slot_grad,
        vec_grad,
        first_moment,
        second_moment,
        updated,
        updated.astype(jnp.bfloat16),
        new_average,
        vec_first,
        vec_second,
        vec_new,
    )


def solution(mesh):
    placed = (
        P("seq", "head", None),
        P("seq", "head", None),
        P("seq", "head"),
        P("seq", "head"),
        P(),
        P(("seq", "head"), None, None),
        P(("seq", "head"), None, None),
        P(("seq", "head"), None, None),
        P(("seq", "head"), None, None),
        P(("seq", "head"), None, None),
        P(("seq", "head"), None, None),
        P(("seq", "head")),
        P(("seq", "head")),
        P(("seq", "head")),
    )
    return jax.shard_map(
        body,
        mesh=mesh,
        in_specs=placed,
        out_specs=(
            P("seq", "head", None),
            P("seq", "head", None),
            P(("seq", "head"), None, None),
            P(("seq", "head")),
            P(("seq", "head"), None, None),
            P(("seq", "head"), None, None),
            P(("seq", "head"), None, None),
            P(("seq", "head"), None, None),
            P(("seq", "head"), None, None),
            P(("seq", "head")),
            P(("seq", "head")),
            P(("seq", "head")),
        ),
        check_vma=False,
    )
```

```python
import functools
import math

import jax
import jax.numpy as jnp
from jax import lax
from jax.experimental import pallas as pl
from jax.experimental.pallas import tpu as pltpu
from jax.sharding import PartitionSpec as P

D = 512
FF = 2048
WIN = 16
BLK = 128
STEP = 5
HD = 64
NBLK = 192
QUERIES = 256
SCALE = 1.0 / math.sqrt(HD)


NORM_EPS = 1e-06
ADAM_EPS = 1e-08
RATE = 0.05
VEC_RATE = 0.2
DECAY = 0.01
KEEP = 0.9
HIGH = lax.Precision.HIGHEST


def split_vector(vector):
    widths = [D, D, D, D, D, FF, D, D, D]
    pieces = []
    offset = 0
    for extent in widths:
        pieces.append(vector[offset : offset + extent])
        offset = offset + extent
    return pieces


def layer_norm(values, gain, shift):
    center = values - jnp.mean(values, axis=-1, keepdims=True)
    spread = jnp.mean(center * center, axis=-1, keepdims=True)
    return center * lax.rsqrt(spread + NORM_EPS) * gain + shift


def gelu_value(values):
    return 0.5 * values * (1.0 + lax.erf(values * 0.7071067811865476))


def gelu_slope(values):
    return (
        0.5 * (1.0 + lax.erf(values * 0.7071067811865476))
        + values * jnp.exp(-0.5 * values * values) * 0.3989422804014327
    )


def span_mask(span_offset, span_len):
    offsets = jnp.repeat(span_offset, WIN, axis=1)
    extents = jnp.repeat(span_len, WIN, axis=1)
    within = (jnp.arange(offsets.shape[1], dtype=jnp.int32) % WIN)[None, :]
    return ((within >= offsets) & (within < offsets + extents)).astype(jnp.float32)


def contract(left, right, left_axis, right_axis):
    return lax.dot_general(
        left, right, (((left_axis,), (right_axis,)), ((), ())), preferred_element_type=jnp.float32
    )


def swap(source, target, send_sem, recv_sem, own_sem, item):
    head_size = source.shape[1]
    seq = lax.axis_index("seq")
    head = lax.axis_index("head")
    copies = []
    for step in [2, 1, 3] if head_size == 4 else range(1, head_size):
        peer = lax.rem(head + step, head_size)
        copies.append(
            pltpu.make_async_remote_copy(
                src_ref=source.at[item, peer],
                dst_ref=target.at[head, item],
                send_sem=send_sem.at[item, step],
                recv_sem=recv_sem.at[item, step],
                device_id=(seq, peer),
                device_id_type=MESH,
            )
        )
    copies.append(
        pltpu.make_async_copy(source.at[item, head], target.at[head, item], own_sem.at[item])
    )
    return copies


def swap_step(source, target, send_sem, recv_sem, own_sem):
    item = pl.program_id(0)
    for copy in swap(source, target, send_sem, recv_sem, own_sem, item):
        copy.start()

    @pl.when(item == pl.num_programs(0) - 1)
    def _():
        for number in range(source.shape[0]):
            for copy in swap(source, target, send_sem, recv_sem, own_sem, number):
                copy.wait()


def swap_scratch(items, head_size, tokens, columns):
    return [
        pltpu.VMEM((items, head_size, tokens, columns), jnp.bfloat16),
        pltpu.SemaphoreType.DMA((items, head_size)),
        pltpu.SemaphoreType.DMA((items, head_size)),
        pltpu.SemaphoreType.DMA((items,)),
    ]


def forward_kernel(
    x_ref, w_ref, b_ref, qkv_ref, ctx_out, lse_ref, ctx_ref, send_sem, recv_sem, own_sem
):
    item = pl.program_id(0)

    @pl.when(item == 0)
    def _():
        greet_head(ctx_ref.shape[1])

    head_size, tokens, width = x_ref.shape[0], x_ref.shape[1], x_ref.shape[2]
    length = head_size * tokens
    cols = w_ref.shape[1] // 3
    rows = x_ref[...].reshape(length, width)
    qkv_ref[...] = (contract(rows, w_ref[...], 1, 0) + b_ref[...]).astype(jnp.bfloat16)
    step = min(QUERIES, tokens)
    for number in range(cols // HD):
        low = number * HD
        keys = qkv_ref[:, cols + low : cols + low + HD]
        values = qkv_ref[:, 2 * cols + low : 2 * cols + low + HD]
        for begin in range(0, length, step):
            query = qkv_ref[begin : begin + step, low : low + HD] * jnp.bfloat16(SCALE)
            scores = contract(keys, query, 1, 1)
            highest = jnp.max(scores, axis=0, keepdims=True)
            weights = jnp.exp(scores - highest)
            summed = jnp.sum(weights, axis=0, keepdims=True)
            probs = (weights * (1.0 / summed)).astype(jnp.bfloat16)
            context = contract(values, probs, 0, 0).T.astype(jnp.bfloat16)
            ctx_ref[item, begin // tokens, pl.ds(begin % tokens, step), low : low + HD] = context
            lse_ref[number : number + 1, begin : begin + step] = highest + jnp.log(summed)
    swap_step(ctx_ref, ctx_out, send_sem, recv_sem, own_sem)


def attend(inputs_full, weights, bias):
    seq_local, head_size, tokens, width = inputs_full.shape
    length = head_size * tokens
    cols = weights.shape[1] // 3
    return pl.pallas_call(
        forward_kernel,
        grid=(seq_local,),
        out_shape=(
            jax.ShapeDtypeStruct((seq_local, length, 3 * cols), jnp.bfloat16),
            jax.ShapeDtypeStruct((head_size, seq_local, tokens, cols), jnp.bfloat16),
            jax.ShapeDtypeStruct((seq_local, 8, length), jnp.float32),
        ),
        in_specs=[
            pl.BlockSpec((None, head_size, tokens, width), lambda s: (s, 0, 0, 0)),
            pl.BlockSpec((width, 3 * cols), lambda s: (0, 0)),
            pl.BlockSpec((1, 3 * cols), lambda s: (0, 0)),
        ],
        out_specs=(
            pl.BlockSpec((None, length, 3 * cols), lambda s: (s, 0, 0)),
            pl.BlockSpec(memory_space=pl.ANY),
            pl.BlockSpec((None, 8, length), lambda s: (s, 0, 0)),
        ),
        scratch_shapes=swap_scratch(seq_local, head_size, tokens, cols),
        compiler_params=pltpu.CompilerParams(
            collective_id=2, has_side_effects=True, vmem_limit_bytes=48 * 1024 * 1024
        ),
        name="attend",
    )(inputs_full, weights, bias)


def backward_kernel(
    da_ref,
    wo_ref,
    w_ref,
    lse_ref,
    dz_ref,
    df_ref,
    yb_ref,
    ctx_ref,
    h_any,
    du_any,
    x_any,
    qkv_any,
    blocks_ref,
    db_ref,
    grad_ref,
    h_ref,
    du_ref,
    x_ref,
    qkv_ref,
    load_sem,
    dall,
    acc,
    dw_ref,
    dctx_src,
    dctx_send,
    dctx_recv,
    dctx_own,
    d_src,
    d_send,
    d_recv,
    d_own,
    dctx_got,
    d_got,
):
    loads = [
        pltpu.make_async_copy(source, target, load_sem.at[number])
        for number, (source, target) in enumerate(
            [(h_any, h_ref), (du_any, du_ref), (qkv_any, qkv_ref), (x_any, x_ref)]
        )
    ]
    for load in loads:
        load.start()
    head_size, items, tokens, cols = ctx_ref.shape
    width = yb_ref.shape[1]
    hidden = h_ref.shape[1]
    length = head_size * tokens
    across = width // BLK
    greet_head(head_size)

    def dctx_swap(item):
        return swap(dctx_src, dctx_got, dctx_send, dctx_recv, dctx_own, item)

    def d_swap(item):
        return swap(d_src, d_got, d_send, d_recv, d_own, item)

    for item in range(items):
        dctx = contract(da_ref[item * tokens : (item + 1) * tokens], wo_ref[...], 1, 1)
        for head in range(head_size):
            dctx_src[item, head] = dctx[:, head * cols : (head + 1) * cols].astype(jnp.bfloat16)
        for copy in dctx_swap(item):
            copy.start()

    first = 3 * across * across
    for head in range(head_size):
        value = contract(ctx_ref[head].reshape(items * tokens, cols), da_ref[...], 0, 0)
        value = value.astype(jnp.bfloat16)
        for begin in range(0, cols, min(cols, BLK)):
            row = head * cols + begin
            part = min(cols, BLK)
            for col in range(across):
                number = first + (row // BLK) * across + col
                blocks_ref[number, row % BLK : row % BLK + part] = value[
                    begin : begin + part, col * BLK : (col + 1) * BLK
                ]
    first = 4 * across * across
    wide = hidden // BLK
    loads[1].wait()

    def up_part(turn, carry):
        span = pl.ds(pl.multiple_of(turn * width, width), width)
        value = contract(yb_ref[...], du_ref[:, span], 0, 0).astype(jnp.bfloat16)
        for row in range(across):
            for col in range(across):
                blocks_ref[first + row * wide + turn * across + col] = value[
                    row * BLK : (row + 1) * BLK, col * BLK : (col + 1) * BLK
                ]
        return carry

    lax.fori_loop(0, hidden // width, up_part, 0)
    loads[0].wait()
    second = first + across * wide

    def down_part(turn, carry):
        span = pl.ds(pl.multiple_of(turn * width, width), width)
        value = contract(h_ref[:, span], df_ref[...], 0, 0).astype(jnp.bfloat16)
        for row in range(across):
            for col in range(across):
                blocks_ref[second + (turn * across + row) * across + col] = value[
                    row * BLK : (row + 1) * BLK, col * BLK : (col + 1) * BLK
                ]
        return carry

    lax.fori_loop(0, hidden // width, down_part, 0)
    dw_ref[...] = jnp.zeros_like(dw_ref)
    db_ref[...] = jnp.zeros_like(db_ref)
    loads[2].wait()
    loads[3].wait()
    step = min(QUERIES, tokens)
    scale = jnp.bfloat16(SCALE)

    def attend_item(item, carry):
        for copy in dctx_swap(item):
            copy.wait()
        for number in range(cols // HD):
            low = number * HD
            keys = qkv_ref[item, :, cols + low : cols + low + HD]
            values = qkv_ref[item, :, 2 * cols + low : 2 * cols + low + HD]
            for begin in range(0, length, step):
                query = qkv_ref[item, begin : begin + step, low : low + HD] * scale
                dctx = dctx_got[
                    begin // tokens, item, pl.ds(begin % tokens, step), low : low + HD
                ]
                scores = contract(keys, query, 1, 1)
                probs = jnp.exp(scores - lse_ref[item, number : number + 1, begin : begin + step])
                dprobs = contract(values, dctx, 1, 1)
                inner = jnp.sum(probs * dprobs, axis=0, keepdims=True)
                dscores = (probs * (dprobs - inner)).astype(jnp.bfloat16)
                dkey = contract(dscores, query, 1, 0)
                dvalue = contract(probs.astype(jnp.bfloat16), dctx, 1, 0)
                if begin == 0:
                    acc[0] = dkey
                    acc[1] = dvalue
                else:
                    acc[0] += dkey
                    acc[1] += dvalue
                dquery = contract(keys, dscores, 0, 0).T * SCALE
                dall[begin : begin + step, low : low + HD] = dquery.astype(jnp.bfloat16)
            dall[:, cols + low : cols + low + HD] = acc[0].astype(jnp.bfloat16)
            dall[:, 2 * cols + low : 2 * cols + low + HD] = acc[1].astype(jnp.bfloat16)
        delta = dall[...]
        d_src[item] = delta.reshape(head_size, tokens, 3 * cols)
        for copy in d_swap(item):
            copy.start()
        dw_ref[...] += contract(x_ref[item].reshape(length, width), delta, 0, 0)
        db_ref[...] += jnp.sum(delta.astype(jnp.float32), axis=0, keepdims=True)
        return carry

    lax.fori_loop(0, items, attend_item, 0)

    head_me = lax.axis_index("head")
    for number in range(3):
        value = dw_ref[:, number * cols : (number + 1) * cols].astype(jnp.bfloat16)
        for row in range(across):
            for col in range(across):
                rows = value[row * BLK : (row + 1) * BLK]
                parts = []
                for begin in range(0, BLK, min(cols, BLK)):
                    lane = col * BLK + begin
                    begin_own = lane % cols
                    part = rows[:, begin_own : begin_own + min(cols, BLK)]
                    parts.append(jnp.where(head_me == lane // cols, part, jnp.zeros_like(part)))
                whole = parts[0] if len(parts) == 1 else jnp.concatenate(parts, 1)
                blocks_ref[number * across * across + row * across + col] = whole

    def input_item(item, carry):
        for copy in d_swap(item):
            copy.wait()
        span = pl.ds(pl.multiple_of(item * tokens, tokens), tokens)
        total = dz_ref[span]
        for head in range(head_size):
            total = total + contract(d_got[head, item], w_ref[head], 1, 1)
        grad_ref[item] = total
        return carry

    lax.fori_loop(0, items, input_item, 0)


def backward(d_branch, w_out, w_qkv, lse, d_zone, d_ffn, first_low, context, hidden, d_hidden, inputs_full, qkv):
    head_size, seq_local, tokens, cols = context.shape
    width = w_out.shape[0]
    length = head_size * tokens
    whole = pl.BlockSpec(memory_space=pltpu.VMEM)
    any_space = pl.BlockSpec(memory_space=pl.ANY)

    def like(array):
        return pltpu.VMEM(array.shape, array.dtype)

    return pl.pallas_call(
        backward_kernel,
        out_shape=(
            jax.ShapeDtypeStruct((NBLK, BLK, BLK), jnp.bfloat16),
            jax.ShapeDtypeStruct((1, 3 * cols), jnp.float32),
            jax.ShapeDtypeStruct((seq_local, tokens, width), jnp.float32),
        ),
        in_specs=[whole] * 8 + [any_space] * 4,
        out_specs=(whole, whole, whole),
        scratch_shapes=[
            like(hidden),
            like(d_hidden),
            like(inputs_full),
            like(qkv),
            pltpu.SemaphoreType.DMA((4,)),
            pltpu.VMEM((length, 3 * cols), jnp.bfloat16),
            pltpu.VMEM((2, length, HD), jnp.float32),
            pltpu.VMEM((width, 3 * cols), jnp.float32),
        ]
        + swap_scratch(seq_local, head_size, tokens, cols)
        + swap_scratch(seq_local, head_size, tokens, 3 * cols)
        + [
            pltpu.VMEM((head_size, seq_local, tokens, cols), jnp.bfloat16),
            pltpu.VMEM((head_size, seq_local, tokens, 3 * cols), jnp.bfloat16),
        ],
        compiler_params=pltpu.CompilerParams(
            collective_id=4, has_side_effects=True, vmem_limit_bytes=60 * 1024 * 1024
        ),
        name="backward",
    )(
        d_branch,
        w_out,
        w_qkv,
        lse,
        d_zone,
        d_ffn,
        first_low,
        context,
        hidden,
        d_hidden,
        inputs_full,
        qkv,
    )


def rotate_adam(grads, master, moment_one, moment_two, basis_left, basis_right):
    rotated = jnp.einsum("sji,sjk->sik", basis_left, grads, precision=HIGH)
    rotated = jnp.einsum("sik,skl->sil", rotated, basis_right, precision=HIGH)
    first = 0.5 * moment_one + 0.5 * rotated
    second = 0.5 * moment_two + 0.5 * rotated * rotated
    correct = 1.0 - 0.5**STEP
    normed = first / correct / (jnp.sqrt(second / correct) + ADAM_EPS)
    turned = jnp.einsum("sij,sjk->sik", basis_left, normed, precision=HIGH)
    turned = jnp.einsum("sik,slk->sil", turned, basis_right, precision=HIGH)
    updated = master - RATE * (turned + DECAY * master)
    return (first, second, updated)


def back_product(grads, weight):
    return jnp.einsum("to,io->ti", grads, weight, preferred_element_type=jnp.float32)


MESH = pl.DeviceIdType.MESH
VEC_ROWS = 16
PIECE = 16


def cut(seq_size, head_size):
    cores = 2 if head_size % 2 == 0 else 1
    rows = 1
    while 2 * (rows * 2) ** 2 <= seq_size and seq_size % (rows * 2) == 0:
        rows = rows * 2
    return (seq_size // rows, rows, head_size // cores, cores)


def place(dims):
    size_z, size_x, size_y, size_c = dims
    seq = lax.axis_index("seq")
    head = lax.axis_index("head")
    return (
        lax.div(seq, size_x),
        lax.rem(seq, size_x),
        lax.div(head, size_c),
        lax.rem(head, size_c),
    )


def device(dims, coords):
    return (coords[0] * dims[1] + coords[1], coords[2] * dims[3] + coords[3])


def flat(dims, coords):
    return ((coords[0] * dims[1] + coords[1]) * dims[2] + coords[2]) * dims[3] + coords[3]


def moved(dims, coords, axis, step):
    new = list(coords)
    new[axis] = lax.rem(coords[axis] + step, dims[axis])
    return tuple(new)


def greet(dims, coords):
    barrier = pltpu.get_barrier_semaphore()
    count = 0
    for axis in range(4):
        for step in range(1, dims[axis]):
            pl.semaphore_signal(
                barrier,
                inc=1,
                device_id=device(dims, moved(dims, coords, axis, step)),
                device_id_type=MESH,
            )
            count = count + 1
    pl.semaphore_wait(barrier, count)


def greet_head(head_size):
    barrier = pltpu.get_barrier_semaphore()
    seq = lax.axis_index("seq")
    head = lax.axis_index("head")
    for step in range(1, head_size):
        pl.semaphore_signal(
            barrier, inc=1, device_id=(seq, lax.rem(head + step, head_size)), device_id_type=MESH
        )
    pl.semaphore_wait(barrier, head_size - 1)


def gather_kernel(
    dims,
    inv_ref,
    x_ref,
    w_ref,
    xf_ref,
    qkv_ref,
    out_ref,
    up_ref,
    down_ref,
    vec_ref,
    wf_ref,
    own_sem,
    x_send,
    x_recv,
    w_send,
    w_recv,
):
    me = place(dims)
    size_z, size_x, size_y, size_c = dims
    head_me = me[2] * size_c + me[3]
    chunk = w_ref.shape[0]

    def spot(index):
        return wf_ref.at[pl.ds(index * chunk, chunk)]

    own_x = pltpu.make_async_copy(x_ref, xf_ref.at[:, head_me], own_sem.at[0])
    own_w = pltpu.make_async_copy(w_ref, spot(flat(dims, me)), own_sem.at[1])
    own_x.start()
    own_w.start()
    greet(dims, me)
    started = []

    def send_x(source, head, target, number):
        copy = pltpu.make_async_remote_copy(
            src_ref=source,
            dst_ref=xf_ref.at[:, head],
            send_sem=x_send.at[number],
            recv_sem=x_recv.at[head],
            device_id=device(dims, target),
            device_id_type=MESH,
        )
        copy.start()
        started.append(copy)

    def arrived_x(head):
        pltpu.make_async_remote_copy(
            src_ref=x_ref,
            dst_ref=xf_ref.at[:, head],
            send_sem=x_send.at[0],
            recv_sem=x_recv.at[head],
            device_id=device(dims, me),
            device_id_type=MESH,
        ).wait_recv()

    count = [0]

    def send_w(source, index, target):
        number = count[0]
        count[0] = number + 1
        copy = pltpu.make_async_remote_copy(
            src_ref=source,
            dst_ref=spot(index),
            send_sem=w_send.at[number],
            recv_sem=w_recv.at[index],
            device_id=device(dims, target),
            device_id_type=MESH,
        )
        copy.start()
        started.append(copy)

    def arrived_w(index):
        pltpu.make_async_remote_copy(
            src_ref=w_ref,
            dst_ref=spot(index),
            send_sem=w_send.at[0],
            recv_sem=w_recv.at[index],
            device_id=device(dims, me),
            device_id_type=MESH,
        ).wait_recv()

    order = [0, 2, 1, 3]

    def forward(source, coords, after):
        for axis in order[after:]:
            for step in range(1, dims[axis]):
                send_w(source, flat(dims, coords), moved(dims, me, axis, step))

    number = 0
    for step in range(1, size_y):
        send_x(x_ref, head_me, moved(dims, me, 2, step), number)
        number = number + 1
    for step in range(1, size_c):
        send_x(x_ref, head_me, moved(dims, me, 3, step), number)
        number = number + 1
    forward(w_ref, me, 0)
    held = [me]
    for level in range(3):
        axis = order[level]
        fresh = []
        for step in range(1, dims[axis]):
            for coords in held:
                source = moved(dims, coords, axis, step)
                arrived_w(flat(dims, source))
                forward(spot(flat(dims, source)), source, level + 1)
                fresh.append(source)
        held = held + fresh
        if level == 1:
            for step in range(1, size_y):
                other = moved(dims, me, 2, step)
                head = other[2] * size_c + other[3]
                arrived_x(head)
                for hop in range(1, size_c):
                    send_x(xf_ref.at[:, head], head, moved(dims, me, 3, hop), number)
                    number = number + 1
    for step in range(1, size_c):
        for coords in held:
            arrived_w(flat(dims, moved(dims, coords, 3, step)))
        for across in range(size_y):
            other = moved(dims, moved(dims, me, 3, step), 2, across)
            arrived_x(other[2] * size_c + other[3])
    for copy in started:
        copy.wait_send()
    own_x.wait()
    own_w.wait()
    unpack(dims, inv_ref, wf_ref, qkv_ref, out_ref, up_ref, down_ref)
    chunk = w_ref.shape[0]
    for number in range(vec_ref.shape[0]):
        vec_ref[number] = wf_ref[(number + 1) * chunk - 1]


def unpack(dims, inv_ref, wf_ref, qkv_ref, out_ref, up_ref, down_ref):
    head_size = dims[2] * dims[3]
    width = out_ref.shape[0]
    hidden = up_ref.shape[1]
    cols = width // head_size
    across = width // BLK

    def block(number):
        piece = inv_ref[number]
        return jnp.concatenate([wf_ref[piece + part] for part in range(BLK // PIECE)], 0)

    def rows_of(row_count, first, col_count, store):
        def one(row, carry):
            span = pl.ds(pl.multiple_of(row * BLK, BLK), BLK)
            for col in range(col_count):
                store(span, col, block(first + row * col_count + col))
            return carry

        lax.fori_loop(0, row_count, one, 0)

    for number in range(3):

        def store_qkv(span, col, value, number=number):
            for begin in range(0, BLK, min(cols, BLK)):
                head = (col * BLK + begin) // cols
                lane = (col * BLK + begin) % cols
                part = min(cols, BLK)
                qkv_ref[head, span, number * cols + lane : number * cols + lane + part] = value[
                    :, begin : begin + part
                ]

        rows_of(across, number * across * across, across, store_qkv)

    def store_in(ref):
        def store(span, col, value):
            ref[span, col * BLK : (col + 1) * BLK] = value

        return store

    rows_of(across, 3 * across * across, across, store_in(out_ref))
    first = 4 * across * across
    rows_of(across, first, hidden // BLK, store_in(up_ref))
    first = first + across * (hidden // BLK)
    rows_of(hidden // BLK, first, across, store_in(down_ref))


def gather_all(dims, inverse, inputs, packed):
    size_z, size_x, size_y, size_c = dims
    total = size_z * size_x * size_y * size_c
    head_size = size_y * size_c
    seq_local, tok_local, width = inputs.shape
    any_space = pl.BlockSpec(memory_space=pl.ANY)
    whole = pl.BlockSpec(memory_space=pltpu.VMEM)
    sends_x = (size_y - 1) * size_c + size_c - 1
    sends_w = (
        (size_z - 1)
        + size_z * (size_y - 1)
        + size_z * size_y * (size_x - 1)
        + size_z * size_y * size_x * (size_c - 1)
    )
    return pl.pallas_call(
        functools.partial(gather_kernel, dims),
        out_shape=(
            jax.ShapeDtypeStruct((seq_local, head_size, tok_local, width), inputs.dtype),
            jax.ShapeDtypeStruct((head_size, width, 3 * width // head_size), packed.dtype),
            jax.ShapeDtypeStruct((width, width), packed.dtype),
            jax.ShapeDtypeStruct((width, FF), packed.dtype),
            jax.ShapeDtypeStruct((FF, width), packed.dtype),
            jax.ShapeDtypeStruct((total, VEC_ROWS, BLK), packed.dtype),
        ),
        in_specs=[pl.BlockSpec(memory_space=pltpu.SMEM), whole, whole],
        out_specs=(any_space, whole, whole, whole, whole, whole),
        scratch_shapes=[
            pltpu.VMEM((total * packed.shape[0],) + packed.shape[1:], packed.dtype),
            pltpu.SemaphoreType.DMA((2,)),
            pltpu.SemaphoreType.DMA((max(sends_x, 1),)),
            pltpu.SemaphoreType.DMA((head_size,)),
            pltpu.SemaphoreType.DMA((max(sends_w, 1),)),
            pltpu.SemaphoreType.DMA((total,)),
        ],
        compiler_params=pltpu.CompilerParams(
            collective_id=0, has_side_effects=True, vmem_limit_bytes=40 * 1024 * 1024
        ),
        name="gather_all",
    )(inverse, inputs, packed)


def scatter_kernel(
    dims,
    slots,
    owner_ref,
    blocks_ref,
    vec_ref,
    grad_ref,
    vec_out_ref,
    term,
    got_c,
    got_x,
    got_y,
    got_z,
    send_c,
    send_x,
    send_y,
    send_z,
    recv_c,
    recv_x,
    recv_y,
    recv_z,
):
    me = place(dims)
    size_z, size_x, size_y, size_c = dims
    rows = slots * BLK
    greet(dims, me)

    def block_of(dest, slot):
        owner = owner_ref[dest * slots + slot]
        block = blocks_ref[jnp.minimum(owner, NBLK - 1)]
        return jnp.where(owner < NBLK, block, jnp.zeros_like(block))

    def total_of(dest, extras, keep_block, keep_vec):
        def one(slot, carry):
            value = block_of(dest, slot).astype(jnp.float32)
            span = pl.ds(pl.multiple_of(slot * BLK, BLK), BLK)
            for ref, lead in extras:
                value = value + ref[lead + (span,)].astype(jnp.float32)
            keep_block(slot, span, value)
            return carry

        lax.fori_loop(0, slots, one, 0)
        value = vec_ref[dest].astype(jnp.float32)
        for ref, lead in extras:
            value = value + ref[lead + (pl.ds(rows, VEC_ROWS),)].astype(jnp.float32)
        keep_vec(value)

    def into_term(dest, extras):
        def keep_block(slot, span, value):
            term[dest, span] = value.astype(jnp.bfloat16)

        def keep_vec(value):
            term[dest, pl.ds(rows, VEC_ROWS)] = value.astype(jnp.bfloat16)

        total_of(dest, extras, keep_block, keep_vec)

    def remote(dest, got, send, recv, hop, index, target):
        return pltpu.make_async_remote_copy(
            src_ref=term.at[dest],
            dst_ref=got.at[hop, index],
            send_sem=send.at[hop, index],
            recv_sem=recv.at[hop, index],
            device_id=device(dims, target),
            device_id_type=MESH,
        )

    def each(axis, begin, end, coords_of, extras_of, got, send, recv, only=None):
        for step in range(1, dims[axis]) if only is None else [only]:
            target = moved(dims, me, axis, step)

            def one(index, carry, step=step, target=target):
                coords = list(coords_of(index))
                coords[axis] = target[axis]
                dest = flat(dims, coords)
                into_term(dest, extras_of(coords))
                remote(dest, got, send, recv, step - 1, index, target).start()
                return carry

            if end == begin + 1:
                one(begin, 0)
            else:
                lax.fori_loop(begin, end, one, 0)

    def wait_for(axis, got, send, recv, index):
        found = []
        for step in range(1, dims[axis]):
            remote(0, got, send, recv, step - 1, index, moved(dims, me, axis, step)).wait_recv()
            found.append((got, (step - 1, index)))
        return found

    def turn_z(order):
        return lax.rem(me[0] + 1 + order, size_z)

    def order_z(coords):
        return lax.rem(coords[0] - me[0] + 2 * size_z - 1, size_z)

    def index_c(coords):
        order_x = lax.rem(coords[1] - me[1] + size_x - 1 + size_x, size_x)
        return (order_z(coords) * size_x + order_x) * size_y + coords[2]

    def coords_c(index):
        order_x = lax.rem(lax.div(index, size_y), size_x)
        return (
            turn_z(lax.div(index, size_x * size_y)),
            lax.rem(me[1] + 1 + order_x, size_x),
            lax.rem(index, size_y),
            me[3],
        )

    def coords_x(index):
        return (turn_z(lax.div(index, size_y)), me[1], lax.rem(index, size_y), me[3])

    def coords_y(index):
        return (turn_z(index), me[1], me[2], me[3])

    def coords_z(index):
        return me

    def extras_c(coords):
        return []

    def extras_x(coords):
        return wait_for(3, got_c, send_c, recv_c, index_c(coords))

    def extras_y(coords):
        return extras_x(coords) + wait_for(
            1, got_x, send_x, recv_x, order_z(coords) * size_y + coords[2]
        )

    def extras_z(coords):
        return extras_y(coords) + wait_for(2, got_y, send_y, recv_y, order_z(coords))

    def stage_c(order):
        group = size_x * size_y
        each(3, order * group, (order + 1) * group, coords_c, extras_c, got_c, send_c, recv_c)

    def stage_x(order):
        group = size_y
        each(1, order * group, (order + 1) * group, coords_x, extras_x, got_x, send_x, recv_x)

    stage_c(0)
    for order in range(1, size_z):
        stage_c(order)
        stage_x(order - 1)
    stage_x(size_z - 1)
    for order in range(size_z):
        each(2, order, order + 1, coords_y, extras_y, got_y, send_y, recv_y)
        if order + 1 < size_z:
            each(0, 0, 1, coords_z, extras_z, got_z, send_z, recv_z, only=order + 1)
    extras = extras_z(me) + wait_for(0, got_z, send_z, recv_z, 0)

    def keep_block(slot, span, value):
        grad_ref[slot] = value

    def keep_vec(value):
        vec_out_ref[...] = value

    total_of(flat(dims, me), extras, keep_block, keep_vec)

    def drain(axis, count, got, send, recv):
        for step in range(1, dims[axis]):

            def one(index, carry, step=step):
                remote(
                    0, got, send, recv, step - 1, index, moved(dims, me, axis, step)
                ).wait_send()
                return carry

            lax.fori_loop(0, count, one, 0)

    drain(3, size_z * size_x * size_y, got_c, send_c, recv_c)
    drain(1, size_z * size_y, got_x, send_x, recv_x)
    drain(2, size_z, got_y, send_y, recv_y)
    drain(0, 1, got_z, send_z, recv_z)


def scatter_sums(dims, owner_slot, blocks, vec_terms):
    size_z, size_x, size_y, size_c = dims
    total = size_z * size_x * size_y * size_c
    slots = owner_slot.shape[0] // total
    chunk = (slots * BLK + VEC_ROWS, BLK)
    shapes = [
        (max(size_c - 1, 1), size_z * size_x * size_y),
        (max(size_x - 1, 1), size_z * size_y),
        (max(size_y - 1, 1), size_z),
        (max(size_z - 1, 1), 1),
    ]
    whole = pl.BlockSpec(memory_space=pltpu.VMEM)
    return pl.pallas_call(
        functools.partial(scatter_kernel, dims, slots),
        out_shape=(
            jax.ShapeDtypeStruct((slots, BLK, BLK), jnp.float32),
            jax.ShapeDtypeStruct((VEC_ROWS, BLK), jnp.float32),
        ),
        in_specs=[pl.BlockSpec(memory_space=pltpu.SMEM), whole, whole],
        out_specs=(whole, whole),
        scratch_shapes=[pltpu.VMEM((total,) + chunk, jnp.bfloat16)]
        + [pltpu.VMEM(shape + chunk, jnp.bfloat16) for shape in shapes]
        + [pltpu.SemaphoreType.DMA(shape) for shape in shapes]
        + [pltpu.SemaphoreType.DMA(shape) for shape in shapes],
        compiler_params=pltpu.CompilerParams(
            collective_id=1, has_side_effects=True, vmem_limit_bytes=60 * 1024 * 1024
        ),
        name="scatter_sums",
    )(owner_slot, blocks, vec_terms)


def three_parts(values):
    high = lax.reduce_precision(values, 8, 7)
    rest = values - high
    middle = lax.reduce_precision(rest, 8, 7)
    low = lax.reduce_precision(rest - middle, 8, 7)
    return [part.astype(jnp.bfloat16) for part in (high, middle, low)]


def as_rows(vector, rows):
    return jnp.pad(vector, (0, rows * BLK - vector.shape[0])).reshape(rows, BLK)


def ceil_to(value, unit):
    return -(-value // unit) * unit


def body(
    inputs,
    cotangent,
    span_offset,
    span_len,
    owner_slot,
    master,
    moment_one,
    moment_two,
    basis_left,
    basis_right,
    average,
    vec_master,
    vec_moment_one,
    vec_moment_two,
):
    both = ("seq", "head")
    seq_size = lax.axis_size("seq")
    head_size = lax.axis_size("head")
    total = seq_size * head_size
    head_index = lax.axis_index("head")
    seq_local, tok_local, width = inputs.shape
    slots_local = master.shape[0]
    slot_total = slots_local * total
    vec_local = vec_master.shape[0]

    dims = cut(seq_size, head_size)

    packed = jnp.concatenate(
        [
            master.astype(jnp.bfloat16).reshape(slots_local * BLK, BLK),
            as_rows(jnp.concatenate(three_parts(vec_master)), VEC_ROWS),
        ],
        0,
    ).reshape(-1, PIECE, BLK)
    numbers = jnp.arange(slot_total, dtype=jnp.int32)
    inverse = jnp.sum(
        jnp.where(owner_slot[:, None] == numbers[None, :], numbers[:, None], 0), axis=0
    )
    pieces = (inverse // slots_local) * packed.shape[0]
    pieces = pieces + (inverse % slots_local) * (BLK // PIECE)
    inputs_full, w_qkv, w_out, w_up, w_down, vec_parts = gather_all(
        dims, pieces, inputs, packed
    )
    parts = (
        vec_parts
        .reshape(total, VEC_ROWS * BLK)[:, : 3 * vec_local]
        .reshape(total, 3, vec_local)
        .astype(jnp.float32)
    )
    all_vector = ((parts[:, 2] + parts[:, 1]) + parts[:, 0]).reshape(-1)

    b_query, b_value, b_out, gain_one, shift_one, b_up, b_down, gain_two, shift_two = split_vector(
        all_vector
    )
    token_rows = inputs.reshape(seq_local * tok_local, width)
    local_shape = (seq_local, tok_local, width)
    cols = width // head_size
    begin = head_index * cols

    def own(array):
        return lax.dynamic_slice_in_dim(array, begin, cols, array.ndim - 1)

    w_own = lax.dynamic_index_in_dim(w_qkv, head_index, 0, keepdims=False)
    b_own = jnp.concatenate([own(b_query), jnp.zeros((cols,), jnp.float32), own(b_value)], 0)
    qkv, context, log_total = attend(inputs_full, w_own, b_own[None, :])
    context_rows = context.transpose(1, 2, 0, 3).reshape(seq_local * tok_local, width)
    branch = jnp.dot(context_rows, w_out, preferred_element_type=jnp.float32) + b_out
    z_one = token_rows.astype(jnp.float32) + branch
    first = layer_norm(z_one, gain_one, shift_one)
    first_low = first.astype(jnp.bfloat16)
    hidden_in = jnp.dot(first_low, w_up, preferred_element_type=jnp.float32) + b_up
    hidden_act = gelu_value(hidden_in).astype(jnp.bfloat16)
    ffn_out = jnp.dot(hidden_act, w_down, preferred_element_type=jnp.float32) + b_down
    z_two = first + ffn_out
    result, pull_two = jax.vjp(layer_norm, z_two, gain_two, shift_two)
    layer_out = result.astype(jnp.bfloat16).reshape(local_shape)
    mask = span_mask(span_offset, span_len)
    grad_out = (cotangent.astype(jnp.float32) * mask[:, :, None]).reshape(
        seq_local * tok_local, width
    )
    d_ztwo, d_gain_two, d_shift_two = pull_two(grad_out)
    d_ffn = d_ztwo.astype(jnp.bfloat16)
    grad_bdown = jnp.sum(d_ffn.astype(jnp.float32), axis=0)
    d_hidden = back_product(d_ffn, w_down)
    d_hidden_in = (d_hidden * gelu_slope(hidden_in)).astype(jnp.bfloat16)
    grad_bup = jnp.sum(d_hidden_in.astype(jnp.float32), axis=0)
    d_first = d_ztwo + back_product(d_hidden_in, w_up)
    sink, pull_one = jax.vjp(layer_norm, z_one, gain_one, shift_one)
    d_zone, d_gain_one, d_shift_one = pull_one(d_first)
    d_branch = d_zone.astype(jnp.bfloat16)
    grad_bout = jnp.sum(d_branch.astype(jnp.float32), axis=0)

    blocks, grad_b_own, input_grad = backward(
        d_branch,
        w_out,
        w_qkv,
        log_total,
        d_zone,
        d_ffn,
        first_low,
        context,
        hidden_act,
        d_hidden_in,
        inputs_full,
        qkv,
    )
    grad_b_own = grad_b_own.reshape(-1)

    def put(array):
        empty = jnp.zeros(array.shape[:-1] + (width,), array.dtype)
        return lax.dynamic_update_slice_in_dim(empty, array, begin, array.ndim - 1)

    vector_terms = jnp.concatenate(
        [
            put(grad_b_own[:cols]),
            put(grad_b_own[2 * cols :]),
            grad_bout,
            d_gain_one,
            d_shift_one,
            grad_bup,
            grad_bdown,
            d_gain_two,
            d_shift_two,
        ],
        0,
    ).reshape(total, vec_local)
    vec_terms = jnp.pad(vector_terms, ((0, 0), (0, VEC_ROWS * BLK - vec_local)))
    vec_terms = vec_terms.astype(jnp.bfloat16).reshape(total, VEC_ROWS, BLK)
    slot_grad, vec_sums = scatter_sums(dims, owner_slot, blocks, vec_terms)
    vec_grad = vec_sums.reshape(-1)[:vec_local]
    first_moment, second_moment, updated = rotate_adam(
        slot_grad, master, moment_one, moment_two, basis_left, basis_right
    )
    correct = 1.0 - 0.5**STEP
    vec_first = 0.5 * vec_moment_one + 0.5 * vec_grad
    vec_second = 0.5 * vec_moment_two + 0.5 * vec_grad * vec_grad
    vec_new = vec_master - VEC_RATE * (vec_first / correct) / (
        jnp.sqrt(vec_second / correct) + ADAM_EPS
    )
    new_average = KEEP * average + (1.0 - KEEP) * updated
    return (
        layer_out,
        input_grad,
        slot_grad,
        vec_grad,
        first_moment,
        second_moment,
        updated,
        updated.astype(jnp.bfloat16),
        new_average,
        vec_first,
        vec_second,
        vec_new,
    )


def solution(mesh):
    placed = (
        P("seq", "head", None),
        P("seq", "head", None),
        P("seq", "head"),
        P("seq", "head"),
        P(),
        P(("seq", "head"), None, None),
        P(("seq", "head"), None, None),
        P(("seq", "head"), None, None),
        P(("seq", "head"), None, None),
        P(("seq", "head"), None, None),
        P(("seq", "head"), None, None),
        P(("seq", "head")),
        P(("seq", "head")),
        P(("seq", "head")),
    )
    return jax.shard_map(
        body,
        mesh=mesh,
        in_specs=placed,
        out_specs=(
            P("seq", "head", None),
            P("seq", "head", None),
            P(("seq", "head"), None, None),
            P(("seq", "head")),
            P(("seq", "head"), None, None),
            P(("seq", "head"), None, None),
            P(("seq", "head"), None, None),
            P(("seq", "head"), None, None),
            P(("seq", "head"), None, None),
            P(("seq", "head")),
            P(("seq", "head")),
            P(("seq", "head")),
        ),
        check_vma=False,
    )
```

```python
import functools
import math

import jax
import jax.numpy as jnp
from jax import lax
from jax.experimental import pallas as pl
from jax.experimental.pallas import tpu as pltpu
from jax.sharding import PartitionSpec as P

D = 512
FF = 2048
WIN = 16
BLK = 128
STEP = 5
HD = 64
NBLK = 192
QUERIES = 256
SCALE = 1.0 / math.sqrt(HD)


NORM_EPS = 1e-06
ADAM_EPS = 1e-08
RATE = 0.05
VEC_RATE = 0.2
DECAY = 0.01
KEEP = 0.9
HIGH = lax.Precision.HIGHEST


def split_vector(vector):
    widths = [D, D, D, D, D, FF, D, D, D]
    pieces = []
    offset = 0
    for extent in widths:
        pieces.append(vector[offset : offset + extent])
        offset = offset + extent
    return pieces


def layer_norm(values, gain, shift):
    center = values - jnp.mean(values, axis=-1, keepdims=True)
    spread = jnp.mean(center * center, axis=-1, keepdims=True)
    return center * lax.rsqrt(spread + NORM_EPS) * gain + shift


def gelu_value(values):
    return 0.5 * values * (1.0 + lax.erf(values * 0.7071067811865476))


def gelu_slope(values):
    return (
        0.5 * (1.0 + lax.erf(values * 0.7071067811865476))
        + values * jnp.exp(-0.5 * values * values) * 0.3989422804014327
    )


def span_mask(span_offset, span_len):
    offsets = jnp.repeat(span_offset, WIN, axis=1)
    extents = jnp.repeat(span_len, WIN, axis=1)
    within = (jnp.arange(offsets.shape[1], dtype=jnp.int32) % WIN)[None, :]
    return ((within >= offsets) & (within < offsets + extents)).astype(jnp.float32)


def contract(left, right, left_axis, right_axis):
    return lax.dot_general(
        left, right, (((left_axis,), (right_axis,)), ((), ())), preferred_element_type=jnp.float32
    )


def swap(source, target, send_sem, recv_sem, own_sem, item):
    head_size = source.shape[1]
    seq = lax.axis_index("seq")
    head = lax.axis_index("head")
    copies = []
    for step in [2, 1, 3] if head_size == 4 else range(1, head_size):
        peer = lax.rem(head + step, head_size)
        copies.append(
            pltpu.make_async_remote_copy(
                src_ref=source.at[item, peer],
                dst_ref=target.at[head, item],
                send_sem=send_sem.at[item, step],
                recv_sem=recv_sem.at[item, step],
                device_id=(seq, peer),
                device_id_type=MESH,
            )
        )
    copies.append(
        pltpu.make_async_copy(source.at[item, head], target.at[head, item], own_sem.at[item])
    )
    return copies


def swap_step(source, target, send_sem, recv_sem, own_sem):
    item = pl.program_id(0)
    for copy in swap(source, target, send_sem, recv_sem, own_sem, item):
        copy.start()

    @pl.when(item == pl.num_programs(0) - 1)
    def _():
        for number in range(source.shape[0]):
            for copy in swap(source, target, send_sem, recv_sem, own_sem, number):
                copy.wait()


def swap_scratch(items, head_size, tokens, columns):
    return [
        pltpu.VMEM((items, head_size, tokens, columns), jnp.bfloat16),
        pltpu.SemaphoreType.DMA((items, head_size)),
        pltpu.SemaphoreType.DMA((items, head_size)),
        pltpu.SemaphoreType.DMA((items,)),
    ]


def forward_kernel(
    x_ref, w_ref, b_ref, qkv_ref, ctx_out, lse_ref, ctx_ref, send_sem, recv_sem, own_sem
):
    item = pl.program_id(0)

    @pl.when(item == 0)
    def _():
        greet_head(ctx_ref.shape[1])

    head_size, tokens, width = x_ref.shape[0], x_ref.shape[1], x_ref.shape[2]
    length = head_size * tokens
    cols = w_ref.shape[1] // 3
    rows = x_ref[...].reshape(length, width)
    qkv_ref[...] = (contract(rows, w_ref[...], 1, 0) + b_ref[...]).astype(jnp.bfloat16)
    step = min(QUERIES, tokens)
    for number in range(cols // HD):
        low = number * HD
        keys = qkv_ref[:, cols + low : cols + low + HD]
        values = qkv_ref[:, 2 * cols + low : 2 * cols + low + HD]
        for begin in range(0, length, step):
            query = qkv_ref[begin : begin + step, low : low + HD] * jnp.bfloat16(SCALE)
            scores = contract(keys, query, 1, 1)
            highest = jnp.max(scores, axis=0, keepdims=True)
            weights = jnp.exp(scores - highest)
            summed = jnp.sum(weights, axis=0, keepdims=True)
            probs = (weights * (1.0 / summed)).astype(jnp.bfloat16)
            context = contract(values, probs, 0, 0).T.astype(jnp.bfloat16)
            ctx_ref[item, begin // tokens, pl.ds(begin % tokens, step), low : low + HD] = context
            lse_ref[number : number + 1, begin : begin + step] = highest + jnp.log(summed)
    swap_step(ctx_ref, ctx_out, send_sem, recv_sem, own_sem)


def attend(inputs_full, weights, bias):
    seq_local, head_size, tokens, width = inputs_full.shape
    length = head_size * tokens
    cols = weights.shape[1] // 3
    return pl.pallas_call(
        forward_kernel,
        grid=(seq_local,),
        out_shape=(
            jax.ShapeDtypeStruct((seq_local, length, 3 * cols), jnp.bfloat16),
            jax.ShapeDtypeStruct((head_size, seq_local, tokens, cols), jnp.bfloat16),
            jax.ShapeDtypeStruct((seq_local, 8, length), jnp.float32),
        ),
        in_specs=[
            pl.BlockSpec((None, head_size, tokens, width), lambda s: (s, 0, 0, 0)),
            pl.BlockSpec((width, 3 * cols), lambda s: (0, 0)),
            pl.BlockSpec((1, 3 * cols), lambda s: (0, 0)),
        ],
        out_specs=(
            pl.BlockSpec((None, length, 3 * cols), lambda s: (s, 0, 0)),
            pl.BlockSpec(memory_space=pl.ANY),
            pl.BlockSpec((None, 8, length), lambda s: (s, 0, 0)),
        ),
        scratch_shapes=swap_scratch(seq_local, head_size, tokens, cols),
        compiler_params=pltpu.CompilerParams(
            collective_id=2, has_side_effects=True, vmem_limit_bytes=48 * 1024 * 1024
        ),
        name="attend",
    )(inputs_full, weights, bias)


def backward_kernel(
    da_ref,
    wo_ref,
    w_ref,
    lse_ref,
    dz_ref,
    df_ref,
    yb_ref,
    ctx_ref,
    h_any,
    du_any,
    x_any,
    qkv_any,
    blocks_ref,
    db_ref,
    grad_ref,
    h_ref,
    du_ref,
    x_ref,
    qkv_ref,
    load_sem,
    dall,
    acc,
    dw_ref,
    dctx_src,
    dctx_send,
    dctx_recv,
    dctx_own,
    d_src,
    d_send,
    d_recv,
    d_own,
    dctx_got,
    d_got,
):
    loads = [
        pltpu.make_async_copy(source, target, load_sem.at[number])
        for number, (source, target) in enumerate(
            [(h_any, h_ref), (du_any, du_ref), (qkv_any, qkv_ref), (x_any, x_ref)]
        )
    ]
    for load in loads:
        load.start()
    head_size, items, tokens, cols = ctx_ref.shape
    width = yb_ref.shape[1]
    hidden = h_ref.shape[1]
    length = head_size * tokens
    across = width // BLK
    greet_head(head_size)

    def dctx_swap(item):
        return swap(dctx_src, dctx_got, dctx_send, dctx_recv, dctx_own, item)

    def d_swap(item):
        return swap(d_src, d_got, d_send, d_recv, d_own, item)

    for item in range(items):
        dctx = contract(da_ref[item * tokens : (item + 1) * tokens], wo_ref[...], 1, 1)
        for head in range(head_size):
            dctx_src[item, head] = dctx[:, head * cols : (head + 1) * cols].astype(jnp.bfloat16)
        for copy in dctx_swap(item):
            copy.start()

    first = 3 * across * across
    for head in range(head_size):
        value = contract(ctx_ref[head].reshape(items * tokens, cols), da_ref[...], 0, 0)
        value = value.astype(jnp.bfloat16)
        for begin in range(0, cols, min(cols, BLK)):
            row = head * cols + begin
            part = min(cols, BLK)
            for col in range(across):
                number = first + (row // BLK) * across + col
                blocks_ref[number, row % BLK : row % BLK + part] = value[
                    begin : begin + part, col * BLK : (col + 1) * BLK
                ]
    first = 4 * across * across
    wide = hidden // BLK
    loads[1].wait()

    def up_part(turn, carry):
        span = pl.ds(pl.multiple_of(turn * width, width), width)
        value = contract(yb_ref[...], du_ref[:, span], 0, 0).astype(jnp.bfloat16)
        for row in range(across):
            for col in range(across):
                blocks_ref[first + row * wide + turn * across + col] = value[
                    row * BLK : (row + 1) * BLK, col * BLK : (col + 1) * BLK
                ]
        return carry

    lax.fori_loop(0, hidden // width, up_part, 0)
    loads[0].wait()
    second = first + across * wide

    def down_part(turn, carry):
        span = pl.ds(pl.multiple_of(turn * width, width), width)
        value = contract(h_ref[:, span], df_ref[...], 0, 0).astype(jnp.bfloat16)
        for row in range(across):
            for col in range(across):
                blocks_ref[second + (turn * across + row) * across + col] = value[
                    row * BLK : (row + 1) * BLK, col * BLK : (col + 1) * BLK
                ]
        return carry

    lax.fori_loop(0, hidden // width, down_part, 0)
    dw_ref[...] = jnp.zeros_like(dw_ref)
    db_ref[...] = jnp.zeros_like(db_ref)
    loads[2].wait()
    loads[3].wait()
    step = min(QUERIES, tokens)
    scale = jnp.bfloat16(SCALE)

    def attend_item(item, carry):
        for copy in dctx_swap(item):
            copy.wait()
        for number in range(cols // HD):
            low = number * HD
            keys = qkv_ref[item, :, cols + low : cols + low + HD]
            values = qkv_ref[item, :, 2 * cols + low : 2 * cols + low + HD]
            for begin in range(0, length, step):
                query = qkv_ref[item, begin : begin + step, low : low + HD] * scale
                dctx = dctx_got[
                    begin // tokens, item, pl.ds(begin % tokens, step), low : low + HD
                ]
                scores = contract(keys, query, 1, 1)
                probs = jnp.exp(scores - lse_ref[item, number : number + 1, begin : begin + step])
                dprobs = contract(values, dctx, 1, 1)
                inner = jnp.sum(probs * dprobs, axis=0, keepdims=True)
                dscores = (probs * (dprobs - inner)).astype(jnp.bfloat16)
                dkey = contract(dscores, query, 1, 0)
                dvalue = contract(probs.astype(jnp.bfloat16), dctx, 1, 0)
                if begin == 0:
                    acc[0] = dkey
                    acc[1] = dvalue
                else:
                    acc[0] += dkey
                    acc[1] += dvalue
                dquery = contract(keys, dscores, 0, 0).T * SCALE
                dall[begin : begin + step, low : low + HD] = dquery.astype(jnp.bfloat16)
            dall[:, cols + low : cols + low + HD] = acc[0].astype(jnp.bfloat16)
            dall[:, 2 * cols + low : 2 * cols + low + HD] = acc[1].astype(jnp.bfloat16)
        delta = dall[...]
        d_src[item] = delta.reshape(head_size, tokens, 3 * cols)
        for copy in d_swap(item):
            copy.start()
        dw_ref[...] += contract(x_ref[item].reshape(length, width), delta, 0, 0)
        db_ref[...] += jnp.sum(delta.astype(jnp.float32), axis=0, keepdims=True)
        return carry

    lax.fori_loop(0, items, attend_item, 0)

    head_me = lax.axis_index("head")
    for number in range(3):
        value = dw_ref[:, number * cols : (number + 1) * cols].astype(jnp.bfloat16)
        for row in range(across):
            for col in range(across):
                rows = value[row * BLK : (row + 1) * BLK]
                parts = []
                for begin in range(0, BLK, min(cols, BLK)):
                    lane = col * BLK + begin
                    begin_own = lane % cols
                    part = rows[:, begin_own : begin_own + min(cols, BLK)]
                    parts.append(jnp.where(head_me == lane // cols, part, jnp.zeros_like(part)))
                whole = parts[0] if len(parts) == 1 else jnp.concatenate(parts, 1)
                blocks_ref[number * across * across + row * across + col] = whole

    def input_item(item, carry):
        for copy in d_swap(item):
            copy.wait()
        span = pl.ds(pl.multiple_of(item * tokens, tokens), tokens)
        total = dz_ref[span]
        for head in range(head_size):
            total = total + contract(d_got[head, item], w_ref[head], 1, 1)
        grad_ref[item] = total
        return carry

    lax.fori_loop(0, items, input_item, 0)


def backward(d_branch, w_out, w_qkv, lse, d_zone, d_ffn, first_low, context, hidden, d_hidden, inputs_full, qkv):
    head_size, seq_local, tokens, cols = context.shape
    width = w_out.shape[0]
    length = head_size * tokens
    whole = pl.BlockSpec(memory_space=pltpu.VMEM)
    any_space = pl.BlockSpec(memory_space=pl.ANY)

    def like(array):
        return pltpu.VMEM(array.shape, array.dtype)

    return pl.pallas_call(
        backward_kernel,
        out_shape=(
            jax.ShapeDtypeStruct((NBLK, BLK, BLK), jnp.bfloat16),
            jax.ShapeDtypeStruct((1, 3 * cols), jnp.float32),
            jax.ShapeDtypeStruct((seq_local, tokens, width), jnp.float32),
        ),
        in_specs=[whole] * 8 + [any_space] * 4,
        out_specs=(whole, whole, whole),
        scratch_shapes=[
            like(hidden),
            like(d_hidden),
            like(inputs_full),
            like(qkv),
            pltpu.SemaphoreType.DMA((4,)),
            pltpu.VMEM((length, 3 * cols), jnp.bfloat16),
            pltpu.VMEM((2, length, HD), jnp.float32),
            pltpu.VMEM((width, 3 * cols), jnp.float32),
        ]
        + swap_scratch(seq_local, head_size, tokens, cols)
        + swap_scratch(seq_local, head_size, tokens, 3 * cols)
        + [
            pltpu.VMEM((head_size, seq_local, tokens, cols), jnp.bfloat16),
            pltpu.VMEM((head_size, seq_local, tokens, 3 * cols), jnp.bfloat16),
        ],
        compiler_params=pltpu.CompilerParams(
            collective_id=4, has_side_effects=True, vmem_limit_bytes=60 * 1024 * 1024
        ),
        name="backward",
    )(
        d_branch,
        w_out,
        w_qkv,
        lse,
        d_zone,
        d_ffn,
        first_low,
        context,
        hidden,
        d_hidden,
        inputs_full,
        qkv,
    )


def high_product(left, right, left_axis, right_axis):
    return lax.dot_general(
        left,
        right,
        (((left_axis,), (right_axis,)), ((), ())),
        precision=HIGH,
        preferred_element_type=jnp.float32,
    )


def adam_kernel(
    grad_ref,
    master_ref,
    one_ref,
    two_ref,
    left_ref,
    right_ref,
    average_ref,
    new_one_ref,
    new_two_ref,
    new_master_ref,
    new_short_ref,
    new_average_ref,
):
    slots = range(grad_ref.shape[0])
    correct = 1.0 - 0.5**STEP
    rotated = [high_product(left_ref[slot], grad_ref[slot], 0, 0) for slot in slots]
    rotated = [high_product(rotated[slot], right_ref[slot], 1, 0) for slot in slots]
    normed = []
    for slot in slots:
        first = 0.5 * one_ref[slot] + 0.5 * rotated[slot]
        second = 0.5 * two_ref[slot] + 0.5 * rotated[slot] * rotated[slot]
        new_one_ref[slot] = first
        new_two_ref[slot] = second
        normed.append(first / correct / (jnp.sqrt(second / correct) + ADAM_EPS))
    turned = [high_product(left_ref[slot], normed[slot], 1, 0) for slot in slots]
    turned = [high_product(turned[slot], right_ref[slot], 1, 1) for slot in slots]
    for slot in slots:
        updated = master_ref[slot] - RATE * (turned[slot] + DECAY * master_ref[slot])
        new_master_ref[slot] = updated
        new_short_ref[slot] = updated.astype(jnp.bfloat16)
        new_average_ref[slot] = KEEP * average_ref[slot] + (1.0 - KEEP) * updated


def adam(grads, master, moment_one, moment_two, basis_left, basis_right, average):
    slots = grads.shape[0]
    together = math.gcd(slots, 4)
    spec = pl.BlockSpec((together, BLK, BLK), lambda s: (s, 0, 0))
    full = jax.ShapeDtypeStruct(grads.shape, jnp.float32)
    return pl.pallas_call(
        adam_kernel,
        grid=(slots // together,),
        out_shape=(full, full, full, jax.ShapeDtypeStruct(grads.shape, jnp.bfloat16), full),
        in_specs=[spec] * 7,
        out_specs=(spec,) * 5,
        name="adam",
    )(grads, master, moment_one, moment_two, basis_left, basis_right, average)


def back_product(grads, weight):
    return jnp.einsum("to,io->ti", grads, weight, preferred_element_type=jnp.float32)


MESH = pl.DeviceIdType.MESH
VEC_ROWS = 16
PIECE = 16


def cut(seq_size, head_size):
    cores = 2 if head_size % 2 == 0 else 1
    rows = 1
    while 2 * (rows * 2) ** 2 <= seq_size and seq_size % (rows * 2) == 0:
        rows = rows * 2
    return (seq_size // rows, rows, head_size // cores, cores)


def place(dims):
    size_z, size_x, size_y, size_c = dims
    seq = lax.axis_index("seq")
    head = lax.axis_index("head")
    return (
        lax.div(seq, size_x),
        lax.rem(seq, size_x),
        lax.div(head, size_c),
        lax.rem(head, size_c),
    )


def device(dims, coords):
    return (coords[0] * dims[1] + coords[1], coords[2] * dims[3] + coords[3])


def flat(dims, coords):
    return ((coords[0] * dims[1] + coords[1]) * dims[2] + coords[2]) * dims[3] + coords[3]


def moved(dims, coords, axis, step):
    new = list(coords)
    new[axis] = lax.rem(coords[axis] + step, dims[axis])
    return tuple(new)


def greet(dims, coords):
    barrier = pltpu.get_barrier_semaphore()
    count = 0
    for axis in range(4):
        for step in range(1, dims[axis]):
            pl.semaphore_signal(
                barrier,
                inc=1,
                device_id=device(dims, moved(dims, coords, axis, step)),
                device_id_type=MESH,
            )
            count = count + 1
    pl.semaphore_wait(barrier, count)


def greet_head(head_size):
    barrier = pltpu.get_barrier_semaphore()
    seq = lax.axis_index("seq")
    head = lax.axis_index("head")
    for step in range(1, head_size):
        pl.semaphore_signal(
            barrier, inc=1, device_id=(seq, lax.rem(head + step, head_size)), device_id_type=MESH
        )
    pl.semaphore_wait(barrier, head_size - 1)


def gather_kernel(
    dims,
    inv_ref,
    x_ref,
    w_ref,
    xf_ref,
    qkv_ref,
    out_ref,
    up_ref,
    down_ref,
    vec_ref,
    wf_ref,
    own_sem,
    x_send,
    x_recv,
    w_send,
    w_recv,
):
    me = place(dims)
    size_z, size_x, size_y, size_c = dims
    head_me = me[2] * size_c + me[3]
    chunk = w_ref.shape[0]

    def spot(index):
        return wf_ref.at[pl.ds(index * chunk, chunk)]

    own_x = pltpu.make_async_copy(x_ref, xf_ref.at[:, head_me], own_sem.at[0])
    own_w = pltpu.make_async_copy(w_ref, spot(flat(dims, me)), own_sem.at[1])
    own_x.start()
    own_w.start()
    greet(dims, me)
    started = []

    def send_x(source, head, target, number):
        copy = pltpu.make_async_remote_copy(
            src_ref=source,
            dst_ref=xf_ref.at[:, head],
            send_sem=x_send.at[number],
            recv_sem=x_recv.at[head],
            device_id=device(dims, target),
            device_id_type=MESH,
        )
        copy.start()
        started.append(copy)

    def arrived_x(head):
        pltpu.make_async_remote_copy(
            src_ref=x_ref,
            dst_ref=xf_ref.at[:, head],
            send_sem=x_send.at[0],
            recv_sem=x_recv.at[head],
            device_id=device(dims, me),
            device_id_type=MESH,
        ).wait_recv()

    count = [0]

    def send_w(source, index, target):
        number = count[0]
        count[0] = number + 1
        copy = pltpu.make_async_remote_copy(
            src_ref=source,
            dst_ref=spot(index),
            send_sem=w_send.at[number],
            recv_sem=w_recv.at[index],
            device_id=device(dims, target),
            device_id_type=MESH,
        )
        copy.start()
        started.append(copy)

    def arrived_w(index):
        pltpu.make_async_remote_copy(
            src_ref=w_ref,
            dst_ref=spot(index),
            send_sem=w_send.at[0],
            recv_sem=w_recv.at[index],
            device_id=device(dims, me),
            device_id_type=MESH,
        ).wait_recv()

    order = [0, 2, 1, 3]

    def forward(source, coords, after):
        for axis in order[after:]:
            for step in range(1, dims[axis]):
                send_w(source, flat(dims, coords), moved(dims, me, axis, step))

    number = 0
    for step in range(1, size_y):
        send_x(x_ref, head_me, moved(dims, me, 2, step), number)
        number = number + 1
    for step in range(1, size_c):
        send_x(x_ref, head_me, moved(dims, me, 3, step), number)
        number = number + 1
    forward(w_ref, me, 0)
    held = [me]
    for level in range(3):
        axis = order[level]
        fresh = []
        for step in range(1, dims[axis]):
            for coords in held:
                source = moved(dims, coords, axis, step)
                arrived_w(flat(dims, source))
                forward(spot(flat(dims, source)), source, level + 1)
                fresh.append(source)
        held = held + fresh
        if level == 1:
            for step in range(1, size_y):
                other = moved(dims, me, 2, step)
                head = other[2] * size_c + other[3]
                arrived_x(head)
                for hop in range(1, size_c):
                    send_x(xf_ref.at[:, head], head, moved(dims, me, 3, hop), number)
                    number = number + 1
    for step in range(1, size_c):
        for coords in held:
            arrived_w(flat(dims, moved(dims, coords, 3, step)))
        for across in range(size_y):
            other = moved(dims, moved(dims, me, 3, step), 2, across)
            arrived_x(other[2] * size_c + other[3])
    for copy in started:
        copy.wait_send()
    own_x.wait()
    own_w.wait()
    unpack(dims, inv_ref, wf_ref, qkv_ref, out_ref, up_ref, down_ref)
    chunk = w_ref.shape[0]
    for number in range(vec_ref.shape[0]):
        vec_ref[number] = wf_ref[(number + 1) * chunk - 1]


def unpack(dims, inv_ref, wf_ref, qkv_ref, out_ref, up_ref, down_ref):
    head_size = dims[2] * dims[3]
    width = out_ref.shape[0]
    hidden = up_ref.shape[1]
    cols = width // head_size
    across = width // BLK

    def block(number):
        piece = inv_ref[number]
        return jnp.concatenate([wf_ref[piece + part] for part in range(BLK // PIECE)], 0)

    def rows_of(row_count, first, col_count, store):
        def one(row, carry):
            span = pl.ds(pl.multiple_of(row * BLK, BLK), BLK)
            for col in range(col_count):
                store(span, col, block(first + row * col_count + col))
            return carry

        lax.fori_loop(0, row_count, one, 0)

    for number in range(3):

        def store_qkv(span, col, value, number=number):
            for begin in range(0, BLK, min(cols, BLK)):
                head = (col * BLK + begin) // cols
                lane = (col * BLK + begin) % cols
                part = min(cols, BLK)
                qkv_ref[head, span, number * cols + lane : number * cols + lane + part] = value[
                    :, begin : begin + part
                ]

        rows_of(across, number * across * across, across, store_qkv)

    def store_in(ref):
        def store(span, col, value):
            ref[span, col * BLK : (col + 1) * BLK] = value

        return store

    rows_of(across, 3 * across * across, across, store_in(out_ref))
    first = 4 * across * across
    rows_of(across, first, hidden // BLK, store_in(up_ref))
    first = first + across * (hidden // BLK)
    rows_of(hidden // BLK, first, across, store_in(down_ref))


def gather_all(dims, inverse, inputs, packed):
    size_z, size_x, size_y, size_c = dims
    total = size_z * size_x * size_y * size_c
    head_size = size_y * size_c
    seq_local, tok_local, width = inputs.shape
    any_space = pl.BlockSpec(memory_space=pl.ANY)
    whole = pl.BlockSpec(memory_space=pltpu.VMEM)
    sends_x = (size_y - 1) * size_c + size_c - 1
    sends_w = (
        (size_z - 1)
        + size_z * (size_y - 1)
        + size_z * size_y * (size_x - 1)
        + size_z * size_y * size_x * (size_c - 1)
    )
    return pl.pallas_call(
        functools.partial(gather_kernel, dims),
        out_shape=(
            jax.ShapeDtypeStruct((seq_local, head_size, tok_local, width), inputs.dtype),
            jax.ShapeDtypeStruct((head_size, width, 3 * width // head_size), packed.dtype),
            jax.ShapeDtypeStruct((width, width), packed.dtype),
            jax.ShapeDtypeStruct((width, FF), packed.dtype),
            jax.ShapeDtypeStruct((FF, width), packed.dtype),
            jax.ShapeDtypeStruct((total, VEC_ROWS, BLK), packed.dtype),
        ),
        in_specs=[pl.BlockSpec(memory_space=pltpu.SMEM), whole, whole],
        out_specs=(any_space, whole, whole, whole, whole, whole),
        scratch_shapes=[
            pltpu.VMEM((total * packed.shape[0],) + packed.shape[1:], packed.dtype),
            pltpu.SemaphoreType.DMA((2,)),
            pltpu.SemaphoreType.DMA((max(sends_x, 1),)),
            pltpu.SemaphoreType.DMA((head_size,)),
            pltpu.SemaphoreType.DMA((max(sends_w, 1),)),
            pltpu.SemaphoreType.DMA((total,)),
        ],
        compiler_params=pltpu.CompilerParams(
            collective_id=0, has_side_effects=True, vmem_limit_bytes=40 * 1024 * 1024
        ),
        name="gather_all",
    )(inverse, inputs, packed)


def scatter_kernel(
    dims,
    slots,
    owner_ref,
    blocks_ref,
    vec_ref,
    grad_ref,
    vec_out_ref,
    term,
    got_c,
    got_x,
    got_y,
    got_z,
    send_c,
    send_x,
    send_y,
    send_z,
    recv_c,
    recv_x,
    recv_y,
    recv_z,
):
    me = place(dims)
    size_z, size_x, size_y, size_c = dims
    rows = slots * BLK
    greet(dims, me)

    def block_of(dest, slot):
        owner = owner_ref[dest * slots + slot]
        block = blocks_ref[jnp.minimum(owner, NBLK - 1)]
        return jnp.where(owner < NBLK, block, jnp.zeros_like(block))

    def total_of(dest, extras, keep_block, keep_vec):
        def one(slot, carry):
            value = block_of(dest, slot).astype(jnp.float32)
            span = pl.ds(pl.multiple_of(slot * BLK, BLK), BLK)
            for ref, lead in extras:
                value = value + ref[lead + (span,)].astype(jnp.float32)
            keep_block(slot, span, value)
            return carry

        lax.fori_loop(0, slots, one, 0)
        value = vec_ref[dest].astype(jnp.float32)
        for ref, lead in extras:
            value = value + ref[lead + (pl.ds(rows, VEC_ROWS),)].astype(jnp.float32)
        keep_vec(value)

    def into_term(dest, extras):
        def keep_block(slot, span, value):
            term[dest, span] = value.astype(jnp.bfloat16)

        def keep_vec(value):
            term[dest, pl.ds(rows, VEC_ROWS)] = value.astype(jnp.bfloat16)

        total_of(dest, extras, keep_block, keep_vec)

    def remote(dest, got, send, recv, hop, index, target):
        return pltpu.make_async_remote_copy(
            src_ref=term.at[dest],
            dst_ref=got.at[hop, index],
            send_sem=send.at[hop, index],
            recv_sem=recv.at[hop, index],
            device_id=device(dims, target),
            device_id_type=MESH,
        )

    def each(axis, begin, end, coords_of, extras_of, got, send, recv, only=None):
        for step in range(1, dims[axis]) if only is None else [only]:
            target = moved(dims, me, axis, step)

            def one(index, carry, step=step, target=target):
                coords = list(coords_of(index))
                coords[axis] = target[axis]
                dest = flat(dims, coords)
                into_term(dest, extras_of(coords))
                remote(dest, got, send, recv, step - 1, index, target).start()
                return carry

            if end == begin + 1:
                one(begin, 0)
            else:
                lax.fori_loop(begin, end, one, 0)

    def wait_for(axis, got, send, recv, index):
        found = []
        for step in range(1, dims[axis]):
            remote(0, got, send, recv, step - 1, index, moved(dims, me, axis, step)).wait_recv()
            found.append((got, (step - 1, index)))
        return found

    def turned(axis, order):
        return lax.rem(me[axis] + 1 + order, dims[axis])

    def order_of(axis, coords):
        return lax.rem(coords[axis] - me[axis] + 2 * dims[axis] - 1, dims[axis])

    def index_c(coords):
        return (order_of(0, coords) * size_x + order_of(1, coords)) * size_y + order_of(2, coords)

    def coords_c(index):
        return (
            turned(0, lax.div(index, size_x * size_y)),
            turned(1, lax.rem(lax.div(index, size_y), size_x)),
            turned(2, lax.rem(index, size_y)),
            me[3],
        )

    def run(first, second):
        size_s = dims[second]

        def coords_f(index):
            coords = list(me)
            coords[0] = turned(0, lax.div(index, size_s))
            coords[second] = turned(second, lax.rem(index, size_s))
            return coords

        def coords_s(index):
            coords = list(me)
            coords[0] = turned(0, index)
            return coords

        def coords_z(index):
            return me

        def extras_c(coords):
            return []

        def extras_f(coords):
            return wait_for(3, got_c, send_c, recv_c, index_c(coords))

        def extras_s(coords):
            index = order_of(0, coords) * size_s + order_of(second, coords)
            return extras_f(coords) + wait_for(first, got_x, send_x, recv_x, index)

        def extras_z(coords):
            return extras_s(coords) + wait_for(
                second, got_y, send_y, recv_y, order_of(0, coords)
            )

        def stage_c(order):
            group = size_x * size_y
            each(3, order * group, (order + 1) * group, coords_c, extras_c, got_c, send_c, recv_c)

        def stage_f(order):
            group = size_s
            each(
                first, order * group, (order + 1) * group, coords_f, extras_f, got_x, send_x, recv_x
            )

        stage_c(0)
        for order in range(1, size_z):
            stage_c(order)
            stage_f(order - 1)
        stage_f(size_z - 1)
        for order in range(size_z):
            each(second, order, order + 1, coords_s, extras_s, got_y, send_y, recv_y)
            if order + 1 < size_z:
                each(0, 0, 1, coords_z, extras_z, got_z, send_z, recv_z, only=order + 1)
        extras = extras_z(me) + wait_for(0, got_z, send_z, recv_z, 0)

        def keep_block(slot, span, value):
            grad_ref[slot] = value

        def keep_vec(value):
            vec_out_ref[...] = value

        total_of(flat(dims, me), extras, keep_block, keep_vec)
        drain(3, size_z * size_x * size_y, got_c, send_c, recv_c)
        drain(first, size_z * size_s, got_x, send_x, recv_x)
        drain(second, size_z, got_y, send_y, recv_y)
        drain(0, 1, got_z, send_z, recv_z)

    def drain(axis, count, got, send, recv):
        for step in range(1, dims[axis]):

            def one(index, carry, step=step):
                remote(
                    0, got, send, recv, step - 1, index, moved(dims, me, axis, step)
                ).wait_send()
                return carry

            lax.fori_loop(0, count, one, 0)

    for core in range(size_c):

        @pl.when(me[3] == core)
        def _(core=core):
            run(1 + core % 2, 2 - core % 2)


def scatter_sums(dims, owner_slot, blocks, vec_terms):
    size_z, size_x, size_y, size_c = dims
    total = size_z * size_x * size_y * size_c
    slots = owner_slot.shape[0] // total
    chunk = (slots * BLK + VEC_ROWS, BLK)
    shapes = [
        (max(size_c - 1, 1), size_z * size_x * size_y),
        (max(size_x - 1, size_y - 1, 1), size_z * max(size_x, size_y)),
        (max(size_x - 1, size_y - 1, 1), size_z),
        (max(size_z - 1, 1), 1),
    ]
    whole = pl.BlockSpec(memory_space=pltpu.VMEM)
    return pl.pallas_call(
        functools.partial(scatter_kernel, dims, slots),
        out_shape=(
            jax.ShapeDtypeStruct((slots, BLK, BLK), jnp.float32),
            jax.ShapeDtypeStruct((VEC_ROWS, BLK), jnp.float32),
        ),
        in_specs=[pl.BlockSpec(memory_space=pltpu.SMEM), whole, whole],
        out_specs=(whole, whole),
        scratch_shapes=[pltpu.VMEM((total,) + chunk, jnp.bfloat16)]
        + [pltpu.VMEM(shape + chunk, jnp.bfloat16) for shape in shapes]
        + [pltpu.SemaphoreType.DMA(shape) for shape in shapes]
        + [pltpu.SemaphoreType.DMA(shape) for shape in shapes],
        compiler_params=pltpu.CompilerParams(
            collective_id=1, has_side_effects=True, vmem_limit_bytes=60 * 1024 * 1024
        ),
        name="scatter_sums",
    )(owner_slot, blocks, vec_terms)


def three_parts(values):
    high = lax.reduce_precision(values, 8, 7)
    rest = values - high
    middle = lax.reduce_precision(rest, 8, 7)
    low = lax.reduce_precision(rest - middle, 8, 7)
    return [part.astype(jnp.bfloat16) for part in (high, middle, low)]


def as_rows(vector, rows):
    return jnp.pad(vector, (0, rows * BLK - vector.shape[0])).reshape(rows, BLK)


def ceil_to(value, unit):
    return -(-value // unit) * unit


def body(
    inputs,
    cotangent,
    span_offset,
    span_len,
    owner_slot,
    master,
    moment_one,
    moment_two,
    basis_left,
    basis_right,
    average,
    vec_master,
    vec_moment_one,
    vec_moment_two,
):
    both = ("seq", "head")
    seq_size = lax.axis_size("seq")
    head_size = lax.axis_size("head")
    total = seq_size * head_size
    head_index = lax.axis_index("head")
    seq_local, tok_local, width = inputs.shape
    slots_local = master.shape[0]
    slot_total = slots_local * total
    vec_local = vec_master.shape[0]

    dims = cut(seq_size, head_size)

    packed = jnp.concatenate(
        [
            master.astype(jnp.bfloat16).reshape(slots_local * BLK, BLK),
            as_rows(jnp.concatenate(three_parts(vec_master)), VEC_ROWS),
        ],
        0,
    ).reshape(-1, PIECE, BLK)
    numbers = jnp.arange(slot_total, dtype=jnp.int32)
    inverse = jnp.sum(
        jnp.where(owner_slot[:, None] == numbers[None, :], numbers[:, None], 0), axis=0
    )
    pieces = (inverse // slots_local) * packed.shape[0]
    pieces = pieces + (inverse % slots_local) * (BLK // PIECE)
    inputs_full, w_qkv, w_out, w_up, w_down, vec_parts = gather_all(
        dims, pieces, inputs, packed
    )
    parts = (
        vec_parts
        .reshape(total, VEC_ROWS * BLK)[:, : 3 * vec_local]
        .reshape(total, 3, vec_local)
        .astype(jnp.float32)
    )
    all_vector = ((parts[:, 2] + parts[:, 1]) + parts[:, 0]).reshape(-1)

    b_query, b_value, b_out, gain_one, shift_one, b_up, b_down, gain_two, shift_two = split_vector(
        all_vector
    )
    token_rows = inputs.reshape(seq_local * tok_local, width)
    local_shape = (seq_local, tok_local, width)
    cols = width // head_size
    begin = head_index * cols

    def own(array):
        return lax.dynamic_slice_in_dim(array, begin, cols, array.ndim - 1)

    w_own = lax.dynamic_index_in_dim(w_qkv, head_index, 0, keepdims=False)
    b_own = jnp.concatenate([own(b_query), jnp.zeros((cols,), jnp.float32), own(b_value)], 0)
    qkv, context, log_total = attend(inputs_full, w_own, b_own[None, :])
    context_rows = context.transpose(1, 2, 0, 3).reshape(seq_local * tok_local, width)
    branch = jnp.dot(context_rows, w_out, preferred_element_type=jnp.float32) + b_out
    z_one = token_rows.astype(jnp.float32) + branch
    first = layer_norm(z_one, gain_one, shift_one)
    first_low = first.astype(jnp.bfloat16)
    hidden_in = jnp.dot(first_low, w_up, preferred_element_type=jnp.float32) + b_up
    hidden_act = gelu_value(hidden_in).astype(jnp.bfloat16)
    ffn_out = jnp.dot(hidden_act, w_down, preferred_element_type=jnp.float32) + b_down
    z_two = first + ffn_out
    result, pull_two = jax.vjp(layer_norm, z_two, gain_two, shift_two)
    layer_out = result.astype(jnp.bfloat16).reshape(local_shape)
    mask = span_mask(span_offset, span_len)
    grad_out = (cotangent.astype(jnp.float32) * mask[:, :, None]).reshape(
        seq_local * tok_local, width
    )
    d_ztwo, d_gain_two, d_shift_two = pull_two(grad_out)
    d_ffn = d_ztwo.astype(jnp.bfloat16)
    grad_bdown = jnp.sum(d_ffn.astype(jnp.float32), axis=0)
    d_hidden = back_product(d_ffn, w_down)
    d_hidden_in = (d_hidden * gelu_slope(hidden_in)).astype(jnp.bfloat16)
    grad_bup = jnp.sum(d_hidden_in.astype(jnp.float32), axis=0)
    d_first = d_ztwo + back_product(d_hidden_in, w_up)
    sink, pull_one = jax.vjp(layer_norm, z_one, gain_one, shift_one)
    d_zone, d_gain_one, d_shift_one = pull_one(d_first)
    d_branch = d_zone.astype(jnp.bfloat16)
    grad_bout = jnp.sum(d_branch.astype(jnp.float32), axis=0)

    blocks, grad_b_own, input_grad = backward(
        d_branch,
        w_out,
        w_qkv,
        log_total,
        d_zone,
        d_ffn,
        first_low,
        context,
        hidden_act,
        d_hidden_in,
        inputs_full,
        qkv,
    )
    grad_b_own = grad_b_own.reshape(-1)

    def put(array):
        empty = jnp.zeros(array.shape[:-1] + (width,), array.dtype)
        return lax.dynamic_update_slice_in_dim(empty, array, begin, array.ndim - 1)

    vector_terms = jnp.concatenate(
        [
            put(grad_b_own[:cols]),
            put(grad_b_own[2 * cols :]),
            grad_bout,
            d_gain_one,
            d_shift_one,
            grad_bup,
            grad_bdown,
            d_gain_two,
            d_shift_two,
        ],
        0,
    ).reshape(total, vec_local)
    vec_terms = jnp.pad(vector_terms, ((0, 0), (0, VEC_ROWS * BLK - vec_local)))
    vec_terms = vec_terms.astype(jnp.bfloat16).reshape(total, VEC_ROWS, BLK)
    slot_grad, vec_sums = scatter_sums(dims, owner_slot, blocks, vec_terms)
    vec_grad = vec_sums.reshape(-1)[:vec_local]
    first_moment, second_moment, updated, updated_short, new_average = adam(
        slot_grad, master, moment_one, moment_two, basis_left, basis_right, average
    )
    correct = 1.0 - 0.5**STEP
    vec_first = 0.5 * vec_moment_one + 0.5 * vec_grad
    vec_second = 0.5 * vec_moment_two + 0.5 * vec_grad * vec_grad
    vec_new = vec_master - VEC_RATE * (vec_first / correct) / (
        jnp.sqrt(vec_second / correct) + ADAM_EPS
    )
    return (
        layer_out,
        input_grad,
        slot_grad,
        vec_grad,
        first_moment,
        second_moment,
        updated,
        updated_short,
        new_average,
        vec_first,
        vec_second,
        vec_new,
    )


def solution(mesh):
    placed = (
        P("seq", "head", None),
        P("seq", "head", None),
        P("seq", "head"),
        P("seq", "head"),
        P(),
        P(("seq", "head"), None, None),
        P(("seq", "head"), None, None),
        P(("seq", "head"), None, None),
        P(("seq", "head"), None, None),
        P(("seq", "head"), None, None),
        P(("seq", "head"), None, None),
        P(("seq", "head")),
        P(("seq", "head")),
        P(("seq", "head")),
    )
    return jax.shard_map(
        body,
        mesh=mesh,
        in_specs=placed,
        out_specs=(
            P("seq", "head", None),
            P("seq", "head", None),
            P(("seq", "head"), None, None),
            P(("seq", "head")),
            P(("seq", "head"), None, None),
            P(("seq", "head"), None, None),
            P(("seq", "head"), None, None),
            P(("seq", "head"), None, None),
            P(("seq", "head"), None, None),
            P(("seq", "head")),
            P(("seq", "head")),
            P(("seq", "head")),
        ),
        check_vma=False,
    )
```

```python
import functools
import math

import jax
import jax.numpy as jnp
from jax import lax
from jax.experimental import pallas as pl
from jax.experimental.pallas import tpu as pltpu
from jax.sharding import PartitionSpec as P

D = 512
FF = 2048
WIN = 16
BLK = 128
STEP = 5
HD = 64
NBLK = 192
QUERIES = 256
SCALE = 1.0 / math.sqrt(HD)


NORM_EPS = 1e-06
ADAM_EPS = 1e-08
RATE = 0.05
VEC_RATE = 0.2
DECAY = 0.01
KEEP = 0.9
HIGH = lax.Precision.HIGHEST


def split_vector(vector):
    widths = [D, D, D, D, D, FF, D, D, D]
    pieces = []
    offset = 0
    for extent in widths:
        pieces.append(vector[offset : offset + extent])
        offset = offset + extent
    return pieces


def span_mask(span_offset, span_len):
    offsets = jnp.repeat(span_offset, WIN, axis=1)
    extents = jnp.repeat(span_len, WIN, axis=1)
    within = (jnp.arange(offsets.shape[1], dtype=jnp.int32) % WIN)[None, :]
    return ((within >= offsets) & (within < offsets + extents)).astype(jnp.float32)


def contract(left, right, left_axis, right_axis):
    return lax.dot_general(
        left, right, (((left_axis,), (right_axis,)), ((), ())), preferred_element_type=jnp.float32
    )


def swap(source, target, send_sem, recv_sem, own_sem, item):
    head_size = source.shape[1]
    seq = lax.axis_index("seq")
    head = lax.axis_index("head")
    copies = []
    for step in [2, 1, 3] if head_size == 4 else range(1, head_size):
        peer = lax.rem(head + step, head_size)
        copies.append(
            pltpu.make_async_remote_copy(
                src_ref=source.at[item, peer],
                dst_ref=target.at[head, item],
                send_sem=send_sem.at[item, step],
                recv_sem=recv_sem.at[item, step],
                device_id=(seq, peer),
                device_id_type=MESH,
            )
        )
    copies.append(
        pltpu.make_async_copy(source.at[item, head], target.at[head, item], own_sem.at[item])
    )
    return copies


def swap_step(source, target, send_sem, recv_sem, own_sem):
    item = pl.program_id(0)
    for copy in swap(source, target, send_sem, recv_sem, own_sem, item):
        copy.start()

    @pl.when(item == pl.num_programs(0) - 1)
    def _():
        for number in range(source.shape[0]):
            for copy in swap(source, target, send_sem, recv_sem, own_sem, number):
                copy.wait()


def swap_scratch(items, head_size, tokens, columns):
    return [
        pltpu.VMEM((items, head_size, tokens, columns), jnp.bfloat16),
        pltpu.SemaphoreType.DMA((items, head_size)),
        pltpu.SemaphoreType.DMA((items, head_size)),
        pltpu.SemaphoreType.DMA((items,)),
    ]


def normalize(values):
    center = values - jnp.mean(values, axis=-1, keepdims=True)
    spread = jnp.mean(center * center, axis=-1, keepdims=True)
    rate = lax.rsqrt(spread + NORM_EPS)
    return center * rate, rate


def normalize_back(grads, hat, rate, gain):
    scaled = grads * gain
    mean = jnp.mean(scaled, axis=-1, keepdims=True)
    along = jnp.mean(scaled * hat, axis=-1, keepdims=True)
    return rate * (scaled - mean - hat * along)


def column_sum(values):
    return jnp.sum(values, axis=0, keepdims=True)


def forward_kernel(
    w_ref,
    b_ref,
    wo_ref,
    up_ref,
    down_ref,
    rows_ref,
    bup_ref,
    tok_ref,
    cot_ref,
    x_any,
    qkv_out,
    h_out,
    du_out,
    ctx_got,
    lse_ref,
    lo_ref,
    df_ref,
    yb_ref,
    da_ref,
    dz_ref,
    sums_ref,
    bup_sum_ref,
    x_ref,
    qkv_ref,
    h_ref,
    du_ref,
    slope_ref,
    first_ref,
    load_sem,
    out_sem,
    ctx_src,
    ctx_send,
    ctx_recv,
    ctx_own,
):
    head_size, items, tokens, cols = ctx_got.shape
    width = wo_ref.shape[0]
    hidden = up_ref.shape[1]
    length = head_size * tokens

    def load(item):
        return pltpu.make_async_copy(x_any.at[item], x_ref.at[item], load_sem.at[item])

    def save(number, item):
        source, target = ((qkv_ref, qkv_out), (h_ref, h_out), (du_ref, du_out))[number]
        return pltpu.make_async_copy(
            source.at[item], target.at[item], out_sem.at[number, item]
        )

    def ctx_swap(item):
        return swap(ctx_src, ctx_got, ctx_send, ctx_recv, ctx_own, item)

    for item in range(items):
        load(item).start()
    greet_head(head_size)
    step = min(QUERIES, tokens)

    def attend_item(item, carry):
        load(item).wait()
        rows = x_ref[item].reshape(length, width)
        qkv_ref[item] = (contract(rows, w_ref[...], 1, 0) + b_ref[...]).astype(jnp.bfloat16)
        save(0, item).start()
        for number in range(cols // HD):
            low = number * HD
            keys = qkv_ref[item, :, cols + low : cols + low + HD]
            values = qkv_ref[item, :, 2 * cols + low : 2 * cols + low + HD]
            for begin in range(0, length, step):
                query = qkv_ref[item, begin : begin + step, low : low + HD] * jnp.bfloat16(SCALE)
                scores = contract(keys, query, 1, 1)
                highest = jnp.max(scores, axis=0, keepdims=True)
                weights = jnp.exp(scores - highest)
                summed = jnp.sum(weights, axis=0, keepdims=True)
                probs = (weights * (1.0 / summed)).astype(jnp.bfloat16)
                context = contract(values, probs, 0, 0).T.astype(jnp.bfloat16)
                ctx_src[
                    item, begin // tokens, pl.ds(begin % tokens, step), low : low + HD
                ] = context
                lse_ref[item, number : number + 1, begin : begin + step] = highest + jnp.log(
                    summed
                )
        for copy in ctx_swap(item):
            copy.start()
        return carry

    lax.fori_loop(0, items, attend_item, 0)
    sums_ref[...] = jnp.zeros_like(sums_ref)
    bup_sum_ref[...] = jnp.zeros_like(bup_sum_ref)
    parts = range(hidden // width)

    def layer_item(item, carry):
        for copy in ctx_swap(item):
            copy.wait()
        span = pl.ds(pl.multiple_of(item * tokens, tokens), tokens)
        z_one = tok_ref[span].astype(jnp.float32) + rows_ref[0:1]
        for head in range(head_size):
            z_one = z_one + contract(
                ctx_got[head, item], wo_ref[head * cols : (head + 1) * cols], 1, 0
            )
        hat_one, rate_one = normalize(z_one)
        first = hat_one * rows_ref[1:2] + rows_ref[2:3]
        first_ref[...] = first
        first_low = first.astype(jnp.bfloat16)
        yb_ref[span] = first_low
        for part in parts:
            lanes = slice(part * width, (part + 1) * width)
            value = contract(first_low, up_ref[:, lanes], 1, 0) + bup_ref[:, lanes]
            half = 0.5 * (1.0 + lax.erf(value * 0.7071067811865476))
            h_ref[item, :, lanes] = (value * half).astype(jnp.bfloat16)
            slope_ref[:, lanes] = (
                half + value * jnp.exp(-0.5 * value * value) * 0.3989422804014327
            )
        save(1, item).start()
        z_two = first_ref[...] + contract(h_ref[item], down_ref[...], 1, 0) + rows_ref[3:4]
        hat_two, rate_two = normalize(z_two)
        lo_ref[span] = (hat_two * rows_ref[4:5] + rows_ref[5:6]).astype(jnp.bfloat16)
        grads = cot_ref[span].astype(jnp.float32)
        d_two = normalize_back(grads, hat_two, rate_two, rows_ref[4:5])
        d_low = d_two.astype(jnp.bfloat16)
        df_ref[span] = d_low
        sums_ref[4:5] += column_sum(d_low.astype(jnp.float32))
        sums_ref[5:6] += column_sum(grads * hat_two)
        sums_ref[6:7] += column_sum(grads)
        d_first = d_two
        for part in parts:
            lanes = slice(part * width, (part + 1) * width)
            value = contract(d_low, down_ref[lanes], 1, 1) * slope_ref[:, lanes]
            short = value.astype(jnp.bfloat16)
            du_ref[item, :, lanes] = short
            bup_sum_ref[:, lanes] += column_sum(short.astype(jnp.float32))
        save(2, item).start()
        d_first = d_first + contract(du_ref[item], up_ref[...], 1, 1)
        d_one = normalize_back(d_first, hat_one, rate_one, rows_ref[1:2])
        dz_ref[span] = d_one
        short = d_one.astype(jnp.bfloat16)
        da_ref[span] = short
        sums_ref[0:1] += column_sum(short.astype(jnp.float32))
        sums_ref[1:2] += column_sum(d_first * hat_one)
        sums_ref[2:3] += column_sum(d_first)
        return carry

    lax.fori_loop(0, items, layer_item, 0)
    for number in range(3):
        for item in range(items):
            save(number, item).wait()


def forward_all(w_own, b_own, w_out, w_up, w_down, rows, b_up, token_rows, masked, inputs_full):
    seq_local, head_size, tokens, width = inputs_full.shape
    length = head_size * tokens
    cols = w_own.shape[1] // 3
    hidden = w_up.shape[1]
    own = seq_local * tokens
    short = jnp.bfloat16
    whole = pl.BlockSpec(memory_space=pltpu.VMEM)
    any_space = pl.BlockSpec(memory_space=pl.ANY)
    return pl.pallas_call(
        forward_kernel,
        out_shape=(
            jax.ShapeDtypeStruct((seq_local, length, 3 * cols), short),
            jax.ShapeDtypeStruct((seq_local, tokens, hidden), short),
            jax.ShapeDtypeStruct((seq_local, tokens, hidden), short),
            jax.ShapeDtypeStruct((head_size, seq_local, tokens, cols), short),
            jax.ShapeDtypeStruct((seq_local, 8, length), jnp.float32),
            jax.ShapeDtypeStruct((own, width), short),
            jax.ShapeDtypeStruct((own, width), short),
            jax.ShapeDtypeStruct((own, width), short),
            jax.ShapeDtypeStruct((own, width), short),
            jax.ShapeDtypeStruct((own, width), jnp.float32),
            jax.ShapeDtypeStruct((8, width), jnp.float32),
            jax.ShapeDtypeStruct((1, hidden), jnp.float32),
        ),
        in_specs=[whole] * 9 + [any_space],
        out_specs=(any_space,) * 3 + (whole,) * 9,
        scratch_shapes=[
            pltpu.VMEM(inputs_full.shape, short),
            pltpu.VMEM((seq_local, length, 3 * cols), short),
            pltpu.VMEM((seq_local, tokens, hidden), short),
            pltpu.VMEM((seq_local, tokens, hidden), short),
            pltpu.VMEM((tokens, hidden), jnp.float32),
            pltpu.VMEM((tokens, width), jnp.float32),
            pltpu.SemaphoreType.DMA((seq_local,)),
            pltpu.SemaphoreType.DMA((3, seq_local)),
        ]
        + swap_scratch(seq_local, head_size, tokens, cols),
        compiler_params=pltpu.CompilerParams(
            collective_id=2, has_side_effects=True, vmem_limit_bytes=60 * 1024 * 1024
        ),
        name="forward_all",
    )(w_own, b_own, w_out, w_up, w_down, rows, b_up, token_rows, masked, inputs_full)


def backward_kernel(
    da_ref,
    wo_ref,
    w_ref,
    lse_ref,
    dz_ref,
    df_ref,
    yb_ref,
    ctx_ref,
    h_any,
    du_any,
    x_any,
    qkv_any,
    blocks_ref,
    db_ref,
    grad_ref,
    h_ref,
    du_ref,
    x_ref,
    qkv_ref,
    load_sem,
    dall,
    acc,
    dw_ref,
    dctx_src,
    dctx_send,
    dctx_recv,
    dctx_own,
    d_src,
    d_send,
    d_recv,
    d_own,
    dctx_got,
    d_got,
):
    loads = [
        pltpu.make_async_copy(source, target, load_sem.at[number])
        for number, (source, target) in enumerate(
            [(h_any, h_ref), (du_any, du_ref), (qkv_any, qkv_ref), (x_any, x_ref)]
        )
    ]
    for load in loads:
        load.start()
    head_size, items, tokens, cols = ctx_ref.shape
    width = yb_ref.shape[1]
    hidden = h_ref.shape[1]
    length = head_size * tokens
    across = width // BLK
    greet_head(head_size)

    def dctx_swap(item):
        return swap(dctx_src, dctx_got, dctx_send, dctx_recv, dctx_own, item)

    def d_swap(item):
        return swap(d_src, d_got, d_send, d_recv, d_own, item)

    for item in range(items):
        dctx = contract(da_ref[item * tokens : (item + 1) * tokens], wo_ref[...], 1, 1)
        for head in range(head_size):
            dctx_src[item, head] = dctx[:, head * cols : (head + 1) * cols].astype(jnp.bfloat16)
        for copy in dctx_swap(item):
            copy.start()

    first = 3 * across * across
    for head in range(head_size):
        value = contract(ctx_ref[head].reshape(items * tokens, cols), da_ref[...], 0, 0)
        value = value.astype(jnp.bfloat16)
        for begin in range(0, cols, min(cols, BLK)):
            row = head * cols + begin
            part = min(cols, BLK)
            for col in range(across):
                number = first + (row // BLK) * across + col
                blocks_ref[number, row % BLK : row % BLK + part] = value[
                    begin : begin + part, col * BLK : (col + 1) * BLK
                ]
    first = 4 * across * across
    wide = hidden // BLK
    loads[1].wait()

    def up_part(turn, carry):
        span = pl.ds(pl.multiple_of(turn * width, width), width)
        value = contract(yb_ref[...], du_ref[:, span], 0, 0).astype(jnp.bfloat16)
        for row in range(across):
            for col in range(across):
                blocks_ref[first + row * wide + turn * across + col] = value[
                    row * BLK : (row + 1) * BLK, col * BLK : (col + 1) * BLK
                ]
        return carry

    lax.fori_loop(0, hidden // width, up_part, 0)
    loads[0].wait()
    second = first + across * wide

    def down_part(turn, carry):
        span = pl.ds(pl.multiple_of(turn * width, width), width)
        value = contract(h_ref[:, span], df_ref[...], 0, 0).astype(jnp.bfloat16)
        for row in range(across):
            for col in range(across):
                blocks_ref[second + (turn * across + row) * across + col] = value[
                    row * BLK : (row + 1) * BLK, col * BLK : (col + 1) * BLK
                ]
        return carry

    lax.fori_loop(0, hidden // width, down_part, 0)
    dw_ref[...] = jnp.zeros_like(dw_ref)
    db_ref[...] = jnp.zeros_like(db_ref)
    loads[2].wait()
    loads[3].wait()
    step = min(QUERIES, tokens)
    scale = jnp.bfloat16(SCALE)

    def attend_item(item, carry):
        for copy in dctx_swap(item):
            copy.wait()
        for number in range(cols // HD):
            low = number * HD
            keys = qkv_ref[item, :, cols + low : cols + low + HD]
            values = qkv_ref[item, :, 2 * cols + low : 2 * cols + low + HD]
            for begin in range(0, length, step):
                query = qkv_ref[item, begin : begin + step, low : low + HD] * scale
                dctx = dctx_got[
                    begin // tokens, item, pl.ds(begin % tokens, step), low : low + HD
                ]
                scores = contract(keys, query, 1, 1)
                probs = jnp.exp(scores - lse_ref[item, number : number + 1, begin : begin + step])
                dprobs = contract(values, dctx, 1, 1)
                inner = jnp.sum(probs * dprobs, axis=0, keepdims=True)
                dscores = (probs * (dprobs - inner)).astype(jnp.bfloat16)
                dkey = contract(dscores, query, 1, 0)
                dvalue = contract(probs.astype(jnp.bfloat16), dctx, 1, 0)
                if begin == 0:
                    acc[0] = dkey
                    acc[1] = dvalue
                else:
                    acc[0] += dkey
                    acc[1] += dvalue
                dquery = contract(keys, dscores, 0, 0).T * SCALE
                dall[begin : begin + step, low : low + HD] = dquery.astype(jnp.bfloat16)
            dall[:, cols + low : cols + low + HD] = acc[0].astype(jnp.bfloat16)
            dall[:, 2 * cols + low : 2 * cols + low + HD] = acc[1].astype(jnp.bfloat16)
        delta = dall[...]
        d_src[item] = delta.reshape(head_size, tokens, 3 * cols)
        for copy in d_swap(item):
            copy.start()
        dw_ref[...] += contract(x_ref[item].reshape(length, width), delta, 0, 0)
        db_ref[...] += jnp.sum(delta.astype(jnp.float32), axis=0, keepdims=True)
        return carry

    lax.fori_loop(0, items, attend_item, 0)

    head_me = lax.axis_index("head")
    for number in range(3):
        value = dw_ref[:, number * cols : (number + 1) * cols].astype(jnp.bfloat16)
        for row in range(across):
            for col in range(across):
                rows = value[row * BLK : (row + 1) * BLK]
                parts = []
                for begin in range(0, BLK, min(cols, BLK)):
                    lane = col * BLK + begin
                    begin_own = lane % cols
                    part = rows[:, begin_own : begin_own + min(cols, BLK)]
                    parts.append(jnp.where(head_me == lane // cols, part, jnp.zeros_like(part)))
                whole = parts[0] if len(parts) == 1 else jnp.concatenate(parts, 1)
                blocks_ref[number * across * across + row * across + col] = whole

    def input_item(item, carry):
        for copy in d_swap(item):
            copy.wait()
        span = pl.ds(pl.multiple_of(item * tokens, tokens), tokens)
        total = dz_ref[span]
        for head in range(head_size):
            total = total + contract(d_got[head, item], w_ref[head], 1, 1)
        grad_ref[item] = total
        return carry

    lax.fori_loop(0, items, input_item, 0)


def backward(d_branch, w_out, w_qkv, lse, d_zone, d_ffn, first_low, context, hidden, d_hidden, inputs_full, qkv):
    head_size, seq_local, tokens, cols = context.shape
    width = w_out.shape[0]
    length = head_size * tokens
    whole = pl.BlockSpec(memory_space=pltpu.VMEM)
    any_space = pl.BlockSpec(memory_space=pl.ANY)

    def like(array):
        return pltpu.VMEM(array.shape, array.dtype)

    return pl.pallas_call(
        backward_kernel,
        out_shape=(
            jax.ShapeDtypeStruct((NBLK, BLK, BLK), jnp.bfloat16),
            jax.ShapeDtypeStruct((1, 3 * cols), jnp.float32),
            jax.ShapeDtypeStruct((seq_local, tokens, width), jnp.float32),
        ),
        in_specs=[whole] * 8 + [any_space] * 4,
        out_specs=(whole, whole, whole),
        scratch_shapes=[
            like(hidden),
            like(d_hidden),
            like(inputs_full),
            like(qkv),
            pltpu.SemaphoreType.DMA((4,)),
            pltpu.VMEM((length, 3 * cols), jnp.bfloat16),
            pltpu.VMEM((2, length, HD), jnp.float32),
            pltpu.VMEM((width, 3 * cols), jnp.float32),
        ]
        + swap_scratch(seq_local, head_size, tokens, cols)
        + swap_scratch(seq_local, head_size, tokens, 3 * cols)
        + [
            pltpu.VMEM((head_size, seq_local, tokens, cols), jnp.bfloat16),
            pltpu.VMEM((head_size, seq_local, tokens, 3 * cols), jnp.bfloat16),
        ],
        compiler_params=pltpu.CompilerParams(
            collective_id=4, has_side_effects=True, vmem_limit_bytes=60 * 1024 * 1024
        ),
        name="backward",
    )(
        d_branch,
        w_out,
        w_qkv,
        lse,
        d_zone,
        d_ffn,
        first_low,
        context,
        hidden,
        d_hidden,
        inputs_full,
        qkv,
    )


def high_product(left, right, left_axis, right_axis):
    return lax.dot_general(
        left,
        right,
        (((left_axis,), (right_axis,)), ((), ())),
        precision=HIGH,
        preferred_element_type=jnp.float32,
    )


def adam_kernel(
    grad_ref,
    master_ref,
    one_ref,
    two_ref,
    left_ref,
    right_ref,
    average_ref,
    new_one_ref,
    new_two_ref,
    new_master_ref,
    new_short_ref,
    new_average_ref,
):
    slots = range(grad_ref.shape[0])
    correct = 1.0 - 0.5**STEP
    rotated = [high_product(left_ref[slot], grad_ref[slot], 0, 0) for slot in slots]
    rotated = [high_product(rotated[slot], right_ref[slot], 1, 0) for slot in slots]
    normed = []
    for slot in slots:
        first = 0.5 * one_ref[slot] + 0.5 * rotated[slot]
        second = 0.5 * two_ref[slot] + 0.5 * rotated[slot] * rotated[slot]
        new_one_ref[slot] = first
        new_two_ref[slot] = second
        normed.append(first / correct / (jnp.sqrt(second / correct) + ADAM_EPS))
    turned = [high_product(left_ref[slot], normed[slot], 1, 0) for slot in slots]
    turned = [high_product(turned[slot], right_ref[slot], 1, 1) for slot in slots]
    for slot in slots:
        updated = master_ref[slot] - RATE * (turned[slot] + DECAY * master_ref[slot])
        new_master_ref[slot] = updated
        new_short_ref[slot] = updated.astype(jnp.bfloat16)
        new_average_ref[slot] = KEEP * average_ref[slot] + (1.0 - KEEP) * updated


def adam(grads, master, moment_one, moment_two, basis_left, basis_right, average):
    slots = grads.shape[0]
    together = math.gcd(slots, 4)
    spec = pl.BlockSpec((together, BLK, BLK), lambda s: (s, 0, 0))
    full = jax.ShapeDtypeStruct(grads.shape, jnp.float32)
    return pl.pallas_call(
        adam_kernel,
        grid=(slots // together,),
        out_shape=(full, full, full, jax.ShapeDtypeStruct(grads.shape, jnp.bfloat16), full),
        in_specs=[spec] * 7,
        out_specs=(spec,) * 5,
        name="adam",
    )(grads, master, moment_one, moment_two, basis_left, basis_right, average)


MESH = pl.DeviceIdType.MESH
VEC_ROWS = 16
PIECE = 16


def cut(seq_size, head_size):
    cores = 2 if head_size % 2 == 0 else 1
    rows = 1
    while 2 * (rows * 2) ** 2 <= seq_size and seq_size % (rows * 2) == 0:
        rows = rows * 2
    return (seq_size // rows, rows, head_size // cores, cores)


def place(dims):
    size_z, size_x, size_y, size_c = dims
    seq = lax.axis_index("seq")
    head = lax.axis_index("head")
    return (
        lax.div(seq, size_x),
        lax.rem(seq, size_x),
        lax.div(head, size_c),
        lax.rem(head, size_c),
    )


def device(dims, coords):
    return (coords[0] * dims[1] + coords[1], coords[2] * dims[3] + coords[3])


def flat(dims, coords):
    return ((coords[0] * dims[1] + coords[1]) * dims[2] + coords[2]) * dims[3] + coords[3]


def moved(dims, coords, axis, step):
    new = list(coords)
    new[axis] = lax.rem(coords[axis] + step, dims[axis])
    return tuple(new)


def greet(dims, coords):
    barrier = pltpu.get_barrier_semaphore()
    count = 0
    for axis in range(4):
        for step in range(1, dims[axis]):
            pl.semaphore_signal(
                barrier,
                inc=1,
                device_id=device(dims, moved(dims, coords, axis, step)),
                device_id_type=MESH,
            )
            count = count + 1
    pl.semaphore_wait(barrier, count)


def greet_head(head_size):
    barrier = pltpu.get_barrier_semaphore()
    seq = lax.axis_index("seq")
    head = lax.axis_index("head")
    for step in range(1, head_size):
        pl.semaphore_signal(
            barrier, inc=1, device_id=(seq, lax.rem(head + step, head_size)), device_id_type=MESH
        )
    pl.semaphore_wait(barrier, head_size - 1)


def gather_kernel(
    dims,
    inv_ref,
    x_ref,
    w_ref,
    xf_ref,
    qkv_ref,
    out_ref,
    up_ref,
    down_ref,
    vec_ref,
    wf_ref,
    own_sem,
    x_send,
    x_recv,
    w_send,
    w_recv,
):
    me = place(dims)
    size_z, size_x, size_y, size_c = dims
    head_me = me[2] * size_c + me[3]
    chunk = w_ref.shape[0]

    def spot(index):
        return wf_ref.at[pl.ds(index * chunk, chunk)]

    own_x = pltpu.make_async_copy(x_ref, xf_ref.at[:, head_me], own_sem.at[0])
    own_w = pltpu.make_async_copy(w_ref, spot(flat(dims, me)), own_sem.at[1])
    own_x.start()
    own_w.start()
    greet(dims, me)
    started = []

    def send_x(source, head, target, number):
        copy = pltpu.make_async_remote_copy(
            src_ref=source,
            dst_ref=xf_ref.at[:, head],
            send_sem=x_send.at[number],
            recv_sem=x_recv.at[head],
            device_id=device(dims, target),
            device_id_type=MESH,
        )
        copy.start()
        started.append(copy)

    def arrived_x(head):
        pltpu.make_async_remote_copy(
            src_ref=x_ref,
            dst_ref=xf_ref.at[:, head],
            send_sem=x_send.at[0],
            recv_sem=x_recv.at[head],
            device_id=device(dims, me),
            device_id_type=MESH,
        ).wait_recv()

    count = [0]

    def send_w(source, index, target):
        number = count[0]
        count[0] = number + 1
        copy = pltpu.make_async_remote_copy(
            src_ref=source,
            dst_ref=spot(index),
            send_sem=w_send.at[number],
            recv_sem=w_recv.at[index],
            device_id=device(dims, target),
            device_id_type=MESH,
        )
        copy.start()
        started.append(copy)

    def arrived_w(index):
        pltpu.make_async_remote_copy(
            src_ref=w_ref,
            dst_ref=spot(index),
            send_sem=w_send.at[0],
            recv_sem=w_recv.at[index],
            device_id=device(dims, me),
            device_id_type=MESH,
        ).wait_recv()

    order = [0, 2, 1, 3]

    def forward(source, coords, after):
        for axis in order[after:]:
            for step in range(1, dims[axis]):
                send_w(source, flat(dims, coords), moved(dims, me, axis, step))

    number = 0
    for step in range(1, size_y):
        send_x(x_ref, head_me, moved(dims, me, 2, step), number)
        number = number + 1
    for step in range(1, size_c):
        send_x(x_ref, head_me, moved(dims, me, 3, step), number)
        number = number + 1
    forward(w_ref, me, 0)
    held = [me]
    for level in range(3):
        axis = order[level]
        fresh = []
        for step in range(1, dims[axis]):
            for coords in held:
                source = moved(dims, coords, axis, step)
                arrived_w(flat(dims, source))
                forward(spot(flat(dims, source)), source, level + 1)
                fresh.append(source)
        held = held + fresh
        if level == 1:
            for step in range(1, size_y):
                other = moved(dims, me, 2, step)
                head = other[2] * size_c + other[3]
                arrived_x(head)
                for hop in range(1, size_c):
                    send_x(xf_ref.at[:, head], head, moved(dims, me, 3, hop), number)
                    number = number + 1
    for step in range(1, size_c):
        for coords in held:
            arrived_w(flat(dims, moved(dims, coords, 3, step)))
        for across in range(size_y):
            other = moved(dims, moved(dims, me, 3, step), 2, across)
            arrived_x(other[2] * size_c + other[3])
    for copy in started:
        copy.wait_send()
    own_x.wait()
    own_w.wait()
    unpack(dims, inv_ref, wf_ref, qkv_ref, out_ref, up_ref, down_ref)
    chunk = w_ref.shape[0]
    for number in range(vec_ref.shape[0]):
        vec_ref[number] = wf_ref[(number + 1) * chunk - 1]


def unpack(dims, inv_ref, wf_ref, qkv_ref, out_ref, up_ref, down_ref):
    head_size = dims[2] * dims[3]
    width = out_ref.shape[0]
    hidden = up_ref.shape[1]
    cols = width // head_size
    across = width // BLK

    def block(number):
        piece = inv_ref[number]
        return jnp.concatenate([wf_ref[piece + part] for part in range(BLK // PIECE)], 0)

    def rows_of(row_count, first, col_count, store):
        def one(row, carry):
            span = pl.ds(pl.multiple_of(row * BLK, BLK), BLK)
            for col in range(col_count):
                store(span, col, block(first + row * col_count + col))
            return carry

        lax.fori_loop(0, row_count, one, 0)

    for number in range(3):

        def store_qkv(span, col, value, number=number):
            for begin in range(0, BLK, min(cols, BLK)):
                head = (col * BLK + begin) // cols
                lane = (col * BLK + begin) % cols
                part = min(cols, BLK)
                qkv_ref[head, span, number * cols + lane : number * cols + lane + part] = value[
                    :, begin : begin + part
                ]

        rows_of(across, number * across * across, across, store_qkv)

    def store_in(ref):
        def store(span, col, value):
            ref[span, col * BLK : (col + 1) * BLK] = value

        return store

    rows_of(across, 3 * across * across, across, store_in(out_ref))
    first = 4 * across * across
    rows_of(across, first, hidden // BLK, store_in(up_ref))
    first = first + across * (hidden // BLK)
    rows_of(hidden // BLK, first, across, store_in(down_ref))


def gather_all(dims, inverse, inputs, packed):
    size_z, size_x, size_y, size_c = dims
    total = size_z * size_x * size_y * size_c
    head_size = size_y * size_c
    seq_local, tok_local, width = inputs.shape
    any_space = pl.BlockSpec(memory_space=pl.ANY)
    whole = pl.BlockSpec(memory_space=pltpu.VMEM)
    sends_x = (size_y - 1) * size_c + size_c - 1
    sends_w = (
        (size_z - 1)
        + size_z * (size_y - 1)
        + size_z * size_y * (size_x - 1)
        + size_z * size_y * size_x * (size_c - 1)
    )
    return pl.pallas_call(
        functools.partial(gather_kernel, dims),
        out_shape=(
            jax.ShapeDtypeStruct((seq_local, head_size, tok_local, width), inputs.dtype),
            jax.ShapeDtypeStruct((head_size, width, 3 * width // head_size), packed.dtype),
            jax.ShapeDtypeStruct((width, width), packed.dtype),
            jax.ShapeDtypeStruct((width, FF), packed.dtype),
            jax.ShapeDtypeStruct((FF, width), packed.dtype),
            jax.ShapeDtypeStruct((total, VEC_ROWS, BLK), packed.dtype),
        ),
        in_specs=[pl.BlockSpec(memory_space=pltpu.SMEM), whole, whole],
        out_specs=(any_space, whole, whole, whole, whole, whole),
        scratch_shapes=[
            pltpu.VMEM((total * packed.shape[0],) + packed.shape[1:], packed.dtype),
            pltpu.SemaphoreType.DMA((2,)),
            pltpu.SemaphoreType.DMA((max(sends_x, 1),)),
            pltpu.SemaphoreType.DMA((head_size,)),
            pltpu.SemaphoreType.DMA((max(sends_w, 1),)),
            pltpu.SemaphoreType.DMA((total,)),
        ],
        compiler_params=pltpu.CompilerParams(
            collective_id=0, has_side_effects=True, vmem_limit_bytes=40 * 1024 * 1024
        ),
        name="gather_all",
    )(inverse, inputs, packed)


def scatter_kernel(
    dims,
    slots,
    owner_ref,
    blocks_ref,
    vec_ref,
    grad_ref,
    vec_out_ref,
    term,
    got_c,
    got_x,
    got_y,
    got_z,
    send_c,
    send_x,
    send_y,
    send_z,
    recv_c,
    recv_x,
    recv_y,
    recv_z,
):
    me = place(dims)
    size_z, size_x, size_y, size_c = dims
    rows = slots * BLK
    greet(dims, me)

    def block_of(dest, slot):
        owner = owner_ref[dest * slots + slot]
        block = blocks_ref[jnp.minimum(owner, NBLK - 1)]
        return jnp.where(owner < NBLK, block, jnp.zeros_like(block))

    def total_of(dest, extras, keep_block, keep_vec):
        def one(slot, carry):
            value = block_of(dest, slot).astype(jnp.float32)
            span = pl.ds(pl.multiple_of(slot * BLK, BLK), BLK)
            for ref, lead in extras:
                value = value + ref[lead + (span,)].astype(jnp.float32)
            keep_block(slot, span, value)
            return carry

        lax.fori_loop(0, slots, one, 0)
        value = vec_ref[dest].astype(jnp.float32)
        for ref, lead in extras:
            value = value + ref[lead + (pl.ds(rows, VEC_ROWS),)].astype(jnp.float32)
        keep_vec(value)

    def into_term(dest, extras):
        def keep_block(slot, span, value):
            term[dest, span] = value.astype(jnp.bfloat16)

        def keep_vec(value):
            term[dest, pl.ds(rows, VEC_ROWS)] = value.astype(jnp.bfloat16)

        total_of(dest, extras, keep_block, keep_vec)

    def remote(dest, got, send, recv, hop, index, target):
        return pltpu.make_async_remote_copy(
            src_ref=term.at[dest],
            dst_ref=got.at[hop, index],
            send_sem=send.at[hop, index],
            recv_sem=recv.at[hop, index],
            device_id=device(dims, target),
            device_id_type=MESH,
        )

    def each(axis, begin, end, coords_of, extras_of, got, send, recv, only=None):
        for step in range(1, dims[axis]) if only is None else [only]:
            target = moved(dims, me, axis, step)

            def one(index, carry, step=step, target=target):
                coords = list(coords_of(index))
                coords[axis] = target[axis]
                dest = flat(dims, coords)
                into_term(dest, extras_of(coords))
                remote(dest, got, send, recv, step - 1, index, target).start()
                return carry

            if end == begin + 1:
                one(begin, 0)
            else:
                lax.fori_loop(begin, end, one, 0)

    def wait_for(axis, got, send, recv, index):
        found = []
        for step in range(1, dims[axis]):
            remote(0, got, send, recv, step - 1, index, moved(dims, me, axis, step)).wait_recv()
            found.append((got, (step - 1, index)))
        return found

    def turned(axis, order):
        return lax.rem(me[axis] + 1 + order, dims[axis])

    def order_of(axis, coords):
        return lax.rem(coords[axis] - me[axis] + 2 * dims[axis] - 1, dims[axis])

    def index_c(coords):
        return (order_of(0, coords) * size_x + order_of(1, coords)) * size_y + order_of(2, coords)

    def coords_c(index):
        return (
            turned(0, lax.div(index, size_x * size_y)),
            turned(1, lax.rem(lax.div(index, size_y), size_x)),
            turned(2, lax.rem(index, size_y)),
            me[3],
        )

    def run(first, second):
        size_s = dims[second]

        def coords_f(index):
            coords = list(me)
            coords[0] = turned(0, lax.div(index, size_s))
            coords[second] = turned(second, lax.rem(index, size_s))
            return coords

        def coords_s(index):
            coords = list(me)
            coords[0] = turned(0, index)
            return coords

        def coords_z(index):
            return me

        def extras_c(coords):
            return []

        def extras_f(coords):
            return wait_for(3, got_c, send_c, recv_c, index_c(coords))

        def extras_s(coords):
            index = order_of(0, coords) * size_s + order_of(second, coords)
            return extras_f(coords) + wait_for(first, got_x, send_x, recv_x, index)

        def extras_z(coords):
            return extras_s(coords) + wait_for(
                second, got_y, send_y, recv_y, order_of(0, coords)
            )

        def stage_c(order):
            group = size_x * size_y
            each(3, order * group, (order + 1) * group, coords_c, extras_c, got_c, send_c, recv_c)

        def stage_f(order):
            group = size_s
            each(
                first, order * group, (order + 1) * group, coords_f, extras_f, got_x, send_x, recv_x
            )

        stage_c(0)
        for order in range(1, size_z):
            stage_c(order)
            stage_f(order - 1)
        stage_f(size_z - 1)
        for order in range(size_z):
            each(second, order, order + 1, coords_s, extras_s, got_y, send_y, recv_y)
            if order + 1 < size_z:
                each(0, 0, 1, coords_z, extras_z, got_z, send_z, recv_z, only=order + 1)
        extras = extras_z(me) + wait_for(0, got_z, send_z, recv_z, 0)

        def keep_block(slot, span, value):
            grad_ref[slot] = value

        def keep_vec(value):
            vec_out_ref[...] = value

        total_of(flat(dims, me), extras, keep_block, keep_vec)
        drain(3, size_z * size_x * size_y, got_c, send_c, recv_c)
        drain(first, size_z * size_s, got_x, send_x, recv_x)
        drain(second, size_z, got_y, send_y, recv_y)
        drain(0, 1, got_z, send_z, recv_z)

    def drain(axis, count, got, send, recv):
        for step in range(1, dims[axis]):

            def one(index, carry, step=step):
                remote(
                    0, got, send, recv, step - 1, index, moved(dims, me, axis, step)
                ).wait_send()
                return carry

            lax.fori_loop(0, count, one, 0)

    for core in range(size_c):

        @pl.when(me[3] == core)
        def _(core=core):
            run(1 + core % 2, 2 - core % 2)


def scatter_sums(dims, owner_slot, blocks, vec_terms):
    size_z, size_x, size_y, size_c = dims
    total = size_z * size_x * size_y * size_c
    slots = owner_slot.shape[0] // total
    chunk = (slots * BLK + VEC_ROWS, BLK)
    shapes = [
        (max(size_c - 1, 1), size_z * size_x * size_y),
        (max(size_x - 1, size_y - 1, 1), size_z * max(size_x, size_y)),
        (max(size_x - 1, size_y - 1, 1), size_z),
        (max(size_z - 1, 1), 1),
    ]
    whole = pl.BlockSpec(memory_space=pltpu.VMEM)
    return pl.pallas_call(
        functools.partial(scatter_kernel, dims, slots),
        out_shape=(
            jax.ShapeDtypeStruct((slots, BLK, BLK), jnp.float32),
            jax.ShapeDtypeStruct((VEC_ROWS, BLK), jnp.float32),
        ),
        in_specs=[pl.BlockSpec(memory_space=pltpu.SMEM), whole, whole],
        out_specs=(whole, whole),
        scratch_shapes=[pltpu.VMEM((total,) + chunk, jnp.bfloat16)]
        + [pltpu.VMEM(shape + chunk, jnp.bfloat16) for shape in shapes]
        + [pltpu.SemaphoreType.DMA(shape) for shape in shapes]
        + [pltpu.SemaphoreType.DMA(shape) for shape in shapes],
        compiler_params=pltpu.CompilerParams(
            collective_id=1, has_side_effects=True, vmem_limit_bytes=60 * 1024 * 1024
        ),
        name="scatter_sums",
    )(owner_slot, blocks, vec_terms)


def three_parts(values):
    high = lax.reduce_precision(values, 8, 7)
    rest = values - high
    middle = lax.reduce_precision(rest, 8, 7)
    low = lax.reduce_precision(rest - middle, 8, 7)
    return [part.astype(jnp.bfloat16) for part in (high, middle, low)]


def as_rows(vector, rows):
    return jnp.pad(vector, (0, rows * BLK - vector.shape[0])).reshape(rows, BLK)


def ceil_to(value, unit):
    return -(-value // unit) * unit


def body(
    inputs,
    cotangent,
    span_offset,
    span_len,
    owner_slot,
    master,
    moment_one,
    moment_two,
    basis_left,
    basis_right,
    average,
    vec_master,
    vec_moment_one,
    vec_moment_two,
):
    both = ("seq", "head")
    seq_size = lax.axis_size("seq")
    head_size = lax.axis_size("head")
    total = seq_size * head_size
    head_index = lax.axis_index("head")
    seq_local, tok_local, width = inputs.shape
    slots_local = master.shape[0]
    slot_total = slots_local * total
    vec_local = vec_master.shape[0]

    dims = cut(seq_size, head_size)

    mask = span_mask(span_offset, span_len)
    masked = jnp.where(mask[:, :, None] > 0, cotangent, jnp.zeros_like(cotangent))
    masked = masked.reshape(seq_local * tok_local, width)

    packed = jnp.concatenate(
        [
            master.astype(jnp.bfloat16).reshape(slots_local * BLK, BLK),
            as_rows(jnp.concatenate(three_parts(vec_master)), VEC_ROWS),
        ],
        0,
    ).reshape(-1, PIECE, BLK)
    numbers = jnp.arange(slot_total, dtype=jnp.int32)
    inverse = jnp.sum(
        jnp.where(owner_slot[:, None] == numbers[None, :], numbers[:, None], 0), axis=0
    )
    pieces = (inverse // slots_local) * packed.shape[0]
    pieces = pieces + (inverse % slots_local) * (BLK // PIECE)
    inputs_full, w_qkv, w_out, w_up, w_down, vec_parts = gather_all(
        dims, pieces, inputs, packed
    )
    parts = (
        vec_parts
        .reshape(total, VEC_ROWS * BLK)[:, : 3 * vec_local]
        .reshape(total, 3, vec_local)
        .astype(jnp.float32)
    )
    all_vector = ((parts[:, 2] + parts[:, 1]) + parts[:, 0]).reshape(-1)

    b_query, b_value, b_out, gain_one, shift_one, b_up, b_down, gain_two, shift_two = split_vector(
        all_vector
    )
    token_rows = inputs.reshape(seq_local * tok_local, width)
    local_shape = (seq_local, tok_local, width)
    cols = width // head_size
    begin = head_index * cols

    def own(array):
        return lax.dynamic_slice_in_dim(array, begin, cols, array.ndim - 1)

    w_own = lax.dynamic_index_in_dim(w_qkv, head_index, 0, keepdims=False)
    b_own = jnp.concatenate([own(b_query), jnp.zeros((cols,), jnp.float32), own(b_value)], 0)
    rows = jnp.stack(
        [b_out, gain_one, shift_one, b_down, gain_two, shift_two, b_down, b_down], 0
    )
    (
        qkv,
        hidden_act,
        d_hidden_in,
        context,
        log_total,
        layer_out,
        d_ffn,
        first_low,
        d_branch,
        d_zone,
        sums,
        grad_bup,
    ) = forward_all(
        w_own,
        b_own[None, :],
        w_out,
        w_up,
        w_down,
        rows,
        b_up[None, :],
        token_rows,
        masked,
        inputs_full,
    )
    layer_out = layer_out.reshape(local_shape)
    blocks, grad_b_own, input_grad = backward(
        d_branch,
        w_out,
        w_qkv,
        log_total,
        d_zone,
        d_ffn,
        first_low,
        context,
        hidden_act.reshape(seq_local * tok_local, FF),
        d_hidden_in.reshape(seq_local * tok_local, FF),
        inputs_full,
        qkv,
    )
    grad_b_own = grad_b_own.reshape(-1)

    def put(array):
        empty = jnp.zeros(array.shape[:-1] + (width,), array.dtype)
        return lax.dynamic_update_slice_in_dim(empty, array, begin, array.ndim - 1)

    vector_terms = jnp.concatenate(
        [
            put(grad_b_own[:cols]),
            put(grad_b_own[2 * cols :]),
            sums[0:3].reshape(-1),
            grad_bup.reshape(-1),
            sums[4:7].reshape(-1),
        ],
        0,
    ).reshape(total, vec_local)
    vec_terms = jnp.pad(vector_terms, ((0, 0), (0, VEC_ROWS * BLK - vec_local)))
    vec_terms = vec_terms.astype(jnp.bfloat16).reshape(total, VEC_ROWS, BLK)
    slot_grad, vec_sums = scatter_sums(dims, owner_slot, blocks, vec_terms)
    vec_grad = vec_sums.reshape(-1)[:vec_local]
    first_moment, second_moment, updated, updated_short, new_average = adam(
        slot_grad, master, moment_one, moment_two, basis_left, basis_right, average
    )
    correct = 1.0 - 0.5**STEP
    vec_first = 0.5 * vec_moment_one + 0.5 * vec_grad
    vec_second = 0.5 * vec_moment_two + 0.5 * vec_grad * vec_grad
    vec_new = vec_master - VEC_RATE * (vec_first / correct) / (
        jnp.sqrt(vec_second / correct) + ADAM_EPS
    )
    return (
        layer_out,
        input_grad,
        slot_grad,
        vec_grad,
        first_moment,
        second_moment,
        updated,
        updated_short,
        new_average,
        vec_first,
        vec_second,
        vec_new,
    )


def solution(mesh):
    placed = (
        P("seq", "head", None),
        P("seq", "head", None),
        P("seq", "head"),
        P("seq", "head"),
        P(),
        P(("seq", "head"), None, None),
        P(("seq", "head"), None, None),
        P(("seq", "head"), None, None),
        P(("seq", "head"), None, None),
        P(("seq", "head"), None, None),
        P(("seq", "head"), None, None),
        P(("seq", "head")),
        P(("seq", "head")),
        P(("seq", "head")),
    )
    return jax.shard_map(
        body,
        mesh=mesh,
        in_specs=placed,
        out_specs=(
            P("seq", "head", None),
            P("seq", "head", None),
            P(("seq", "head"), None, None),
            P(("seq", "head")),
            P(("seq", "head"), None, None),
            P(("seq", "head"), None, None),
            P(("seq", "head"), None, None),
            P(("seq", "head"), None, None),
            P(("seq", "head"), None, None),
            P(("seq", "head")),
            P(("seq", "head")),
            P(("seq", "head")),
        ),
        check_vma=False,
    )
```

```python
import functools
import math

import jax
import jax.numpy as jnp
from jax import lax
from jax.experimental import pallas as pl
from jax.experimental.pallas import tpu as pltpu
from jax.sharding import PartitionSpec as P

D = 512
FF = 2048
WIN = 16
BLK = 128
STEP = 5
HD = 64
NBLK = 192
QUERIES = 256
SCALE = 1.0 / math.sqrt(HD)


NORM_EPS = 1e-06
ADAM_EPS = 1e-08
RATE = 0.05
VEC_RATE = 0.2
DECAY = 0.01
KEEP = 0.9
HIGH = lax.Precision.HIGHEST


def split_vector(vector):
    widths = [D, D, D, D, D, FF, D, D, D]
    pieces = []
    offset = 0
    for extent in widths:
        pieces.append(vector[offset : offset + extent])
        offset = offset + extent
    return pieces


def span_mask(span_offset, span_len):
    offsets = jnp.repeat(span_offset, WIN, axis=1)
    extents = jnp.repeat(span_len, WIN, axis=1)
    within = (jnp.arange(offsets.shape[1], dtype=jnp.int32) % WIN)[None, :]
    return ((within >= offsets) & (within < offsets + extents)).astype(jnp.float32)


def contract(left, right, left_axis, right_axis):
    return lax.dot_general(
        left, right, (((left_axis,), (right_axis,)), ((), ())), preferred_element_type=jnp.float32
    )


def swap(source, target, send_sem, recv_sem, own_sem, item):
    head_size = source.shape[1]
    seq = lax.axis_index("seq")
    head = lax.axis_index("head")
    copies = []
    for step in [2, 1, 3] if head_size == 4 else range(1, head_size):
        peer = lax.rem(head + step, head_size)
        copies.append(
            pltpu.make_async_remote_copy(
                src_ref=source.at[item, peer],
                dst_ref=target.at[head, item],
                send_sem=send_sem.at[item, step],
                recv_sem=recv_sem.at[item, step],
                device_id=(seq, peer),
                device_id_type=MESH,
            )
        )
    copies.append(
        pltpu.make_async_copy(source.at[item, head], target.at[head, item], own_sem.at[item])
    )
    return copies


def swap_step(source, target, send_sem, recv_sem, own_sem):
    item = pl.program_id(0)
    for copy in swap(source, target, send_sem, recv_sem, own_sem, item):
        copy.start()

    @pl.when(item == pl.num_programs(0) - 1)
    def _():
        for number in range(source.shape[0]):
            for copy in swap(source, target, send_sem, recv_sem, own_sem, number):
                copy.wait()


def swap_scratch(items, head_size, tokens, columns):
    return [
        pltpu.VMEM((items, head_size, tokens, columns), jnp.bfloat16),
        pltpu.SemaphoreType.DMA((items, head_size)),
        pltpu.SemaphoreType.DMA((items, head_size)),
        pltpu.SemaphoreType.DMA((items,)),
    ]


def normalize(values):
    center = values - jnp.mean(values, axis=-1, keepdims=True)
    spread = jnp.mean(center * center, axis=-1, keepdims=True)
    rate = lax.rsqrt(spread + NORM_EPS)
    return center * rate, rate


def normalize_back(grads, hat, rate, gain):
    scaled = grads * gain
    mean = jnp.mean(scaled, axis=-1, keepdims=True)
    along = jnp.mean(scaled * hat, axis=-1, keepdims=True)
    return rate * (scaled - mean - hat * along)


def column_sum(values):
    return jnp.sum(values, axis=0, keepdims=True)


def forward_kernel(
    w_ref,
    b_ref,
    wo_ref,
    up_ref,
    down_ref,
    rows_ref,
    bup_ref,
    tok_ref,
    cot_ref,
    x_any,
    qkv_out,
    h_out,
    du_out,
    ctx_got,
    lse_ref,
    lo_ref,
    df_ref,
    yb_ref,
    da_ref,
    dz_ref,
    sums_ref,
    bup_sum_ref,
    x_ref,
    qkv_ref,
    h_ref,
    du_ref,
    slope_ref,
    first_ref,
    load_sem,
    out_sem,
    ctx_src,
    ctx_send,
    ctx_recv,
    ctx_own,
):
    head_size, items, tokens, cols = ctx_got.shape
    width = wo_ref.shape[0]
    hidden = up_ref.shape[1]
    length = head_size * tokens

    def load(item):
        return pltpu.make_async_copy(x_any.at[item], x_ref.at[item], load_sem.at[item])

    def save(number, item):
        source, target = ((qkv_ref, qkv_out), (h_ref, h_out), (du_ref, du_out))[number]
        return pltpu.make_async_copy(
            source.at[item], target.at[item], out_sem.at[number, item]
        )

    def ctx_swap(item):
        return swap(ctx_src, ctx_got, ctx_send, ctx_recv, ctx_own, item)

    for item in range(items):
        load(item).start()
    greet_head(head_size)
    step = min(QUERIES, tokens)

    def attend_item(item, carry):
        load(item).wait()
        rows = x_ref[item].reshape(length, width)
        qkv_ref[item] = (contract(rows, w_ref[...], 1, 0) + b_ref[...]).astype(jnp.bfloat16)
        save(0, item).start()
        for number in range(cols // HD):
            low = number * HD
            keys = qkv_ref[item, :, cols + low : cols + low + HD]
            values = qkv_ref[item, :, 2 * cols + low : 2 * cols + low + HD]
            for begin in range(0, length, step):
                query = qkv_ref[item, begin : begin + step, low : low + HD] * jnp.bfloat16(SCALE)
                scores = contract(keys, query, 1, 1)
                highest = jnp.max(scores, axis=0, keepdims=True)
                weights = jnp.exp(scores - highest)
                summed = jnp.sum(weights, axis=0, keepdims=True)
                probs = (weights * (1.0 / summed)).astype(jnp.bfloat16)
                context = contract(values, probs, 0, 0).T.astype(jnp.bfloat16)
                ctx_src[
                    item, begin // tokens, pl.ds(begin % tokens, step), low : low + HD
                ] = context
                lse_ref[item, number : number + 1, begin : begin + step] = highest + jnp.log(
                    summed
                )
        for copy in ctx_swap(item):
            copy.start()
        return carry

    lax.fori_loop(0, items, attend_item, 0)
    sums_ref[...] = jnp.zeros_like(sums_ref)
    bup_sum_ref[...] = jnp.zeros_like(bup_sum_ref)
    parts = range(hidden // width)

    def layer_item(item, carry):
        for copy in ctx_swap(item):
            copy.wait()
        span = pl.ds(pl.multiple_of(item * tokens, tokens), tokens)
        z_one = tok_ref[span].astype(jnp.float32) + rows_ref[0:1]
        for head in range(head_size):
            z_one = z_one + contract(
                ctx_got[head, item], wo_ref[head * cols : (head + 1) * cols], 1, 0
            )
        hat_one, rate_one = normalize(z_one)
        first = hat_one * rows_ref[1:2] + rows_ref[2:3]
        first_ref[...] = first
        first_low = first.astype(jnp.bfloat16)
        yb_ref[span] = first_low
        for part in parts:
            lanes = slice(part * width, (part + 1) * width)
            value = contract(first_low, up_ref[:, lanes], 1, 0) + bup_ref[:, lanes]
            half = 0.5 * (1.0 + lax.erf(value * 0.7071067811865476))
            h_ref[item, :, lanes] = (value * half).astype(jnp.bfloat16)
            slope_ref[:, lanes] = (
                half + value * jnp.exp(-0.5 * value * value) * 0.3989422804014327
            )
        save(1, item).start()
        z_two = first_ref[...] + contract(h_ref[item], down_ref[...], 1, 0) + rows_ref[3:4]
        hat_two, rate_two = normalize(z_two)
        lo_ref[span] = (hat_two * rows_ref[4:5] + rows_ref[5:6]).astype(jnp.bfloat16)
        grads = cot_ref[span].astype(jnp.float32)
        d_two = normalize_back(grads, hat_two, rate_two, rows_ref[4:5])
        d_low = d_two.astype(jnp.bfloat16)
        df_ref[span] = d_low
        sums_ref[4:5] += column_sum(d_low.astype(jnp.float32))
        sums_ref[5:6] += column_sum(grads * hat_two)
        sums_ref[6:7] += column_sum(grads)
        d_first = d_two
        for part in parts:
            lanes = slice(part * width, (part + 1) * width)
            value = contract(d_low, down_ref[lanes], 1, 1) * slope_ref[:, lanes]
            short = value.astype(jnp.bfloat16)
            du_ref[item, :, lanes] = short
            bup_sum_ref[:, lanes] += column_sum(short.astype(jnp.float32))
        save(2, item).start()
        d_first = d_first + contract(du_ref[item], up_ref[...], 1, 1)
        d_one = normalize_back(d_first, hat_one, rate_one, rows_ref[1:2])
        dz_ref[span] = d_one
        short = d_one.astype(jnp.bfloat16)
        da_ref[span] = short
        sums_ref[0:1] += column_sum(short.astype(jnp.float32))
        sums_ref[1:2] += column_sum(d_first * hat_one)
        sums_ref[2:3] += column_sum(d_first)
        return carry

    lax.fori_loop(0, items, layer_item, 0)
    for number in range(3):
        for item in range(items):
            save(number, item).wait()


def forward_all(w_own, b_own, w_out, w_up, w_down, rows, b_up, token_rows, masked, inputs_full):
    seq_local, head_size, tokens, width = inputs_full.shape
    length = head_size * tokens
    cols = w_own.shape[1] // 3
    hidden = w_up.shape[1]
    own = seq_local * tokens
    short = jnp.bfloat16
    whole = pl.BlockSpec(memory_space=pltpu.VMEM)
    any_space = pl.BlockSpec(memory_space=pl.ANY)
    return pl.pallas_call(
        forward_kernel,
        out_shape=(
            jax.ShapeDtypeStruct((seq_local, length, 3 * cols), short),
            jax.ShapeDtypeStruct((seq_local, tokens, hidden), short),
            jax.ShapeDtypeStruct((seq_local, tokens, hidden), short),
            jax.ShapeDtypeStruct((head_size, seq_local, tokens, cols), short),
            jax.ShapeDtypeStruct((seq_local, 8, length), jnp.float32),
            jax.ShapeDtypeStruct((own, width), short),
            jax.ShapeDtypeStruct((own, width), short),
            jax.ShapeDtypeStruct((own, width), short),
            jax.ShapeDtypeStruct((own, width), short),
            jax.ShapeDtypeStruct((own, width), jnp.float32),
            jax.ShapeDtypeStruct((8, width), jnp.float32),
            jax.ShapeDtypeStruct((1, hidden), jnp.float32),
        ),
        in_specs=[whole] * 9 + [any_space],
        out_specs=(any_space,) * 3 + (whole,) * 9,
        scratch_shapes=[
            pltpu.VMEM(inputs_full.shape, short),
            pltpu.VMEM((seq_local, length, 3 * cols), short),
            pltpu.VMEM((seq_local, tokens, hidden), short),
            pltpu.VMEM((seq_local, tokens, hidden), short),
            pltpu.VMEM((tokens, hidden), jnp.float32),
            pltpu.VMEM((tokens, width), jnp.float32),
            pltpu.SemaphoreType.DMA((seq_local,)),
            pltpu.SemaphoreType.DMA((3, seq_local)),
        ]
        + swap_scratch(seq_local, head_size, tokens, cols),
        compiler_params=pltpu.CompilerParams(
            collective_id=2, has_side_effects=True, vmem_limit_bytes=60 * 1024 * 1024
        ),
        name="forward_all",
    )(w_own, b_own, w_out, w_up, w_down, rows, b_up, token_rows, masked, inputs_full)


def backward_kernel(
    da_ref,
    wo_ref,
    w_ref,
    lse_ref,
    dz_ref,
    df_ref,
    yb_ref,
    ctx_ref,
    h_any,
    du_any,
    x_any,
    qkv_any,
    blocks_ref,
    db_ref,
    grad_ref,
    h_ref,
    du_ref,
    x_ref,
    qkv_ref,
    load_sem,
    dall,
    acc,
    dw_ref,
    dctx_src,
    dctx_send,
    dctx_recv,
    dctx_own,
    d_src,
    d_send,
    d_recv,
    d_own,
    dctx_got,
    d_got,
):
    loads = [
        pltpu.make_async_copy(source, target, load_sem.at[number])
        for number, (source, target) in enumerate(
            [(h_any, h_ref), (du_any, du_ref), (qkv_any, qkv_ref), (x_any, x_ref)]
        )
    ]
    for load in loads:
        load.start()
    head_size, items, tokens, cols = ctx_ref.shape
    width = yb_ref.shape[1]
    hidden = h_ref.shape[1]
    length = head_size * tokens
    across = width // BLK
    greet_head(head_size)

    def dctx_swap(item):
        return swap(dctx_src, dctx_got, dctx_send, dctx_recv, dctx_own, item)

    def d_swap(item):
        return swap(d_src, d_got, d_send, d_recv, d_own, item)

    for item in range(items):
        dctx = contract(da_ref[item * tokens : (item + 1) * tokens], wo_ref[...], 1, 1)
        for head in range(head_size):
            dctx_src[item, head] = dctx[:, head * cols : (head + 1) * cols].astype(jnp.bfloat16)
        for copy in dctx_swap(item):
            copy.start()

    blocks_ref[NBLK] = jnp.zeros((BLK, BLK), jnp.bfloat16)

    first = 3 * across * across
    for head in range(head_size):
        value = contract(ctx_ref[head].reshape(items * tokens, cols), da_ref[...], 0, 0)
        value = value.astype(jnp.bfloat16)
        for begin in range(0, cols, min(cols, BLK)):
            row = head * cols + begin
            part = min(cols, BLK)
            for col in range(across):
                number = first + (row // BLK) * across + col
                blocks_ref[number, row % BLK : row % BLK + part] = value[
                    begin : begin + part, col * BLK : (col + 1) * BLK
                ]
    first = 4 * across * across
    wide = hidden // BLK
    loads[1].wait()

    def up_part(turn, carry):
        span = pl.ds(pl.multiple_of(turn * width, width), width)
        value = contract(yb_ref[...], du_ref[:, span], 0, 0).astype(jnp.bfloat16)
        for row in range(across):
            for col in range(across):
                blocks_ref[first + row * wide + turn * across + col] = value[
                    row * BLK : (row + 1) * BLK, col * BLK : (col + 1) * BLK
                ]
        return carry

    lax.fori_loop(0, hidden // width, up_part, 0)
    loads[0].wait()
    second = first + across * wide

    def down_part(turn, carry):
        span = pl.ds(pl.multiple_of(turn * width, width), width)
        value = contract(h_ref[:, span], df_ref[...], 0, 0).astype(jnp.bfloat16)
        for row in range(across):
            for col in range(across):
                blocks_ref[second + (turn * across + row) * across + col] = value[
                    row * BLK : (row + 1) * BLK, col * BLK : (col + 1) * BLK
                ]
        return carry

    lax.fori_loop(0, hidden // width, down_part, 0)
    dw_ref[...] = jnp.zeros_like(dw_ref)
    db_ref[...] = jnp.zeros_like(db_ref)
    loads[2].wait()
    loads[3].wait()
    step = min(QUERIES, tokens)
    scale = jnp.bfloat16(SCALE)

    def attend_item(item, carry):
        for copy in dctx_swap(item):
            copy.wait()
        for number in range(cols // HD):
            low = number * HD
            keys = qkv_ref[item, :, cols + low : cols + low + HD]
            values = qkv_ref[item, :, 2 * cols + low : 2 * cols + low + HD]
            for begin in range(0, length, step):
                query = qkv_ref[item, begin : begin + step, low : low + HD] * scale
                dctx = dctx_got[
                    begin // tokens, item, pl.ds(begin % tokens, step), low : low + HD
                ]
                scores = contract(keys, query, 1, 1)
                probs = jnp.exp(scores - lse_ref[item, number : number + 1, begin : begin + step])
                dprobs = contract(values, dctx, 1, 1)
                inner = jnp.sum(probs * dprobs, axis=0, keepdims=True)
                dscores = (probs * (dprobs - inner)).astype(jnp.bfloat16)
                dkey = contract(dscores, query, 1, 0)
                dvalue = contract(probs.astype(jnp.bfloat16), dctx, 1, 0)
                if begin == 0:
                    acc[0] = dkey
                    acc[1] = dvalue
                else:
                    acc[0] += dkey
                    acc[1] += dvalue
                dquery = contract(keys, dscores, 0, 0).T * SCALE
                dall[begin : begin + step, low : low + HD] = dquery.astype(jnp.bfloat16)
            dall[:, cols + low : cols + low + HD] = acc[0].astype(jnp.bfloat16)
            dall[:, 2 * cols + low : 2 * cols + low + HD] = acc[1].astype(jnp.bfloat16)
        delta = dall[...]
        d_src[item] = delta.reshape(head_size, tokens, 3 * cols)
        for copy in d_swap(item):
            copy.start()
        dw_ref[...] += contract(x_ref[item].reshape(length, width), delta, 0, 0)
        db_ref[...] += jnp.sum(delta.astype(jnp.float32), axis=0, keepdims=True)
        return carry

    lax.fori_loop(0, items, attend_item, 0)

    head_me = lax.axis_index("head")
    for number in range(3):
        value = dw_ref[:, number * cols : (number + 1) * cols].astype(jnp.bfloat16)
        for row in range(across):
            for col in range(across):
                rows = value[row * BLK : (row + 1) * BLK]
                parts = []
                for begin in range(0, BLK, min(cols, BLK)):
                    lane = col * BLK + begin
                    begin_own = lane % cols
                    part = rows[:, begin_own : begin_own + min(cols, BLK)]
                    parts.append(jnp.where(head_me == lane // cols, part, jnp.zeros_like(part)))
                whole = parts[0] if len(parts) == 1 else jnp.concatenate(parts, 1)
                blocks_ref[number * across * across + row * across + col] = whole

    def input_item(item, carry):
        for copy in d_swap(item):
            copy.wait()
        span = pl.ds(pl.multiple_of(item * tokens, tokens), tokens)
        total = dz_ref[span]
        for head in range(head_size):
            total = total + contract(d_got[head, item], w_ref[head], 1, 1)
        grad_ref[item] = total
        return carry

    lax.fori_loop(0, items, input_item, 0)


def backward(d_branch, w_out, w_qkv, lse, d_zone, d_ffn, first_low, context, hidden, d_hidden, inputs_full, qkv):
    head_size, seq_local, tokens, cols = context.shape
    width = w_out.shape[0]
    length = head_size * tokens
    whole = pl.BlockSpec(memory_space=pltpu.VMEM)
    any_space = pl.BlockSpec(memory_space=pl.ANY)

    def like(array):
        return pltpu.VMEM(array.shape, array.dtype)

    return pl.pallas_call(
        backward_kernel,
        out_shape=(
            jax.ShapeDtypeStruct((NBLK + 1, BLK, BLK), jnp.bfloat16),
            jax.ShapeDtypeStruct((1, 3 * cols), jnp.float32),
            jax.ShapeDtypeStruct((seq_local, tokens, width), jnp.float32),
        ),
        in_specs=[whole] * 8 + [any_space] * 4,
        out_specs=(whole, whole, whole),
        scratch_shapes=[
            like(hidden),
            like(d_hidden),
            like(inputs_full),
            like(qkv),
            pltpu.SemaphoreType.DMA((4,)),
            pltpu.VMEM((length, 3 * cols), jnp.bfloat16),
            pltpu.VMEM((2, length, HD), jnp.float32),
            pltpu.VMEM((width, 3 * cols), jnp.float32),
        ]
        + swap_scratch(seq_local, head_size, tokens, cols)
        + swap_scratch(seq_local, head_size, tokens, 3 * cols)
        + [
            pltpu.VMEM((head_size, seq_local, tokens, cols), jnp.bfloat16),
            pltpu.VMEM((head_size, seq_local, tokens, 3 * cols), jnp.bfloat16),
        ],
        compiler_params=pltpu.CompilerParams(
            collective_id=4, has_side_effects=True, vmem_limit_bytes=60 * 1024 * 1024
        ),
        name="backward",
    )(
        d_branch,
        w_out,
        w_qkv,
        lse,
        d_zone,
        d_ffn,
        first_low,
        context,
        hidden,
        d_hidden,
        inputs_full,
        qkv,
    )


def high_product(left, right, left_axis, right_axis):
    return lax.dot_general(
        left,
        right,
        (((left_axis,), (right_axis,)), ((), ())),
        precision=HIGH,
        preferred_element_type=jnp.float32,
    )


def adam_kernel(
    grad_ref,
    master_ref,
    one_ref,
    two_ref,
    left_ref,
    right_ref,
    average_ref,
    new_one_ref,
    new_two_ref,
    new_master_ref,
    new_short_ref,
    new_average_ref,
):
    slots = range(grad_ref.shape[0])
    correct = 1.0 - 0.5**STEP
    rotated = [high_product(left_ref[slot], grad_ref[slot], 0, 0) for slot in slots]
    rotated = [high_product(rotated[slot], right_ref[slot], 1, 0) for slot in slots]
    normed = []
    for slot in slots:
        first = 0.5 * one_ref[slot] + 0.5 * rotated[slot]
        second = 0.5 * two_ref[slot] + 0.5 * rotated[slot] * rotated[slot]
        new_one_ref[slot] = first
        new_two_ref[slot] = second
        normed.append(first / correct / (jnp.sqrt(second / correct) + ADAM_EPS))
    turned = [high_product(left_ref[slot], normed[slot], 1, 0) for slot in slots]
    turned = [high_product(turned[slot], right_ref[slot], 1, 1) for slot in slots]
    for slot in slots:
        updated = master_ref[slot] - RATE * (turned[slot] + DECAY * master_ref[slot])
        new_master_ref[slot] = updated
        new_short_ref[slot] = updated.astype(jnp.bfloat16)
        new_average_ref[slot] = KEEP * average_ref[slot] + (1.0 - KEEP) * updated


def adam(grads, master, moment_one, moment_two, basis_left, basis_right, average):
    slots = grads.shape[0]
    together = math.gcd(slots, 4)
    spec = pl.BlockSpec((together, BLK, BLK), lambda s: (s, 0, 0))
    full = jax.ShapeDtypeStruct(grads.shape, jnp.float32)
    return pl.pallas_call(
        adam_kernel,
        grid=(slots // together,),
        out_shape=(full, full, full, jax.ShapeDtypeStruct(grads.shape, jnp.bfloat16), full),
        in_specs=[spec] * 7,
        out_specs=(spec,) * 5,
        name="adam",
    )(grads, master, moment_one, moment_two, basis_left, basis_right, average)


MESH = pl.DeviceIdType.MESH
VEC_ROWS = 16
PIECE = 16


def cut(seq_size, head_size):
    cores = 2 if head_size % 2 == 0 else 1
    rows = 1
    while 2 * (rows * 2) ** 2 <= seq_size and seq_size % (rows * 2) == 0:
        rows = rows * 2
    return (seq_size // rows, rows, head_size // cores, cores)


def place(dims):
    size_z, size_x, size_y, size_c = dims
    seq = lax.axis_index("seq")
    head = lax.axis_index("head")
    return (
        lax.div(seq, size_x),
        lax.rem(seq, size_x),
        lax.div(head, size_c),
        lax.rem(head, size_c),
    )


def device(dims, coords):
    return (coords[0] * dims[1] + coords[1], coords[2] * dims[3] + coords[3])


def flat(dims, coords):
    return ((coords[0] * dims[1] + coords[1]) * dims[2] + coords[2]) * dims[3] + coords[3]


def moved(dims, coords, axis, step):
    new = list(coords)
    new[axis] = lax.rem(coords[axis] + step, dims[axis])
    return tuple(new)


def greet(dims, coords):
    barrier = pltpu.get_barrier_semaphore()
    count = 0
    for axis in range(4):
        for step in range(1, dims[axis]):
            pl.semaphore_signal(
                barrier,
                inc=1,
                device_id=device(dims, moved(dims, coords, axis, step)),
                device_id_type=MESH,
            )
            count = count + 1
    pl.semaphore_wait(barrier, count)


def greet_head(head_size):
    barrier = pltpu.get_barrier_semaphore()
    seq = lax.axis_index("seq")
    head = lax.axis_index("head")
    for step in range(1, head_size):
        pl.semaphore_signal(
            barrier, inc=1, device_id=(seq, lax.rem(head + step, head_size)), device_id_type=MESH
        )
    pl.semaphore_wait(barrier, head_size - 1)


def gather_kernel(
    dims,
    inv_ref,
    x_ref,
    w_ref,
    xf_ref,
    qkv_ref,
    out_ref,
    up_ref,
    down_ref,
    vec_ref,
    wf_ref,
    own_sem,
    x_send,
    x_recv,
    w_send,
    w_recv,
):
    me = place(dims)
    size_z, size_x, size_y, size_c = dims
    head_me = me[2] * size_c + me[3]
    chunk = w_ref.shape[0]

    def spot(index):
        return wf_ref.at[pl.ds(index * chunk, chunk)]

    own_x = pltpu.make_async_copy(x_ref, xf_ref.at[:, head_me], own_sem.at[0])
    own_w = pltpu.make_async_copy(w_ref, spot(flat(dims, me)), own_sem.at[1])
    own_x.start()
    own_w.start()
    greet(dims, me)

    def copy_x(source, head, target, number):
        return pltpu.make_async_remote_copy(
            src_ref=source,
            dst_ref=xf_ref.at[:, head],
            send_sem=x_send.at[number],
            recv_sem=x_recv.at[head],
            device_id=device(dims, target),
            device_id_type=MESH,
        )

    def send_x(source, head, target, number):
        copy = copy_x(source, head, target, number)
        copy.start()

    def arrived_x(head):
        pltpu.make_async_remote_copy(
            src_ref=x_ref,
            dst_ref=xf_ref.at[:, head],
            send_sem=x_send.at[0],
            recv_sem=x_recv.at[head],
            device_id=device(dims, me),
            device_id_type=MESH,
        ).wait_recv()

    def first_x():
        number = 0
        for step in range(1, size_y):
            send_x(x_ref, head_me, moved(dims, me, 2, step), number)
            number = number + 1
        for step in range(1, size_c):
            send_x(x_ref, head_me, moved(dims, me, 3, step), number)
            number = number + 1

    def pass_x():
        number = size_y + size_c - 2
        for step in range(1, size_y):
            other = moved(dims, me, 2, step)
            head = other[2] * size_c + other[3]
            arrived_x(head)
            for hop in range(1, size_c):
                send_x(xf_ref.at[:, head], head, moved(dims, me, 3, hop), number)
                number = number + 1

    def end_x():
        for number in range((size_y - 1) * size_c + size_c - 1):
            copy_x(x_ref, head_me, moved(dims, me, 3, 1), number).wait_send()

    def run(order):
        sent = []

        def when(condition, action):
            if condition is None:
                action()
            else:
                pl.when(condition)(action)

        def both(one, other):
            if one is None or other is None:
                return other if one is None else one
            return jnp.logical_and(one, other)

        def send(source, coords, target, condition):
            index = flat(dims, coords)
            copy = pltpu.make_async_remote_copy(
                src_ref=source,
                dst_ref=spot(index),
                send_sem=w_send.at[len(sent)],
                recv_sem=w_recv.at[index],
                device_id=device(dims, target),
                device_id_type=MESH,
            )
            when(condition, copy.start)
            sent.append((condition, copy.wait_send))

        def along(source, coords, direction, condition):
            target = (lax.rem(me[0] + direction + size_z, size_z),) + tuple(me[1:])
            inside = me[0] < size_z - 1 if direction > 0 else me[0] > 0
            send(source, coords, target, both(condition, inside))

        def forward(source, coords, later, condition=None):
            for axis in later:
                if axis == 0:
                    along(source, coords, 1, condition)
                    along(source, coords, -1, condition)
                    continue
                for step in range(1, dims[axis]):
                    send(source, coords, moved(dims, me, axis, step), condition)

        def arrived(coords, condition=None):
            copy = pltpu.make_async_remote_copy(
                src_ref=w_ref,
                dst_ref=spot(flat(dims, coords)),
                send_sem=w_send.at[0],
                recv_sem=w_recv.at[flat(dims, coords)],
                device_id=device(dims, me),
                device_id_type=MESH,
            )
            when(condition, copy.wait_recv)

        forward(w_ref, me, order + [3])
        first_x()
        held = [tuple(me)]
        for level, axis in enumerate(order):
            later = order[level + 1 :] + [3]
            fresh = []
            for step in range(1, dims[axis]):
                for direction in (1, -1) if axis == 0 else (0,):
                    for coords in held:
                        if axis != 0:
                            source = moved(dims, coords, axis, step)
                            arrived(source)
                            forward(spot(flat(dims, source)), source, later)
                            fresh.append(source)
                            continue
                        source = moved(dims, coords, 0, 2 * size_z - direction * step)
                        there = me[0] >= step if direction > 0 else me[0] < size_z - step
                        arrived(source, there)
                        along(spot(flat(dims, source)), source, direction, there)
                        forward(spot(flat(dims, source)), source, later, there)
                        if direction > 0:
                            fresh.append(source)
            held = held + fresh
            if level == 1:
                pass_x()
        for step in range(1, size_c):
            for coords in held:
                arrived(moved(dims, coords, 3, step))
            for across in range(size_y):
                other = moved(dims, moved(dims, me, 3, step), 2, across)
                arrived_x(other[2] * size_c + other[3])
        for condition, wait in sent:
            when(condition, wait)
        end_x()

    for core in range(size_c):

        @pl.when(me[3] == core)
        def _(core=core):
            run([2, 0, 1] if core % 2 == 0 else [2, 1, 0])

    own_x.wait()
    own_w.wait()
    unpack(dims, inv_ref, wf_ref, qkv_ref, out_ref, up_ref, down_ref)
    chunk = w_ref.shape[0]
    for number in range(vec_ref.shape[0]):
        vec_ref[number] = wf_ref[(number + 1) * chunk - 1]


def unpack(dims, inv_ref, wf_ref, qkv_ref, out_ref, up_ref, down_ref):
    head_size = dims[2] * dims[3]
    width = out_ref.shape[0]
    hidden = up_ref.shape[1]
    cols = width // head_size
    across = width // BLK

    def block(number):
        piece = inv_ref[number]
        return jnp.concatenate([wf_ref[piece + part] for part in range(BLK // PIECE)], 0)

    def rows_of(row_count, first, col_count, store):
        def one(row, carry):
            span = pl.ds(pl.multiple_of(row * BLK, BLK), BLK)
            for col in range(col_count):
                store(span, col, block(first + row * col_count + col))
            return carry

        lax.fori_loop(0, row_count, one, 0)

    for number in range(3):

        def store_qkv(span, col, value, number=number):
            for begin in range(0, BLK, min(cols, BLK)):
                head = (col * BLK + begin) // cols
                lane = (col * BLK + begin) % cols
                part = min(cols, BLK)
                qkv_ref[head, span, number * cols + lane : number * cols + lane + part] = value[
                    :, begin : begin + part
                ]

        rows_of(across, number * across * across, across, store_qkv)

    def store_in(ref):
        def store(span, col, value):
            ref[span, col * BLK : (col + 1) * BLK] = value

        return store

    rows_of(across, 3 * across * across, across, store_in(out_ref))
    first = 4 * across * across
    rows_of(across, first, hidden // BLK, store_in(up_ref))
    first = first + across * (hidden // BLK)
    rows_of(hidden // BLK, first, across, store_in(down_ref))


def gather_all(dims, inverse, inputs, packed):
    size_z, size_x, size_y, size_c = dims
    total = size_z * size_x * size_y * size_c
    head_size = size_y * size_c
    seq_local, tok_local, width = inputs.shape
    any_space = pl.BlockSpec(memory_space=pl.ANY)
    whole = pl.BlockSpec(memory_space=pltpu.VMEM)
    sends_x = (size_y - 1) * size_c + size_c - 1
    sends_w = 3 * total
    return pl.pallas_call(
        functools.partial(gather_kernel, dims),
        out_shape=(
            jax.ShapeDtypeStruct((seq_local, head_size, tok_local, width), inputs.dtype),
            jax.ShapeDtypeStruct((head_size, width, 3 * width // head_size), packed.dtype),
            jax.ShapeDtypeStruct((width, width), packed.dtype),
            jax.ShapeDtypeStruct((width, FF), packed.dtype),
            jax.ShapeDtypeStruct((FF, width), packed.dtype),
            jax.ShapeDtypeStruct((total, VEC_ROWS, BLK), packed.dtype),
        ),
        in_specs=[pl.BlockSpec(memory_space=pltpu.SMEM), whole, whole],
        out_specs=(any_space, whole, whole, whole, whole, whole),
        scratch_shapes=[
            pltpu.VMEM((total * packed.shape[0],) + packed.shape[1:], packed.dtype),
            pltpu.SemaphoreType.DMA((2,)),
            pltpu.SemaphoreType.DMA((max(sends_x, 1),)),
            pltpu.SemaphoreType.DMA((head_size,)),
            pltpu.SemaphoreType.DMA((max(sends_w, 1),)),
            pltpu.SemaphoreType.DMA((total,)),
        ],
        compiler_params=pltpu.CompilerParams(
            collective_id=0, has_side_effects=True, vmem_limit_bytes=40 * 1024 * 1024
        ),
        name="gather_all",
    )(inverse, inputs, packed)


def scatter_kernel(
    dims,
    slots,
    owner_ref,
    blocks_ref,
    vec_ref,
    grad_ref,
    vec_out_ref,
    term,
    got_c,
    got_x,
    got_y,
    got_z,
    send_c,
    send_x,
    send_y,
    send_z,
    recv_c,
    recv_x,
    recv_y,
    recv_z,
):
    me = place(dims)
    size_z, size_x, size_y, size_c = dims
    rows = slots * BLK
    greet(dims, me)

    def block_of(dest, slot):
        return blocks_ref[jnp.minimum(owner_ref[dest * slots + slot], NBLK)]

    def total_of(dest, extras, keep_block, keep_vec, kind=jnp.float32):
        def one(slot, carry):
            value = block_of(dest, slot).astype(kind)
            span = pl.ds(pl.multiple_of(slot * BLK, BLK), BLK)
            for ref, lead in extras:
                value = value + ref[lead + (span,)].astype(kind)
            keep_block(slot, span, value)
            return carry

        lax.fori_loop(0, slots, one, 0)
        value = vec_ref[dest].astype(kind)
        for ref, lead in extras:
            value = value + ref[lead + (pl.ds(rows, VEC_ROWS),)].astype(kind)
        keep_vec(value)

    def into_term(dest, extras):
        narrow = len(extras) < 2

        def keep_block(slot, span, value):
            term[dest, span] = value.astype(jnp.bfloat16)

        def keep_vec(value):
            term[dest, pl.ds(rows, VEC_ROWS)] = value.astype(jnp.bfloat16)

        total_of(dest, extras, keep_block, keep_vec, jnp.bfloat16 if narrow else jnp.float32)

    def remote(dest, got, send, recv, hop, index, target):
        return pltpu.make_async_remote_copy(
            src_ref=term.at[dest],
            dst_ref=got.at[hop, index],
            send_sem=send.at[hop, index],
            recv_sem=recv.at[hop, index],
            device_id=device(dims, target),
            device_id_type=MESH,
        )

    def each(axis, begin, end, coords_of, extras_of, got, send, recv, only=None):
        for step in range(1, dims[axis]) if only is None else [only]:
            target = moved(dims, me, axis, step)

            def one(index, carry, step=step, target=target):
                coords = list(coords_of(index))
                coords[axis] = target[axis]
                dest = flat(dims, coords)
                into_term(dest, extras_of(coords))
                remote(dest, got, send, recv, step - 1, index, target).start()
                return carry

            if end == begin + 1:
                one(begin, 0)
            else:
                lax.fori_loop(begin, end, one, 0)

    def wait_for(axis, got, send, recv, index):
        found = []
        for step in range(1, dims[axis]):
            remote(0, got, send, recv, step - 1, index, moved(dims, me, axis, step)).wait_recv()
            found.append((got, (step - 1, index)))
        return found

    def turned(axis, order):
        return lax.rem(me[axis] + 1 + order, dims[axis])

    def order_of(axis, coords):
        return lax.rem(coords[axis] - me[axis] + 2 * dims[axis] - 1, dims[axis])

    def index_c(coords):
        return (order_of(0, coords) * size_x + order_of(1, coords)) * size_y + order_of(2, coords)

    def coords_c(index):
        return (
            turned(0, lax.div(index, size_x * size_y)),
            turned(1, lax.rem(lax.div(index, size_y), size_x)),
            turned(2, lax.rem(index, size_y)),
            me[3],
        )

    def run(first, second):
        size_s = dims[second]

        def coords_f(index):
            coords = list(me)
            coords[0] = turned(0, lax.div(index, size_s))
            coords[second] = turned(second, lax.rem(index, size_s))
            return coords

        def coords_s(index):
            coords = list(me)
            coords[0] = turned(0, index)
            return coords

        def coords_z(index):
            return me

        def extras_c(coords):
            return []

        def extras_f(coords):
            return wait_for(3, got_c, send_c, recv_c, index_c(coords))

        def extras_s(coords):
            index = order_of(0, coords) * size_s + order_of(second, coords)
            return extras_f(coords) + wait_for(first, got_x, send_x, recv_x, index)

        def extras_z(coords):
            return extras_s(coords) + wait_for(
                second, got_y, send_y, recv_y, order_of(0, coords)
            )

        def stage_c(order):
            group = size_x * size_y
            each(3, order * group, (order + 1) * group, coords_c, extras_c, got_c, send_c, recv_c)

        def stage_f(order):
            group = size_s
            each(
                first, order * group, (order + 1) * group, coords_f, extras_f, got_x, send_x, recv_x
            )

        stage_c(0)
        for order in range(1, size_z):
            stage_c(order)
            stage_f(order - 1)
        stage_f(size_z - 1)
        for order in range(size_z):
            each(second, order, order + 1, coords_s, extras_s, got_y, send_y, recv_y)
            if order + 1 < size_z:
                each(0, 0, 1, coords_z, extras_z, got_z, send_z, recv_z, only=order + 1)
        extras = extras_z(me) + wait_for(0, got_z, send_z, recv_z, 0)

        def keep_block(slot, span, value):
            grad_ref[slot] = value

        def keep_vec(value):
            vec_out_ref[...] = value

        total_of(flat(dims, me), extras, keep_block, keep_vec)
        drain(3, size_z * size_x * size_y, got_c, send_c, recv_c)
        drain(first, size_z * size_s, got_x, send_x, recv_x)
        drain(second, size_z, got_y, send_y, recv_y)
        drain(0, 1, got_z, send_z, recv_z)

    def drain(axis, count, got, send, recv):
        for step in range(1, dims[axis]):

            def one(index, carry, step=step):
                remote(
                    0, got, send, recv, step - 1, index, moved(dims, me, axis, step)
                ).wait_send()
                return carry

            lax.fori_loop(0, count, one, 0)

    for core in range(size_c):

        @pl.when(me[3] == core)
        def _(core=core):
            run(1 + core % 2, 2 - core % 2)


def scatter_sums(dims, owner_slot, blocks, vec_terms):
    size_z, size_x, size_y, size_c = dims
    total = size_z * size_x * size_y * size_c
    slots = owner_slot.shape[0] // total
    chunk = (slots * BLK + VEC_ROWS, BLK)
    shapes = [
        (max(size_c - 1, 1), size_z * size_x * size_y),
        (max(size_x - 1, size_y - 1, 1), size_z * max(size_x, size_y)),
        (max(size_x - 1, size_y - 1, 1), size_z),
        (max(size_z - 1, 1), 1),
    ]
    whole = pl.BlockSpec(memory_space=pltpu.VMEM)
    return pl.pallas_call(
        functools.partial(scatter_kernel, dims, slots),
        out_shape=(
            jax.ShapeDtypeStruct((slots, BLK, BLK), jnp.float32),
            jax.ShapeDtypeStruct((VEC_ROWS, BLK), jnp.float32),
        ),
        in_specs=[pl.BlockSpec(memory_space=pltpu.SMEM), whole, whole],
        out_specs=(whole, whole),
        scratch_shapes=[pltpu.VMEM((total,) + chunk, jnp.bfloat16)]
        + [pltpu.VMEM(shape + chunk, jnp.bfloat16) for shape in shapes]
        + [pltpu.SemaphoreType.DMA(shape) for shape in shapes]
        + [pltpu.SemaphoreType.DMA(shape) for shape in shapes],
        compiler_params=pltpu.CompilerParams(
            collective_id=1, has_side_effects=True, vmem_limit_bytes=60 * 1024 * 1024
        ),
        name="scatter_sums",
    )(owner_slot, blocks, vec_terms)


def three_parts(values):
    high = lax.reduce_precision(values, 8, 7)
    rest = values - high
    middle = lax.reduce_precision(rest, 8, 7)
    low = lax.reduce_precision(rest - middle, 8, 7)
    return [part.astype(jnp.bfloat16) for part in (high, middle, low)]


def as_rows(vector, rows):
    return jnp.pad(vector, (0, rows * BLK - vector.shape[0])).reshape(rows, BLK)


def ceil_to(value, unit):
    return -(-value // unit) * unit


def body(
    inputs,
    cotangent,
    span_offset,
    span_len,
    owner_slot,
    master,
    moment_one,
    moment_two,
    basis_left,
    basis_right,
    average,
    vec_master,
    vec_moment_one,
    vec_moment_two,
):
    both = ("seq", "head")
    seq_size = lax.axis_size("seq")
    head_size = lax.axis_size("head")
    total = seq_size * head_size
    head_index = lax.axis_index("head")
    seq_local, tok_local, width = inputs.shape
    slots_local = master.shape[0]
    slot_total = slots_local * total
    vec_local = vec_master.shape[0]

    dims = cut(seq_size, head_size)

    mask = span_mask(span_offset, span_len)
    masked = jnp.where(mask[:, :, None] > 0, cotangent, jnp.zeros_like(cotangent))
    masked = masked.reshape(seq_local * tok_local, width)

    packed = jnp.concatenate(
        [
            master.astype(jnp.bfloat16).reshape(slots_local * BLK, BLK),
            as_rows(jnp.concatenate(three_parts(vec_master)), VEC_ROWS),
        ],
        0,
    ).reshape(-1, PIECE, BLK)
    numbers = jnp.arange(slot_total, dtype=jnp.int32)
    inverse = jnp.sum(
        jnp.where(owner_slot[:, None] == numbers[None, :], numbers[:, None], 0), axis=0
    )
    pieces = (inverse // slots_local) * packed.shape[0]
    pieces = pieces + (inverse % slots_local) * (BLK // PIECE)
    inputs_full, w_qkv, w_out, w_up, w_down, vec_parts = gather_all(
        dims, pieces, inputs, packed
    )
    parts = (
        vec_parts
        .reshape(total, VEC_ROWS * BLK)[:, : 3 * vec_local]
        .reshape(total, 3, vec_local)
        .astype(jnp.float32)
    )
    all_vector = ((parts[:, 2] + parts[:, 1]) + parts[:, 0]).reshape(-1)

    b_query, b_value, b_out, gain_one, shift_one, b_up, b_down, gain_two, shift_two = split_vector(
        all_vector
    )
    token_rows = inputs.reshape(seq_local * tok_local, width)
    local_shape = (seq_local, tok_local, width)
    cols = width // head_size
    begin = head_index * cols

    def own(array):
        return lax.dynamic_slice_in_dim(array, begin, cols, array.ndim - 1)

    w_own = lax.dynamic_index_in_dim(w_qkv, head_index, 0, keepdims=False)
    b_own = jnp.concatenate([own(b_query), jnp.zeros((cols,), jnp.float32), own(b_value)], 0)
    rows = jnp.stack(
        [b_out, gain_one, shift_one, b_down, gain_two, shift_two, b_down, b_down], 0
    )
    (
        qkv,
        hidden_act,
        d_hidden_in,
        context,
        log_total,
        layer_out,
        d_ffn,
        first_low,
        d_branch,
        d_zone,
        sums,
        grad_bup,
    ) = forward_all(
        w_own,
        b_own[None, :],
        w_out,
        w_up,
        w_down,
        rows,
        b_up[None, :],
        token_rows,
        masked,
        inputs_full,
    )
    layer_out = layer_out.reshape(local_shape)
    blocks, grad_b_own, input_grad = backward(
        d_branch,
        w_out,
        w_qkv,
        log_total,
        d_zone,
        d_ffn,
        first_low,
        context,
        hidden_act.reshape(seq_local * tok_local, FF),
        d_hidden_in.reshape(seq_local * tok_local, FF),
        inputs_full,
        qkv,
    )
    grad_b_own = grad_b_own.reshape(-1)

    def put(array):
        empty = jnp.zeros(array.shape[:-1] + (width,), array.dtype)
        return lax.dynamic_update_slice_in_dim(empty, array, begin, array.ndim - 1)

    vector_terms = jnp.concatenate(
        [
            put(grad_b_own[:cols]),
            put(grad_b_own[2 * cols :]),
            sums[0:3].reshape(-1),
            grad_bup.reshape(-1),
            sums[4:7].reshape(-1),
        ],
        0,
    ).reshape(total, vec_local)
    vec_terms = jnp.pad(vector_terms, ((0, 0), (0, VEC_ROWS * BLK - vec_local)))
    vec_terms = vec_terms.astype(jnp.bfloat16).reshape(total, VEC_ROWS, BLK)
    slot_grad, vec_sums = scatter_sums(dims, owner_slot, blocks, vec_terms)
    vec_grad = vec_sums.reshape(-1)[:vec_local]
    first_moment, second_moment, updated, updated_short, new_average = adam(
        slot_grad, master, moment_one, moment_two, basis_left, basis_right, average
    )
    correct = 1.0 - 0.5**STEP
    vec_first = 0.5 * vec_moment_one + 0.5 * vec_grad
    vec_second = 0.5 * vec_moment_two + 0.5 * vec_grad * vec_grad
    vec_new = vec_master - VEC_RATE * (vec_first / correct) / (
        jnp.sqrt(vec_second / correct) + ADAM_EPS
    )
    return (
        layer_out,
        input_grad,
        slot_grad,
        vec_grad,
        first_moment,
        second_moment,
        updated,
        updated_short,
        new_average,
        vec_first,
        vec_second,
        vec_new,
    )


def solution(mesh):
    placed = (
        P("seq", "head", None),
        P("seq", "head", None),
        P("seq", "head"),
        P("seq", "head"),
        P(),
        P(("seq", "head"), None, None),
        P(("seq", "head"), None, None),
        P(("seq", "head"), None, None),
        P(("seq", "head"), None, None),
        P(("seq", "head"), None, None),
        P(("seq", "head"), None, None),
        P(("seq", "head")),
        P(("seq", "head")),
        P(("seq", "head")),
    )
    return jax.shard_map(
        body,
        mesh=mesh,
        in_specs=placed,
        out_specs=(
            P("seq", "head", None),
            P("seq", "head", None),
            P(("seq", "head"), None, None),
            P(("seq", "head")),
            P(("seq", "head"), None, None),
            P(("seq", "head"), None, None),
            P(("seq", "head"), None, None),
            P(("seq", "head"), None, None),
            P(("seq", "head"), None, None),
            P(("seq", "head")),
            P(("seq", "head")),
            P(("seq", "head")),
        ),
        check_vma=False,
    )
```

```python
import functools
import math

import jax
import jax.numpy as jnp
from jax import lax
from jax.experimental import pallas as pl
from jax.experimental.pallas import tpu as pltpu
from jax.sharding import PartitionSpec as P

D = 512
FF = 2048
WIN = 16
BLK = 128
STEP = 5
HD = 64
NBLK = 192
QUERIES = 256
SCALE = 1.0 / math.sqrt(HD)


NORM_EPS = 1e-06
ADAM_EPS = 1e-08
RATE = 0.05
VEC_RATE = 0.2
DECAY = 0.01
KEEP = 0.9
HIGH = lax.Precision.HIGHEST


def split_vector(vector):
    widths = [D, D, D, D, D, FF, D, D, D]
    pieces = []
    offset = 0
    for extent in widths:
        pieces.append(vector[offset : offset + extent])
        offset = offset + extent
    return pieces


def span_mask(span_offset, span_len):
    offsets = jnp.repeat(span_offset, WIN, axis=1)
    extents = jnp.repeat(span_len, WIN, axis=1)
    within = (jnp.arange(offsets.shape[1], dtype=jnp.int32) % WIN)[None, :]
    return ((within >= offsets) & (within < offsets + extents)).astype(jnp.float32)


def contract(left, right, left_axis, right_axis):
    return lax.dot_general(
        left, right, (((left_axis,), (right_axis,)), ((), ())), preferred_element_type=jnp.float32
    )


def swap(source, target, send_sem, recv_sem, own_sem, item):
    head_size = source.shape[1]
    seq = lax.axis_index("seq")
    head = lax.axis_index("head")
    copies = []
    for step in [2, 1, 3] if head_size == 4 else range(1, head_size):
        peer = lax.rem(head + step, head_size)
        copies.append(
            pltpu.make_async_remote_copy(
                src_ref=source.at[item, peer],
                dst_ref=target.at[head, item],
                send_sem=send_sem.at[item, step],
                recv_sem=recv_sem.at[item, step],
                device_id=(seq, peer),
                device_id_type=MESH,
            )
        )
    copies.append(
        pltpu.make_async_copy(source.at[item, head], target.at[head, item], own_sem.at[item])
    )
    return copies


def swap_step(source, target, send_sem, recv_sem, own_sem):
    item = pl.program_id(0)
    for copy in swap(source, target, send_sem, recv_sem, own_sem, item):
        copy.start()

    @pl.when(item == pl.num_programs(0) - 1)
    def _():
        for number in range(source.shape[0]):
            for copy in swap(source, target, send_sem, recv_sem, own_sem, number):
                copy.wait()


def swap_scratch(items, head_size, tokens, columns):
    return [
        pltpu.VMEM((items, head_size, tokens, columns), jnp.bfloat16),
        pltpu.SemaphoreType.DMA((items, head_size)),
        pltpu.SemaphoreType.DMA((items, head_size)),
        pltpu.SemaphoreType.DMA((items,)),
    ]


def normalize(values):
    center = values - jnp.mean(values, axis=-1, keepdims=True)
    spread = jnp.mean(center * center, axis=-1, keepdims=True)
    rate = lax.rsqrt(spread + NORM_EPS)
    return center * rate, rate


def normalize_back(grads, hat, rate, gain):
    scaled = grads * gain
    mean = jnp.mean(scaled, axis=-1, keepdims=True)
    along = jnp.mean(scaled * hat, axis=-1, keepdims=True)
    return rate * (scaled - mean - hat * along)


def column_sum(values):
    return jnp.sum(values, axis=0, keepdims=True)


def forward_kernel(
    b_ref,
    rows_ref,
    bup_ref,
    tok_ref,
    cot_ref,
    w_any,
    wo_any,
    up_any,
    down_any,
    x_any,
    qkv_out,
    h_out,
    du_out,
    ctx_got,
    lse_ref,
    lo_ref,
    df_ref,
    yb_ref,
    da_ref,
    dz_ref,
    sums_ref,
    bup_sum_ref,
    x_ref,
    qkv_ref,
    h_ref,
    du_ref,
    slope_ref,
    first_ref,
    w_ref,
    wo_ref,
    up_ref,
    down_ref,
    weight_sem,
    load_sem,
    out_sem,
    ctx_src,
    ctx_send,
    ctx_recv,
    ctx_own,
):
    head_size, items, tokens, cols = ctx_got.shape
    width = wo_ref.shape[0]
    hidden = up_ref.shape[1]
    length = head_size * tokens

    def load(item):
        return pltpu.make_async_copy(x_any.at[item], x_ref.at[item], load_sem.at[item])

    def save(number, item):
        source, target = ((qkv_ref, qkv_out), (h_ref, h_out), (du_ref, du_out))[number]
        return pltpu.make_async_copy(
            source.at[item], target.at[item], out_sem.at[number, item]
        )

    def ctx_swap(item):
        return swap(ctx_src, ctx_got, ctx_send, ctx_recv, ctx_own, item)

    weights = [
        pltpu.make_async_copy(source, target, weight_sem.at[number])
        for number, (source, target) in enumerate(
            [
                (w_any.at[lax.axis_index("head")], w_ref),
                (wo_any, wo_ref),
                (up_any, up_ref),
                (down_any, down_ref),
            ]
        )
    ]
    weights[0].start()
    for item in range(items):
        load(item).start()
    for copy in weights[1:]:
        copy.start()
    greet_head(head_size)
    weights[0].wait()
    step = min(QUERIES, tokens)

    def attend_item(item, carry):
        load(item).wait()
        rows = x_ref[item].reshape(length, width)
        qkv_ref[item] = (contract(rows, w_ref[...], 1, 0) + b_ref[...]).astype(jnp.bfloat16)
        save(0, item).start()
        for number in range(cols // HD):
            low = number * HD
            keys = qkv_ref[item, :, cols + low : cols + low + HD]
            values = qkv_ref[item, :, 2 * cols + low : 2 * cols + low + HD]
            for begin in range(0, length, step):
                query = qkv_ref[item, begin : begin + step, low : low + HD] * jnp.bfloat16(SCALE)
                scores = contract(keys, query, 1, 1)
                highest = jnp.max(scores, axis=0, keepdims=True)
                weights = jnp.exp(scores - highest)
                summed = jnp.sum(weights, axis=0, keepdims=True)
                probs = (weights * (1.0 / summed)).astype(jnp.bfloat16)
                context = contract(values, probs, 0, 0).T.astype(jnp.bfloat16)
                ctx_src[
                    item, begin // tokens, pl.ds(begin % tokens, step), low : low + HD
                ] = context
                lse_ref[item, number : number + 1, begin : begin + step] = highest + jnp.log(
                    summed
                )
        for copy in ctx_swap(item):
            copy.start()
        return carry

    lax.fori_loop(0, items, attend_item, 0)
    for copy in weights[1:]:
        copy.wait()
    sums_ref[...] = jnp.zeros_like(sums_ref)
    bup_sum_ref[...] = jnp.zeros_like(bup_sum_ref)
    parts = range(hidden // width)

    def layer_item(item, carry):
        for copy in ctx_swap(item):
            copy.wait()
        span = pl.ds(pl.multiple_of(item * tokens, tokens), tokens)
        z_one = tok_ref[span].astype(jnp.float32) + rows_ref[0:1]
        for head in range(head_size):
            z_one = z_one + contract(
                ctx_got[head, item], wo_ref[head * cols : (head + 1) * cols], 1, 0
            )
        hat_one, rate_one = normalize(z_one)
        first = hat_one * rows_ref[1:2] + rows_ref[2:3]
        first_ref[...] = first
        first_low = first.astype(jnp.bfloat16)
        yb_ref[span] = first_low
        for part in parts:
            lanes = slice(part * width, (part + 1) * width)
            value = contract(first_low, up_ref[:, lanes], 1, 0) + bup_ref[:, lanes]
            half = 0.5 * (1.0 + lax.erf(value * 0.7071067811865476))
            h_ref[item, :, lanes] = (value * half).astype(jnp.bfloat16)
            slope_ref[:, lanes] = (
                half + value * jnp.exp(-0.5 * value * value) * 0.3989422804014327
            )
        save(1, item).start()
        z_two = first_ref[...] + contract(h_ref[item], down_ref[...], 1, 0) + rows_ref[3:4]
        hat_two, rate_two = normalize(z_two)
        lo_ref[span] = (hat_two * rows_ref[4:5] + rows_ref[5:6]).astype(jnp.bfloat16)
        grads = cot_ref[span].astype(jnp.float32)
        d_two = normalize_back(grads, hat_two, rate_two, rows_ref[4:5])
        d_low = d_two.astype(jnp.bfloat16)
        df_ref[span] = d_low
        sums_ref[4:5] += column_sum(d_low.astype(jnp.float32))
        sums_ref[5:6] += column_sum(grads * hat_two)
        sums_ref[6:7] += column_sum(grads)
        d_first = d_two
        for part in parts:
            lanes = slice(part * width, (part + 1) * width)
            value = contract(d_low, down_ref[lanes], 1, 1) * slope_ref[:, lanes]
            short = value.astype(jnp.bfloat16)
            du_ref[item, :, lanes] = short
            bup_sum_ref[:, lanes] += column_sum(short.astype(jnp.float32))
        save(2, item).start()
        d_first = d_first + contract(du_ref[item], up_ref[...], 1, 1)
        d_one = normalize_back(d_first, hat_one, rate_one, rows_ref[1:2])
        dz_ref[span] = d_one
        short = d_one.astype(jnp.bfloat16)
        da_ref[span] = short
        sums_ref[0:1] += column_sum(short.astype(jnp.float32))
        sums_ref[1:2] += column_sum(d_first * hat_one)
        sums_ref[2:3] += column_sum(d_first)
        return carry

    lax.fori_loop(0, items, layer_item, 0)
    for number in range(3):
        for item in range(items):
            save(number, item).wait()


def forward_all(b_own, rows, b_up, token_rows, masked, w_qkv, w_out, w_up, w_down, inputs_full):
    seq_local, head_size, tokens, width = inputs_full.shape
    length = head_size * tokens
    cols = w_qkv.shape[2] // 3
    hidden = w_up.shape[1]
    own = seq_local * tokens
    short = jnp.bfloat16
    whole = pl.BlockSpec(memory_space=pltpu.VMEM)
    any_space = pl.BlockSpec(memory_space=pl.ANY)
    return pl.pallas_call(
        forward_kernel,
        out_shape=(
            jax.ShapeDtypeStruct((seq_local, length, 3 * cols), short),
            jax.ShapeDtypeStruct((seq_local, tokens, hidden), short),
            jax.ShapeDtypeStruct((seq_local, tokens, hidden), short),
            jax.ShapeDtypeStruct((head_size, seq_local, tokens, cols), short),
            jax.ShapeDtypeStruct((seq_local, 8, length), jnp.float32),
            jax.ShapeDtypeStruct((own, width), short),
            jax.ShapeDtypeStruct((own, width), short),
            jax.ShapeDtypeStruct((own, width), short),
            jax.ShapeDtypeStruct((own, width), short),
            jax.ShapeDtypeStruct((own, width), jnp.float32),
            jax.ShapeDtypeStruct((8, width), jnp.float32),
            jax.ShapeDtypeStruct((1, hidden), jnp.float32),
        ),
        in_specs=[whole] * 5 + [any_space] * 5,
        out_specs=(any_space,) * 3 + (whole,) * 9,
        scratch_shapes=[
            pltpu.VMEM(inputs_full.shape, short),
            pltpu.VMEM((seq_local, length, 3 * cols), short),
            pltpu.VMEM((seq_local, tokens, hidden), short),
            pltpu.VMEM((seq_local, tokens, hidden), short),
            pltpu.VMEM((tokens, hidden), jnp.float32),
            pltpu.VMEM((tokens, width), jnp.float32),
            pltpu.VMEM(w_qkv.shape[1:], short),
            pltpu.VMEM(w_out.shape, short),
            pltpu.VMEM(w_up.shape, short),
            pltpu.VMEM(w_down.shape, short),
            pltpu.SemaphoreType.DMA((4,)),
            pltpu.SemaphoreType.DMA((seq_local,)),
            pltpu.SemaphoreType.DMA((3, seq_local)),
        ]
        + swap_scratch(seq_local, head_size, tokens, cols),
        compiler_params=pltpu.CompilerParams(
            collective_id=2, has_side_effects=True, vmem_limit_bytes=60 * 1024 * 1024
        ),
        name="forward_all",
    )(b_own, rows, b_up, token_rows, masked, w_qkv, w_out, w_up, w_down, inputs_full)


def backward_kernel(
    da_ref,
    wo_ref,
    w_ref,
    lse_ref,
    dz_ref,
    df_ref,
    yb_ref,
    ctx_ref,
    h_any,
    du_any,
    x_any,
    qkv_any,
    blocks_ref,
    db_ref,
    grad_ref,
    h_ref,
    du_ref,
    x_ref,
    qkv_ref,
    load_sem,
    dall,
    acc,
    dw_ref,
    dctx_src,
    dctx_send,
    dctx_recv,
    dctx_own,
    d_src,
    d_send,
    d_recv,
    d_own,
    dctx_got,
    d_got,
):
    loads = [
        pltpu.make_async_copy(source, target, load_sem.at[number])
        for number, (source, target) in enumerate(
            [(h_any, h_ref), (du_any, du_ref), (qkv_any, qkv_ref), (x_any, x_ref)]
        )
    ]
    for load in loads:
        load.start()
    head_size, items, tokens, cols = ctx_ref.shape
    width = yb_ref.shape[1]
    hidden = h_ref.shape[1]
    length = head_size * tokens
    across = width // BLK
    greet_head(head_size)

    def dctx_swap(item):
        return swap(dctx_src, dctx_got, dctx_send, dctx_recv, dctx_own, item)

    def d_swap(item):
        return swap(d_src, d_got, d_send, d_recv, d_own, item)

    for item in range(items):
        dctx = contract(da_ref[item * tokens : (item + 1) * tokens], wo_ref[...], 1, 1)
        for head in range(head_size):
            dctx_src[item, head] = dctx[:, head * cols : (head + 1) * cols].astype(jnp.bfloat16)
        for copy in dctx_swap(item):
            copy.start()

    blocks_ref[NBLK] = jnp.zeros((BLK, BLK), jnp.bfloat16)

    first = 3 * across * across
    for head in range(head_size):
        value = contract(ctx_ref[head].reshape(items * tokens, cols), da_ref[...], 0, 0)
        value = value.astype(jnp.bfloat16)
        for begin in range(0, cols, min(cols, BLK)):
            row = head * cols + begin
            part = min(cols, BLK)
            for col in range(across):
                number = first + (row // BLK) * across + col
                blocks_ref[number, row % BLK : row % BLK + part] = value[
                    begin : begin + part, col * BLK : (col + 1) * BLK
                ]
    first = 4 * across * across
    wide = hidden // BLK
    loads[1].wait()

    def up_part(turn, carry):
        span = pl.ds(pl.multiple_of(turn * width, width), width)
        value = contract(yb_ref[...], du_ref[:, span], 0, 0).astype(jnp.bfloat16)
        for row in range(across):
            for col in range(across):
                blocks_ref[first + row * wide + turn * across + col] = value[
                    row * BLK : (row + 1) * BLK, col * BLK : (col + 1) * BLK
                ]
        return carry

    lax.fori_loop(0, hidden // width, up_part, 0)
    loads[0].wait()
    second = first + across * wide

    def down_part(turn, carry):
        span = pl.ds(pl.multiple_of(turn * width, width), width)
        value = contract(h_ref[:, span], df_ref[...], 0, 0).astype(jnp.bfloat16)
        for row in range(across):
            for col in range(across):
                blocks_ref[second + (turn * across + row) * across + col] = value[
                    row * BLK : (row + 1) * BLK, col * BLK : (col + 1) * BLK
                ]
        return carry

    lax.fori_loop(0, hidden // width, down_part, 0)
    dw_ref[...] = jnp.zeros_like(dw_ref)
    db_ref[...] = jnp.zeros_like(db_ref)
    loads[2].wait()
    loads[3].wait()
    step = min(QUERIES, tokens)
    scale = jnp.bfloat16(SCALE)

    def attend_item(item, carry):
        for copy in dctx_swap(item):
            copy.wait()
        for number in range(cols // HD):
            low = number * HD
            keys = qkv_ref[item, :, cols + low : cols + low + HD]
            values = qkv_ref[item, :, 2 * cols + low : 2 * cols + low + HD]
            for begin in range(0, length, step):
                query = qkv_ref[item, begin : begin + step, low : low + HD] * scale
                dctx = dctx_got[
                    begin // tokens, item, pl.ds(begin % tokens, step), low : low + HD
                ]
                scores = contract(keys, query, 1, 1)
                probs = jnp.exp(scores - lse_ref[item, number : number + 1, begin : begin + step])
                dprobs = contract(values, dctx, 1, 1)
                inner = jnp.sum(probs * dprobs, axis=0, keepdims=True)
                dscores = (probs * (dprobs - inner)).astype(jnp.bfloat16)
                dkey = contract(dscores, query, 1, 0)
                dvalue = contract(probs.astype(jnp.bfloat16), dctx, 1, 0)
                if begin == 0:
                    acc[0] = dkey
                    acc[1] = dvalue
                else:
                    acc[0] += dkey
                    acc[1] += dvalue
                dquery = contract(keys, dscores, 0, 0).T * SCALE
                dall[begin : begin + step, low : low + HD] = dquery.astype(jnp.bfloat16)
            dall[:, cols + low : cols + low + HD] = acc[0].astype(jnp.bfloat16)
            dall[:, 2 * cols + low : 2 * cols + low + HD] = acc[1].astype(jnp.bfloat16)
        delta = dall[...]
        d_src[item] = delta.reshape(head_size, tokens, 3 * cols)
        for copy in d_swap(item):
            copy.start()
        dw_ref[...] += contract(x_ref[item].reshape(length, width), delta, 0, 0)
        db_ref[...] += jnp.sum(delta.astype(jnp.float32), axis=0, keepdims=True)
        return carry

    lax.fori_loop(0, items, attend_item, 0)

    head_me = lax.axis_index("head")
    for number in range(3):
        value = dw_ref[:, number * cols : (number + 1) * cols].astype(jnp.bfloat16)
        for row in range(across):
            for col in range(across):
                rows = value[row * BLK : (row + 1) * BLK]
                parts = []
                for begin in range(0, BLK, min(cols, BLK)):
                    lane = col * BLK + begin
                    begin_own = lane % cols
                    part = rows[:, begin_own : begin_own + min(cols, BLK)]
                    parts.append(jnp.where(head_me == lane // cols, part, jnp.zeros_like(part)))
                whole = parts[0] if len(parts) == 1 else jnp.concatenate(parts, 1)
                blocks_ref[number * across * across + row * across + col] = whole

    def input_item(item, carry):
        for copy in d_swap(item):
            copy.wait()
        span = pl.ds(pl.multiple_of(item * tokens, tokens), tokens)
        total = dz_ref[span]
        for head in range(head_size):
            total = total + contract(d_got[head, item], w_ref[head], 1, 1)
        grad_ref[item] = total
        return carry

    lax.fori_loop(0, items, input_item, 0)


def backward(d_branch, w_out, w_qkv, lse, d_zone, d_ffn, first_low, context, hidden, d_hidden, inputs_full, qkv):
    head_size, seq_local, tokens, cols = context.shape
    width = w_out.shape[0]
    length = head_size * tokens
    whole = pl.BlockSpec(memory_space=pltpu.VMEM)
    any_space = pl.BlockSpec(memory_space=pl.ANY)

    def like(array):
        return pltpu.VMEM(array.shape, array.dtype)

    return pl.pallas_call(
        backward_kernel,
        out_shape=(
            jax.ShapeDtypeStruct((NBLK + 1, BLK, BLK), jnp.bfloat16),
            jax.ShapeDtypeStruct((1, 3 * cols), jnp.float32),
            jax.ShapeDtypeStruct((seq_local, tokens, width), jnp.float32),
        ),
        in_specs=[whole] * 8 + [any_space] * 4,
        out_specs=(whole, whole, whole),
        scratch_shapes=[
            like(hidden),
            like(d_hidden),
            like(inputs_full),
            like(qkv),
            pltpu.SemaphoreType.DMA((4,)),
            pltpu.VMEM((length, 3 * cols), jnp.bfloat16),
            pltpu.VMEM((2, length, HD), jnp.float32),
            pltpu.VMEM((width, 3 * cols), jnp.float32),
        ]
        + swap_scratch(seq_local, head_size, tokens, cols)
        + swap_scratch(seq_local, head_size, tokens, 3 * cols)
        + [
            pltpu.VMEM((head_size, seq_local, tokens, cols), jnp.bfloat16),
            pltpu.VMEM((head_size, seq_local, tokens, 3 * cols), jnp.bfloat16),
        ],
        compiler_params=pltpu.CompilerParams(
            collective_id=4, has_side_effects=True, vmem_limit_bytes=60 * 1024 * 1024
        ),
        name="backward",
    )(
        d_branch,
        w_out,
        w_qkv,
        lse,
        d_zone,
        d_ffn,
        first_low,
        context,
        hidden,
        d_hidden,
        inputs_full,
        qkv,
    )


def high_product(left, right, left_axis, right_axis):
    return lax.dot_general(
        left,
        right,
        (((left_axis,), (right_axis,)), ((), ())),
        precision=HIGH,
        preferred_element_type=jnp.float32,
    )


def adam_kernel(
    grad_ref,
    master_ref,
    one_ref,
    two_ref,
    left_ref,
    right_ref,
    average_ref,
    new_one_ref,
    new_two_ref,
    new_master_ref,
    new_short_ref,
    new_average_ref,
):
    slots = range(grad_ref.shape[0])
    correct = 1.0 - 0.5**STEP
    rotated = [high_product(left_ref[slot], grad_ref[slot], 0, 0) for slot in slots]
    rotated = [high_product(rotated[slot], right_ref[slot], 1, 0) for slot in slots]
    normed = []
    for slot in slots:
        first = 0.5 * one_ref[slot] + 0.5 * rotated[slot]
        second = 0.5 * two_ref[slot] + 0.5 * rotated[slot] * rotated[slot]
        new_one_ref[slot] = first
        new_two_ref[slot] = second
        normed.append(first / correct / (jnp.sqrt(second / correct) + ADAM_EPS))
    turned = [high_product(left_ref[slot], normed[slot], 1, 0) for slot in slots]
    turned = [high_product(turned[slot], right_ref[slot], 1, 1) for slot in slots]
    for slot in slots:
        updated = master_ref[slot] - RATE * (turned[slot] + DECAY * master_ref[slot])
        new_master_ref[slot] = updated
        new_short_ref[slot] = updated.astype(jnp.bfloat16)
        new_average_ref[slot] = KEEP * average_ref[slot] + (1.0 - KEEP) * updated


def adam(grads, master, moment_one, moment_two, basis_left, basis_right, average):
    slots = grads.shape[0]
    together = math.gcd(slots, 4)
    spec = pl.BlockSpec((together, BLK, BLK), lambda s: (s, 0, 0))
    full = jax.ShapeDtypeStruct(grads.shape, jnp.float32)
    return pl.pallas_call(
        adam_kernel,
        grid=(slots // together,),
        out_shape=(full, full, full, jax.ShapeDtypeStruct(grads.shape, jnp.bfloat16), full),
        in_specs=[spec] * 7,
        out_specs=(spec,) * 5,
        name="adam",
    )(grads, master, moment_one, moment_two, basis_left, basis_right, average)


MESH = pl.DeviceIdType.MESH
VEC_ROWS = 16
PIECE = 16


def cut(seq_size, head_size):
    cores = 2 if head_size % 2 == 0 else 1
    rows = 1
    while 2 * (rows * 2) ** 2 <= seq_size and seq_size % (rows * 2) == 0:
        rows = rows * 2
    return (seq_size // rows, rows, head_size // cores, cores)


def place(dims):
    size_z, size_x, size_y, size_c = dims
    seq = lax.axis_index("seq")
    head = lax.axis_index("head")
    return (
        lax.div(seq, size_x),
        lax.rem(seq, size_x),
        lax.div(head, size_c),
        lax.rem(head, size_c),
    )


def device(dims, coords):
    return (coords[0] * dims[1] + coords[1], coords[2] * dims[3] + coords[3])


def flat(dims, coords):
    return ((coords[0] * dims[1] + coords[1]) * dims[2] + coords[2]) * dims[3] + coords[3]


def moved(dims, coords, axis, step):
    new = list(coords)
    new[axis] = lax.rem(coords[axis] + step, dims[axis])
    return tuple(new)


def greet(dims, coords):
    barrier = pltpu.get_barrier_semaphore()
    count = 0
    for axis in range(4):
        for step in range(1, dims[axis]):
            pl.semaphore_signal(
                barrier,
                inc=1,
                device_id=device(dims, moved(dims, coords, axis, step)),
                device_id_type=MESH,
            )
            count = count + 1
    pl.semaphore_wait(barrier, count)


def greet_head(head_size):
    barrier = pltpu.get_barrier_semaphore()
    seq = lax.axis_index("seq")
    head = lax.axis_index("head")
    for step in range(1, head_size):
        pl.semaphore_signal(
            barrier, inc=1, device_id=(seq, lax.rem(head + step, head_size)), device_id_type=MESH
        )
    pl.semaphore_wait(barrier, head_size - 1)


def gather_kernel(
    dims,
    inv_ref,
    x_ref,
    w_ref,
    xf_ref,
    qkv_ref,
    out_ref,
    up_ref,
    down_ref,
    vec_ref,
    wf_ref,
    own_sem,
    x_send,
    x_recv,
    w_send,
    w_recv,
):
    me = place(dims)
    size_z, size_x, size_y, size_c = dims
    head_me = me[2] * size_c + me[3]
    chunk = w_ref.shape[0]

    def spot(index):
        return wf_ref.at[pl.ds(index * chunk, chunk)]

    own_x = pltpu.make_async_copy(x_ref, xf_ref.at[:, head_me], own_sem.at[0])
    own_w = pltpu.make_async_copy(w_ref, spot(flat(dims, me)), own_sem.at[1])
    own_x.start()
    own_w.start()
    greet(dims, me)

    def copy_x(source, head, target, number):
        return pltpu.make_async_remote_copy(
            src_ref=source,
            dst_ref=xf_ref.at[:, head],
            send_sem=x_send.at[number],
            recv_sem=x_recv.at[head],
            device_id=device(dims, target),
            device_id_type=MESH,
        )

    def send_x(source, head, target, number):
        copy = copy_x(source, head, target, number)
        copy.start()

    def arrived_x(head):
        pltpu.make_async_remote_copy(
            src_ref=x_ref,
            dst_ref=xf_ref.at[:, head],
            send_sem=x_send.at[0],
            recv_sem=x_recv.at[head],
            device_id=device(dims, me),
            device_id_type=MESH,
        ).wait_recv()

    def first_x():
        number = 0
        for step in range(1, size_y):
            send_x(x_ref, head_me, moved(dims, me, 2, step), number)
            number = number + 1
        for step in range(1, size_c):
            send_x(x_ref, head_me, moved(dims, me, 3, step), number)
            number = number + 1

    def pass_x():
        number = size_y + size_c - 2
        for step in range(1, size_y):
            other = moved(dims, me, 2, step)
            head = other[2] * size_c + other[3]
            arrived_x(head)
            for hop in range(1, size_c):
                send_x(xf_ref.at[:, head], head, moved(dims, me, 3, hop), number)
                number = number + 1

    def end_x():
        for number in range((size_y - 1) * size_c + size_c - 1):
            copy_x(x_ref, head_me, moved(dims, me, 3, 1), number).wait_send()

    def run(order):
        sent = []

        def when(condition, action):
            if condition is None:
                action()
            else:
                pl.when(condition)(action)

        def both(one, other):
            if one is None or other is None:
                return other if one is None else one
            return jnp.logical_and(one, other)

        def send(source, coords, target, condition):
            index = flat(dims, coords)
            copy = pltpu.make_async_remote_copy(
                src_ref=source,
                dst_ref=spot(index),
                send_sem=w_send.at[len(sent)],
                recv_sem=w_recv.at[index],
                device_id=device(dims, target),
                device_id_type=MESH,
            )
            when(condition, copy.start)
            sent.append((condition, copy.wait_send))

        def along(source, coords, direction, condition):
            target = (lax.rem(me[0] + direction + size_z, size_z),) + tuple(me[1:])
            inside = me[0] < size_z - 1 if direction > 0 else me[0] > 0
            send(source, coords, target, both(condition, inside))

        def forward(source, coords, later, condition=None):
            for axis in later:
                if axis == 0:
                    along(source, coords, 1, condition)
                    along(source, coords, -1, condition)
                    continue
                for step in range(1, dims[axis]):
                    send(source, coords, moved(dims, me, axis, step), condition)

        def arrived(coords, condition=None):
            copy = pltpu.make_async_remote_copy(
                src_ref=w_ref,
                dst_ref=spot(flat(dims, coords)),
                send_sem=w_send.at[0],
                recv_sem=w_recv.at[flat(dims, coords)],
                device_id=device(dims, me),
                device_id_type=MESH,
            )
            when(condition, copy.wait_recv)

        forward(w_ref, me, order + [3])
        first_x()
        held = [tuple(me)]
        for level, axis in enumerate(order):
            later = order[level + 1 :] + [3]
            fresh = []
            for step in range(1, dims[axis]):
                for direction in (1, -1) if axis == 0 else (0,):
                    for coords in held:
                        if axis != 0:
                            source = moved(dims, coords, axis, step)
                            arrived(source)
                            forward(spot(flat(dims, source)), source, later)
                            fresh.append(source)
                            continue
                        source = moved(dims, coords, 0, 2 * size_z - direction * step)
                        there = me[0] >= step if direction > 0 else me[0] < size_z - step
                        arrived(source, there)
                        along(spot(flat(dims, source)), source, direction, there)
                        forward(spot(flat(dims, source)), source, later, there)
                        if direction > 0:
                            fresh.append(source)
            held = held + fresh
            if level == 1:
                pass_x()
        for step in range(1, size_c):
            for coords in held:
                arrived(moved(dims, coords, 3, step))
            for across in range(size_y):
                other = moved(dims, moved(dims, me, 3, step), 2, across)
                arrived_x(other[2] * size_c + other[3])
        for condition, wait in sent:
            when(condition, wait)
        end_x()

    for core in range(size_c):

        @pl.when(me[3] == core)
        def _(core=core):
            run([2, 0, 1] if core % 2 == 0 else [0, 1, 2])

    own_x.wait()
    own_w.wait()
    unpack(dims, inv_ref, wf_ref, qkv_ref, out_ref, up_ref, down_ref)
    chunk = w_ref.shape[0]
    for number in range(vec_ref.shape[0]):
        vec_ref[number] = wf_ref[(number + 1) * chunk - 1]


def unpack(dims, inv_ref, wf_ref, qkv_ref, out_ref, up_ref, down_ref):
    head_size = dims[2] * dims[3]
    width = out_ref.shape[0]
    hidden = up_ref.shape[1]
    cols = width // head_size
    across = width // BLK

    def block(number):
        piece = inv_ref[number]
        return jnp.concatenate([wf_ref[piece + part] for part in range(BLK // PIECE)], 0)

    def rows_of(row_count, first, col_count, store):
        def one(row, carry):
            span = pl.ds(pl.multiple_of(row * BLK, BLK), BLK)
            for col in range(col_count):
                store(span, col, block(first + row * col_count + col))
            return carry

        lax.fori_loop(0, row_count, one, 0)

    for number in range(3):

        def store_qkv(span, col, value, number=number):
            for begin in range(0, BLK, min(cols, BLK)):
                head = (col * BLK + begin) // cols
                lane = (col * BLK + begin) % cols
                part = min(cols, BLK)
                qkv_ref[head, span, number * cols + lane : number * cols + lane + part] = value[
                    :, begin : begin + part
                ]

        rows_of(across, number * across * across, across, store_qkv)

    def store_in(ref):
        def store(span, col, value):
            ref[span, col * BLK : (col + 1) * BLK] = value

        return store

    rows_of(across, 3 * across * across, across, store_in(out_ref))
    first = 4 * across * across
    rows_of(across, first, hidden // BLK, store_in(up_ref))
    first = first + across * (hidden // BLK)
    rows_of(hidden // BLK, first, across, store_in(down_ref))


def gather_all(dims, inverse, inputs, packed):
    size_z, size_x, size_y, size_c = dims
    total = size_z * size_x * size_y * size_c
    head_size = size_y * size_c
    seq_local, tok_local, width = inputs.shape
    any_space = pl.BlockSpec(memory_space=pl.ANY)
    whole = pl.BlockSpec(memory_space=pltpu.VMEM)
    sends_x = (size_y - 1) * size_c + size_c - 1
    sends_w = 3 * total
    return pl.pallas_call(
        functools.partial(gather_kernel, dims),
        out_shape=(
            jax.ShapeDtypeStruct((seq_local, head_size, tok_local, width), inputs.dtype),
            jax.ShapeDtypeStruct((head_size, width, 3 * width // head_size), packed.dtype),
            jax.ShapeDtypeStruct((width, width), packed.dtype),
            jax.ShapeDtypeStruct((width, FF), packed.dtype),
            jax.ShapeDtypeStruct((FF, width), packed.dtype),
            jax.ShapeDtypeStruct((total, VEC_ROWS, BLK), packed.dtype),
        ),
        in_specs=[pl.BlockSpec(memory_space=pltpu.SMEM), whole, whole],
        out_specs=(any_space, whole, whole, whole, whole, whole),
        scratch_shapes=[
            pltpu.VMEM((total * packed.shape[0],) + packed.shape[1:], packed.dtype),
            pltpu.SemaphoreType.DMA((2,)),
            pltpu.SemaphoreType.DMA((max(sends_x, 1),)),
            pltpu.SemaphoreType.DMA((head_size,)),
            pltpu.SemaphoreType.DMA((max(sends_w, 1),)),
            pltpu.SemaphoreType.DMA((total,)),
        ],
        compiler_params=pltpu.CompilerParams(
            collective_id=0, has_side_effects=True, vmem_limit_bytes=40 * 1024 * 1024
        ),
        name="gather_all",
    )(inverse, inputs, packed)


def scatter_kernel(
    dims,
    slots,
    owner_ref,
    blocks_ref,
    vec_ref,
    grad_ref,
    vec_out_ref,
    term,
    got_c,
    got_x,
    got_y,
    got_z,
    send_c,
    send_x,
    send_y,
    send_z,
    recv_c,
    recv_x,
    recv_y,
    recv_z,
):
    me = place(dims)
    size_z, size_x, size_y, size_c = dims
    rows = slots * BLK
    greet(dims, me)

    def block_of(dest, slot):
        return blocks_ref[jnp.minimum(owner_ref[dest * slots + slot], NBLK)]

    def total_of(dest, extras, keep_block, keep_vec, kind=jnp.float32):
        def one(slot, carry):
            value = block_of(dest, slot).astype(kind)
            span = pl.ds(pl.multiple_of(slot * BLK, BLK), BLK)
            for ref, lead in extras:
                value = value + ref[lead + (span,)].astype(kind)
            keep_block(slot, span, value)
            return carry

        lax.fori_loop(0, slots, one, 0)
        value = vec_ref[dest].astype(kind)
        for ref, lead in extras:
            value = value + ref[lead + (pl.ds(rows, VEC_ROWS),)].astype(kind)
        keep_vec(value)

    def into_term(dest, extras):
        narrow = len(extras) < 2

        def keep_block(slot, span, value):
            term[dest, span] = value.astype(jnp.bfloat16)

        def keep_vec(value):
            term[dest, pl.ds(rows, VEC_ROWS)] = value.astype(jnp.bfloat16)

        total_of(dest, extras, keep_block, keep_vec, jnp.bfloat16 if narrow else jnp.float32)

    def remote(dest, got, send, recv, hop, index, target):
        return pltpu.make_async_remote_copy(
            src_ref=term.at[dest],
            dst_ref=got.at[hop, index],
            send_sem=send.at[hop, index],
            recv_sem=recv.at[hop, index],
            device_id=device(dims, target),
            device_id_type=MESH,
        )

    def each(axis, begin, end, coords_of, extras_of, got, send, recv, only=None):
        for step in range(1, dims[axis]) if only is None else [only]:
            target = moved(dims, me, axis, step)

            def one(index, carry, step=step, target=target):
                coords = list(coords_of(index))
                coords[axis] = target[axis]
                dest = flat(dims, coords)
                into_term(dest, extras_of(coords))
                remote(dest, got, send, recv, step - 1, index, target).start()
                return carry

            if end == begin + 1:
                one(begin, 0)
            else:
                lax.fori_loop(begin, end, one, 0)

    def wait_for(axis, got, send, recv, index):
        found = []
        for step in range(1, dims[axis]):
            remote(0, got, send, recv, step - 1, index, moved(dims, me, axis, step)).wait_recv()
            found.append((got, (step - 1, index)))
        return found

    def turned(axis, order):
        return lax.rem(me[axis] + 1 + order, dims[axis])

    def order_of(axis, coords):
        return lax.rem(coords[axis] - me[axis] + 2 * dims[axis] - 1, dims[axis])

    def index_c(coords):
        return (order_of(0, coords) * size_x + order_of(1, coords)) * size_y + order_of(2, coords)

    def coords_c(index):
        return (
            turned(0, lax.div(index, size_x * size_y)),
            turned(1, lax.rem(lax.div(index, size_y), size_x)),
            turned(2, lax.rem(index, size_y)),
            me[3],
        )

    def run(first, second):
        size_s = dims[second]

        def coords_f(index):
            coords = list(me)
            coords[0] = turned(0, lax.div(index, size_s))
            coords[second] = turned(second, lax.rem(index, size_s))
            return coords

        def coords_s(index):
            coords = list(me)
            coords[0] = turned(0, index)
            return coords

        def coords_z(index):
            return me

        def extras_c(coords):
            return []

        def extras_f(coords):
            return wait_for(3, got_c, send_c, recv_c, index_c(coords))

        def extras_s(coords):
            index = order_of(0, coords) * size_s + order_of(second, coords)
            return extras_f(coords) + wait_for(first, got_x, send_x, recv_x, index)

        def extras_z(coords):
            return extras_s(coords) + wait_for(
                second, got_y, send_y, recv_y, order_of(0, coords)
            )

        def stage_c(order):
            group = size_x * size_y
            each(3, order * group, (order + 1) * group, coords_c, extras_c, got_c, send_c, recv_c)

        def stage_f(order):
            group = size_s
            each(
                first, order * group, (order + 1) * group, coords_f, extras_f, got_x, send_x, recv_x
            )

        stage_c(0)
        for order in range(1, size_z):
            stage_c(order)
            stage_f(order - 1)
        stage_f(size_z - 1)
        for order in range(size_z):
            each(second, order, order + 1, coords_s, extras_s, got_y, send_y, recv_y)
            if order + 1 < size_z:
                each(0, 0, 1, coords_z, extras_z, got_z, send_z, recv_z, only=order + 1)
        extras = extras_z(me) + wait_for(0, got_z, send_z, recv_z, 0)

        def keep_block(slot, span, value):
            grad_ref[slot] = value

        def keep_vec(value):
            vec_out_ref[...] = value

        total_of(flat(dims, me), extras, keep_block, keep_vec)
        drain(3, size_z * size_x * size_y, got_c, send_c, recv_c)
        drain(first, size_z * size_s, got_x, send_x, recv_x)
        drain(second, size_z, got_y, send_y, recv_y)
        drain(0, 1, got_z, send_z, recv_z)

    def drain(axis, count, got, send, recv):
        for step in range(1, dims[axis]):

            def one(index, carry, step=step):
                remote(
                    0, got, send, recv, step - 1, index, moved(dims, me, axis, step)
                ).wait_send()
                return carry

            lax.fori_loop(0, count, one, 0)

    for core in range(size_c):

        @pl.when(me[3] == core)
        def _(core=core):
            run(1 + core % 2, 2 - core % 2)


def scatter_sums(dims, owner_slot, blocks, vec_terms):
    size_z, size_x, size_y, size_c = dims
    total = size_z * size_x * size_y * size_c
    slots = owner_slot.shape[0] // total
    chunk = (slots * BLK + VEC_ROWS, BLK)
    shapes = [
        (max(size_c - 1, 1), size_z * size_x * size_y),
        (max(size_x - 1, size_y - 1, 1), size_z * max(size_x, size_y)),
        (max(size_x - 1, size_y - 1, 1), size_z),
        (max(size_z - 1, 1), 1),
    ]
    whole = pl.BlockSpec(memory_space=pltpu.VMEM)
    return pl.pallas_call(
        functools.partial(scatter_kernel, dims, slots),
        out_shape=(
            jax.ShapeDtypeStruct((slots, BLK, BLK), jnp.float32),
            jax.ShapeDtypeStruct((VEC_ROWS, BLK), jnp.float32),
        ),
        in_specs=[pl.BlockSpec(memory_space=pltpu.SMEM), whole, whole],
        out_specs=(whole, whole),
        scratch_shapes=[pltpu.VMEM((total,) + chunk, jnp.bfloat16)]
        + [pltpu.VMEM(shape + chunk, jnp.bfloat16) for shape in shapes]
        + [pltpu.SemaphoreType.DMA(shape) for shape in shapes]
        + [pltpu.SemaphoreType.DMA(shape) for shape in shapes],
        compiler_params=pltpu.CompilerParams(
            collective_id=1, has_side_effects=True, vmem_limit_bytes=60 * 1024 * 1024
        ),
        name="scatter_sums",
    )(owner_slot, blocks, vec_terms)


def three_parts(values):
    high = lax.reduce_precision(values, 8, 7)
    rest = values - high
    middle = lax.reduce_precision(rest, 8, 7)
    low = lax.reduce_precision(rest - middle, 8, 7)
    return [part.astype(jnp.bfloat16) for part in (high, middle, low)]


def as_rows(vector, rows):
    return jnp.pad(vector, (0, rows * BLK - vector.shape[0])).reshape(rows, BLK)


def ceil_to(value, unit):
    return -(-value // unit) * unit


def body(
    inputs,
    cotangent,
    span_offset,
    span_len,
    owner_slot,
    master,
    moment_one,
    moment_two,
    basis_left,
    basis_right,
    average,
    vec_master,
    vec_moment_one,
    vec_moment_two,
):
    both = ("seq", "head")
    seq_size = lax.axis_size("seq")
    head_size = lax.axis_size("head")
    total = seq_size * head_size
    head_index = lax.axis_index("head")
    seq_local, tok_local, width = inputs.shape
    slots_local = master.shape[0]
    slot_total = slots_local * total
    vec_local = vec_master.shape[0]

    dims = cut(seq_size, head_size)

    mask = span_mask(span_offset, span_len)
    masked = jnp.where(mask[:, :, None] > 0, cotangent, jnp.zeros_like(cotangent))
    masked = masked.reshape(seq_local * tok_local, width)

    packed = jnp.concatenate(
        [
            master.astype(jnp.bfloat16).reshape(slots_local * BLK, BLK),
            as_rows(jnp.concatenate(three_parts(vec_master)), VEC_ROWS),
        ],
        0,
    ).reshape(-1, PIECE, BLK)
    numbers = jnp.arange(slot_total, dtype=jnp.int32)
    inverse = jnp.sum(
        jnp.where(owner_slot[:, None] == numbers[None, :], numbers[:, None], 0), axis=0
    )
    pieces = (inverse // slots_local) * packed.shape[0]
    pieces = pieces + (inverse % slots_local) * (BLK // PIECE)
    inputs_full, w_qkv, w_out, w_up, w_down, vec_parts = gather_all(
        dims, pieces, inputs, packed
    )
    parts = (
        vec_parts
        .reshape(total, VEC_ROWS * BLK)[:, : 3 * vec_local]
        .reshape(total, 3, vec_local)
        .astype(jnp.float32)
    )
    all_vector = ((parts[:, 2] + parts[:, 1]) + parts[:, 0]).reshape(-1)

    b_query, b_value, b_out, gain_one, shift_one, b_up, b_down, gain_two, shift_two = split_vector(
        all_vector
    )
    token_rows = inputs.reshape(seq_local * tok_local, width)
    local_shape = (seq_local, tok_local, width)
    cols = width // head_size
    begin = head_index * cols

    def own(array):
        return lax.dynamic_slice_in_dim(array, begin, cols, array.ndim - 1)

    b_own = jnp.concatenate([own(b_query), jnp.zeros((cols,), jnp.float32), own(b_value)], 0)
    rows = jnp.stack(
        [b_out, gain_one, shift_one, b_down, gain_two, shift_two, b_down, b_down], 0
    )
    (
        qkv,
        hidden_act,
        d_hidden_in,
        context,
        log_total,
        layer_out,
        d_ffn,
        first_low,
        d_branch,
        d_zone,
        sums,
        grad_bup,
    ) = forward_all(
        b_own[None, :],
        rows,
        b_up[None, :],
        token_rows,
        masked,
        w_qkv,
        w_out,
        w_up,
        w_down,
        inputs_full,
    )
    layer_out = layer_out.reshape(local_shape)
    blocks, grad_b_own, input_grad = backward(
        d_branch,
        w_out,
        w_qkv,
        log_total,
        d_zone,
        d_ffn,
        first_low,
        context,
        hidden_act.reshape(seq_local * tok_local, FF),
        d_hidden_in.reshape(seq_local * tok_local, FF),
        inputs_full,
        qkv,
    )
    grad_b_own = grad_b_own.reshape(-1)

    owned = jnp.arange(width, dtype=jnp.int32) // cols == head_index

    def put(array):
        return jnp.where(owned, jnp.tile(array, head_size), 0.0)

    vector_terms = jnp.concatenate(
        [
            put(grad_b_own[:cols]),
            put(grad_b_own[2 * cols :]),
            sums[0:3].reshape(-1),
            grad_bup.reshape(-1),
            sums[4:7].reshape(-1),
        ],
        0,
    ).reshape(total, vec_local)
    vec_terms = jnp.pad(vector_terms, ((0, 0), (0, VEC_ROWS * BLK - vec_local)))
    vec_terms = vec_terms.astype(jnp.bfloat16).reshape(total, VEC_ROWS, BLK)
    slot_grad, vec_sums = scatter_sums(dims, owner_slot, blocks, vec_terms)
    vec_grad = vec_sums.reshape(-1)[:vec_local]
    first_moment, second_moment, updated, updated_short, new_average = adam(
        slot_grad, master, moment_one, moment_two, basis_left, basis_right, average
    )
    correct = 1.0 - 0.5**STEP
    vec_first = 0.5 * vec_moment_one + 0.5 * vec_grad
    vec_second = 0.5 * vec_moment_two + 0.5 * vec_grad * vec_grad
    vec_new = vec_master - VEC_RATE * (vec_first / correct) / (
        jnp.sqrt(vec_second / correct) + ADAM_EPS
    )
    return (
        layer_out,
        input_grad,
        slot_grad,
        vec_grad,
        first_moment,
        second_moment,
        updated,
        updated_short,
        new_average,
        vec_first,
        vec_second,
        vec_new,
    )


def solution(mesh):
    placed = (
        P("seq", "head", None),
        P("seq", "head", None),
        P("seq", "head"),
        P("seq", "head"),
        P(),
        P(("seq", "head"), None, None),
        P(("seq", "head"), None, None),
        P(("seq", "head"), None, None),
        P(("seq", "head"), None, None),
        P(("seq", "head"), None, None),
        P(("seq", "head"), None, None),
        P(("seq", "head")),
        P(("seq", "head")),
        P(("seq", "head")),
    )
    return jax.shard_map(
        body,
        mesh=mesh,
        in_specs=placed,
        out_specs=(
            P("seq", "head", None),
            P("seq", "head", None),
            P(("seq", "head"), None, None),
            P(("seq", "head")),
            P(("seq", "head"), None, None),
            P(("seq", "head"), None, None),
            P(("seq", "head"), None, None),
            P(("seq", "head"), None, None),
            P(("seq", "head"), None, None),
            P(("seq", "head")),
            P(("seq", "head")),
            P(("seq", "head")),
        ),
        check_vma=False,
    )
```
